128 devices in a mesh: ens: 1, part: 16 (over z, y), feat: 8 (over x, core).
Axes of the slice: x: 4, y: 4, z: 4, core: 2. Of those that a mesh axis runs over, the one named last changes fastest.
Arguments:
- particles: float32 [2048, 32768], P(('ens', 'part'), 'feat')
- prec_diag: float32 [32768], P(('ens', 'feat'))
- target_mean: float32 [32768], P(('ens', 'feat'))
- low_factor: bfloat16 [32768, 64], P(('ens', 'feat'))
Outputs:
- output: float32 [2048, 32768], P(('ens', 'part'), 'feat')
All inputs are finite; a program needn't handle non-finite values.
Results may differ from the reference program's by a relative error of at most 0.00350775.
Values are sent between devices in bfloat16 or wider.
A program may use at most 1 GiB of HBM per device.

```python
import math
import jax
import jax.numpy as jnp

NUM_PARTICLES = 2048
FEAT_DIM = 32768
LOW_RANK = 64
NUM_STEPS = 3

KERN_WIDTH = 2.0 * FEAT_DIM / math.log(NUM_PARTICLES)
STEP_SIZE = 0.15 * NUM_PARTICLES * FEAT_DIM / math.log(NUM_PARTICLES)


def setup_inputs(seed: int = 0, part: int = 0) -> dict:
    part_key = jax.random.fold_in(jax.random.key(seed), part)
    sub_keys = jax.random.split(part_key, 6)
    scale_c = math.log(NUM_PARTICLES) / FEAT_DIM
    prec_diag = scale_c * jax.random.uniform(sub_keys[0], (FEAT_DIM,), jnp.float32, 0.5, 1.5)
    low_f32 = (math.sqrt(math.log(NUM_PARTICLES)) / FEAT_DIM) * jax.random.normal(sub_keys[1], (FEAT_DIM, LOW_RANK), jnp.float32)
    low_factor = low_f32.astype(jnp.bfloat16)
    target_mean = 0.5 * jax.random.normal(sub_keys[2], (FEAT_DIM,), jnp.float32)
    offset = 0.5 * jax.random.normal(sub_keys[3], (FEAT_DIM,), jnp.float32)
    spread = math.sqrt(0.5) * jax.random.normal(sub_keys[4], (NUM_PARTICLES, FEAT_DIM), jnp.float32)
    low_coeff = (FEAT_DIM / math.sqrt(2.0 * LOW_RANK * math.log(NUM_PARTICLES))) * jax.random.normal(sub_keys[5], (NUM_PARTICLES, LOW_RANK), jnp.float32)
    low_part = jnp.dot(low_coeff, low_factor.astype(jnp.float32).T)
    particles = target_mean[None, :] + offset[None, :] + spread + low_part
    return {"particles": particles, "prec_diag": prec_diag, "target_mean": target_mean, "low_factor": low_factor}


def svgd_step(cur_theta, prec_diag, target_mean, low_factor):
    x_dev = cur_theta - target_mean[None, :]
    proj_low = jnp.dot(x_dev.astype(jnp.bfloat16), low_factor, preferred_element_type=jnp.float32)
    low_term = jnp.dot(proj_low.astype(jnp.bfloat16), low_factor.T, preferred_element_type=jnp.float32)
    grad_b = (-(x_dev * prec_diag[None, :] + low_term)).astype(jnp.bfloat16)
    theta_b = cur_theta.astype(jnp.bfloat16)
    gram_mat = jnp.dot(theta_b, theta_b.T, preferred_element_type=jnp.float32)
    sq_norm = jnp.sum(jnp.square(theta_b.astype(jnp.float32)), axis=1)
    sq_dist = jnp.maximum(sq_norm[:, None] + sq_norm[None, :] - 2.0 * gram_mat, 0.0)
    kern_b = jnp.exp(-sq_dist / KERN_WIDTH).astype(jnp.bfloat16)
    row_mass = jnp.sum(kern_b.astype(jnp.float32), axis=1)
    drive_term = jnp.dot(kern_b, grad_b, preferred_element_type=jnp.float32)
    pull_term = jnp.dot(kern_b, theta_b, preferred_element_type=jnp.float32)
    update_dir = (drive_term + (2.0 / KERN_WIDTH) * (row_mass[:, None] * theta_b.astype(jnp.float32) - pull_term)) / NUM_PARTICLES
    return cur_theta + STEP_SIZE * update_dir


def reference(particles, prec_diag, target_mean, low_factor):
    cur_theta = particles
    for step_idx in range(NUM_STEPS):
        cur_theta = svgd_step(cur_theta, prec_diag, target_mean, low_factor)
    return cur_theta
```

```python
import math
import jax
import jax.numpy as jnp
from jax import lax
from jax.sharding import PartitionSpec as P

NUM_STEPS = 3
B = 128


def solution(mesh):
    part_size = mesh.shape["part"]
    feat_size = mesh.shape["feat"]
    axes = ("part", "feat")

    def local_steps(local_theta, prec_loc, mean_loc, factor_loc):
        rows_loc, feat_loc = local_theta.shape
        n_total = rows_loc * part_size
        feat_total = feat_loc * feat_size
        nb = n_total // B
        half = nb // 2
        kern_width = 2.0 * feat_total / math.log(n_total)
        step_size = 0.15 * n_total * feat_total / math.log(n_total)
        part_idx = lax.axis_index("part")
        unit_idx = part_idx * feat_size + lax.axis_index("feat")
        fcol = feat_loc // part_size
        theta = lax.all_to_all(local_theta, "part", split_axis=1, concat_axis=0, tiled=True)
        lam = lax.dynamic_slice_in_dim(prec_loc, part_idx * fcol, fcol)
        mu = lax.dynamic_slice_in_dim(mean_loc, part_idx * fcol, fcol)
        fac = lax.dynamic_slice_in_dim(factor_loc, part_idx * fcol, fcol)
        rank = fac.shape[1]
        row = lax.broadcasted_iota(jnp.int32, (B, B), 0)
        col = lax.broadcasted_iota(jnp.int32, (B, B), 1)
        low = row >= col
        eye = row == col
        packed = unit_idx >= (nb * (half - 1) + half)
        first = jnp.logical_or(jnp.logical_not(packed), low)
        second = jnp.logical_or(jnp.logical_not(packed), jnp.logical_not(low))
        for step_idx in range(NUM_STEPS):
            x_dev = theta - mu[None, :]
            theta_b = theta.astype(jnp.bfloat16)
            proj = jnp.dot(x_dev.astype(jnp.bfloat16), fac, preferred_element_type=jnp.float32)
            blk = theta_b.reshape(nb, B, fcol)
            sq = jnp.sum(jnp.square(theta_b.astype(jnp.float32)), axis=1).reshape(nb, B)
            units, s_i, s_j = [], [], []
            for k in range(1, half):
                units.append(jnp.einsum("iad,ibd->iab", blk, jnp.roll(blk, -k, 0), preferred_element_type=jnp.float32))
                s_i.append(sq)
                s_j.append(jnp.roll(sq, -k, 0))
            units.append(jnp.einsum("iad,ibd->iab", blk[:half], blk[half:], preferred_element_type=jnp.float32))
            s_i.append(sq[:half])
            s_j.append(sq[half:])
            diag = jnp.einsum("iad,ibd->iab", blk, blk, preferred_element_type=jnp.float32)
            units.append(jnp.where(low[None], diag[:half], diag[half:]))
            s_i.append(sq[:half])
            s_j.append(sq[half:])
            units = jnp.concatenate(units, 0)
            s_i = jnp.concatenate(s_i, 0)
            s_j = jnp.concatenate(s_j, 0)
            n_units = units.shape[0]
            s_rows = jnp.stack([s_i, s_j], 1)
            s_rows = jnp.pad(s_rows, ((0, 0), (0, 6), (0, 0)))
            z_rows = proj.reshape(n_units, -1, B)
            send = jnp.concatenate([units, s_rows, z_rows], 1)
            got = lax.psum_scatter(send, axes, scatter_dimension=0, tiled=True)[0]
            g_u, si, sj = got[:B], got[B], got[B + 1]
            z_u = got[B + 8:]
            s_row = jnp.where(first, si[:, None], sj[:, None])
            s_col = jnp.where(second, sj[None, :], si[None, :])
            dist = jnp.maximum(s_row + s_col - 2.0 * g_u, 0.0)
            k_u = jnp.exp(-dist / kern_width).astype(jnp.bfloat16)
            out = jnp.concatenate([k_u, z_u.astype(jnp.bfloat16), jnp.zeros_like(z_u, jnp.bfloat16)], 0)
            allk = lax.all_gather(out[None], axes, axis=0, tiled=True)
            z_b = allk[:, B:B + z_u.shape[0]].reshape(n_total, rank)
            ku = allk[:, :B]
            off = {}
            for k in range(1, half):
                u = ku[(k - 1) * nb:k * nb]
                for i in range(nb):
                    off[i, (i + k) % nb] = u[i]
                    off[(i + k) % nb, i] = u[i].T
            for i in range(half):
                u = ku[nb * (half - 1) + i]
                off[i, i + half] = u
                off[i + half, i] = u.T
                d = ku[nb * (half - 1) + half + i]
                off[i, i] = jnp.where(eye, 1.0, jnp.where(low, d, d.T)).astype(jnp.bfloat16)
                off[i + half, i + half] = jnp.where(eye, 1.0, jnp.where(low, d.T, d)).astype(jnp.bfloat16)
            kern = jnp.concatenate([jnp.concatenate([off[i, j] for j in range(nb)], 1) for i in range(nb)], 0)
            row_mass = jnp.sum(kern, axis=1, dtype=jnp.float32)
            low_term = jnp.einsum("nr,dr->nd", z_b, fac, preferred_element_type=jnp.float32)
            grad_b = (-(x_dev * lam[None, :] + low_term)).astype(jnp.bfloat16)
            drive = jnp.dot(kern, grad_b, preferred_element_type=jnp.float32)
            pull = jnp.dot(kern, theta_b, preferred_element_type=jnp.float32)
            upd = (drive + (2.0 / kern_width) * (row_mass[:, None] * theta_b.astype(jnp.float32) - pull)) / n_total
            theta = theta + step_size * upd
        return lax.all_to_all(theta, "part", split_axis=0, concat_axis=1, tiled=True)

    row_spec = P(("ens", "part"), "feat")
    vec_spec = P(("ens", "feat"))
    fac_spec = P(("ens", "feat"), None)
    return jax.shard_map(local_steps, mesh=mesh, in_specs=(row_spec, vec_spec, vec_spec, fac_spec), out_specs=row_spec, check_vma=False)
```

```python
import functools
import math
import jax
import jax.numpy as jnp
from jax import lax
from jax.experimental import pallas as pl
from jax.experimental.pallas import tpu as pltpu
from jax.sharding import PartitionSpec as P

NUM_STEPS = 3
B = 128
PIECE = 48
F32 = jnp.float32
BF16 = jnp.bfloat16
NT = (((1,), (1,)), ((), ()))
TN = (((0,), (0,)), ((), ()))
NUM_SEMS = 160


def rem(a, n):
    return lax.rem(a, n)


def steps_kernel(cfg, theta_ref, lam_ref, mu_ref, fac_ref, fact_ref, out_ref, t_own, t_par, a_buf, zt, zt_par, zt_b,
                 s_all, g, ring1, ring2, dir3, acc2, acc3, unit, ag, ag_par, kfull, send_sems, recv_sems):
    sizes, nb, kern_width, step_size = cfg["sizes"], cfg["nb"], cfg["kern_width"], cfg["step_size"]
    nx, ny, nz = sizes
    n_total = nb * B
    n_chip = nx * ny * nz
    part, feat = lax.axis_index("part"), lax.axis_index("feat")
    core = rem(feat, 2)
    me = (feat // 2, rem(part, ny), part // ny)

    def dev(coord, c):
        return {"part": coord[2] * ny + coord[1], "feat": coord[0] * 2 + c}

    def shifted(dim, by):
        c = list(me)
        c[dim] = rem(me[dim] + by, sizes[dim])
        return dev(c, core)

    partner = dev(me, 1 - core)
    perms = [(k, (k + 1) % 3, (k + 2) % 3) for k in range(3)]

    ids = {}

    def copy(key, src, dst, to):
        idx = ids.setdefault(key, len(ids))
        assert idx < NUM_SEMS
        return pltpu.make_async_remote_copy(
            src_ref=src, dst_ref=dst, send_sem=send_sems.at[idx], recv_sem=recv_sems.at[idx],
            device_id=to, device_id_type=pl.DeviceIdType.MESH)

    barrier = pltpu.get_barrier_semaphore()
    peers = [partner] + [shifted(d, by) for d in range(3) if sizes[d] > 1 for by in range(1, sizes[d])]
    for peer in peers:
        pl.semaphore_signal(barrier, inc=1, device_id=peer, device_id_type=pl.DeviceIdType.MESH)
    pl.semaphore_wait(barrier, len(peers))

    row = lax.broadcasted_iota(jnp.int32, (B, B), 0)
    col = lax.broadcasted_iota(jnp.int32, (B, B), 1)
    low, eye = row >= col, row == col

    def blk(i):
        return pl.ds(pl.multiple_of(i * B, B), B)

    def unit_of(c, q):
        u = c * n_chip + q
        i = rem(u, nb)
        return u, i, rem(i + u // nb + 1, nb), u >= 2 * n_chip - nb // 2

    def chip_index(k, coord):
        p = perms[k]
        return (coord[p[0]] * sizes[p[1]] + coord[p[1]]) * sizes[p[2]] + coord[p[2]]

    def coords_of(q):
        return (q // (ny * nz), rem(q // nz, ny), rem(q, nz))

    def split(n, wide):
        if n > 1:
            return (0, n // 2, 0, PIECE), (n // 2, n // 2, 0, PIECE)
        r = 32 if wide else 24
        return (0, 1, 0, r), (0, 1, r, PIECE - r)

    def part_of(ref, lead, base, half):
        return ref.at[lead, pl.ds(base + half[0], half[1]), pl.ds(half[2], half[3])]

    out_ref[...] = theta_ref[...]

    def one_step(step, carry):
        def prep(r, cc):
            rows = pl.ds(pl.multiple_of(r * 256, 256), 256)
            th = out_ref[rows]
            t_own[rows] = th.astype(BF16)
            xb = (th - mu_ref[...]).astype(BF16)
            zt[:, rows] = lax.dot_general(fact_ref[...], xb, NT, preferred_element_type=F32)
            return cc
        lax.fori_loop(0, n_total // 256, prep, 0)
        zh = zt.shape[0] // 2
        ct = copy("t", t_own, t_par, partner)
        cz = copy("z", zt.at[pl.ds(pl.multiple_of((1 - core) * zh, 8), zh)], zt_par, partner)
        ct.start()
        cz.start()
        ct.wait()
        cz.wait()

        def gram(i, j):
            return (lax.dot_general(t_own[blk(i)], t_own[blk(j)], NT, preferred_element_type=F32)
                    + lax.dot_general(t_par[blk(i)], t_par[blk(j)], NT, preferred_element_type=F32))

        def norms(i, cc):
            s = jnp.sum(jnp.where(eye, gram(i, i), 0.0), axis=0, keepdims=True)
            s_all[i] = jnp.broadcast_to(s, (8, B))
            return cc
        lax.fori_loop(0, nb, norms, 0)

        row8 = lax.broadcasted_iota(jnp.int32, (8, B), 0)

        def form(q, cc):
            u, i, j, packed = unit_of(core, q)
            coord = coords_of(q)
            i0, i1, i2 = (chip_index(k, coord) for k in range(3))
            srows = jnp.where(row8 == 0, s_all[i], s_all[j])
            zrow = u // nb
            zb = (zt[pl.ds(pl.multiple_of(zrow * 8, 8), 8), blk(i)]
                  + zt_par[pl.ds(pl.multiple_of(zrow * 8 - core * zh, 8), 8), blk(i)])
            tail = jnp.concatenate([srows, zb], 0)

            def put(m):
                g[0, i0] = m[:48]
                g[1, i1] = m[48:96]
                g[2, i2] = jnp.concatenate([m[96:], tail], 0)

            @pl.when(jnp.logical_not(packed))
            def _():
                put(gram(i, j))

            @pl.when(packed)
            def _():
                put(jnp.where(low, gram(i, i), gram(j, j)))
            return cc
        lax.fori_loop(0, n_chip, form, 0)

        pending = []
        for ph in (0, 1):
            src = (g, acc2)[ph]
            bufs = (ring1, ring2)[ph]
            dstacc = (acc2, acc3)[ph]
            active = []
            for k in range(3):
                p = perms[k]
                d = p[ph]
                n = sizes[p[2]] * (sizes[p[1]] if ph == 0 else 1)
                if sizes[d] == 1:
                    dstacc[k, pl.ds(0, n)] = src[k, pl.ds(0, n)]
                    continue
                base = [rem(me[d] + s, 4) * n for s in range(4)]
                ha, hb = split(n, False)
                key = ("rs", ph, k)
                right, left = shifted(d, 1), shifted(d, 3)
                m1p = copy(key + (0,), part_of(src, k, base[2], ha), bufs.at[k, 0, pl.ds(0, ha[1]), pl.ds(0, ha[3])], right)
                m1m = copy(key + (1,), part_of(src, k, base[2], hb), bufs.at[k, 1, pl.ds(0, hb[1]), pl.ds(0, hb[3])], left)
                m2p = copy(key + (2,), part_of(src, k, base[1], hb), part_of(bufs.at[k], 2, 0, hb), right)
                m2m = copy(key + (3,), part_of(src, k, base[3], ha), part_of(bufs.at[k], 3, 0, ha), left)
                m3p = copy(key + (4,), part_of(src, k, base[1], ha), part_of(bufs.at[k], 2, 0, ha), right)
                m3m = copy(key + (5,), part_of(src, k, base[3], hb), part_of(bufs.at[k], 3, 0, hb), left)
                for m in (m1p, m1m, m2p, m2m):
                    m.start()
                active.append((k, n, base, ha, hb, m1p, m1m, m2p, m2m, m3p, m3m))
            for k, n, base, ha, hb, m1p, m1m, m2p, m2m, m3p, m3m in active:
                m1p.wait_recv()
                part_of(src, k, base[1], ha)[...] += bufs[k, 0, pl.ds(0, ha[1]), pl.ds(0, ha[3])]
                m3p.start()
                m1m.wait_recv()
                part_of(src, k, base[3], hb)[...] += bufs[k, 1, pl.ds(0, hb[1]), pl.ds(0, hb[3])]
                m3m.start()
            for k, n, base, ha, hb, m1p, m1m, m2p, m2m, m3p, m3m in active:
                for m in (m2p, m2m, m3p, m3m):
                    m.wait_recv()

                def add(v, cc):
                    dstacc[k, v] = src[k, base[0] + v] + bufs[k, 2, v] + bufs[k, 3, v]
                    return cc
                lax.fori_loop(0, n, add, 0)
                pending += [m1p, m1m, m2p, m2m, m3p, m3m]
        active = []
        for k in range(3):
            d = perms[k][2]
            if sizes[d] == 1:
                active.append((k, d, []))
                continue
            ms = []
            for by in range(1, 4):
                m = copy(("rs", 2, k, by), acc3.at[k, rem(me[d] + by, 4)], dir3.at[k, by], shifted(d, by))
                m.start()
                ms.append(m)
            active.append((k, d, ms))
            pending += ms
        for k, d, ms in active:
            tot = acc3[k, me[d] if ms else 0]
            for m in ms:
                m.wait_recv()
            for by in range(1, len(ms) + 1):
                tot = tot + dir3[k, by]
            unit[k] = tot

        packed = unit_of(core, (me[0] * ny + me[1]) * nz + me[2])[3]
        first = jnp.logical_or(jnp.logical_not(packed), low)
        second = jnp.logical_or(jnp.logical_not(packed), jnp.logical_not(low))
        g_u = jnp.concatenate([unit[0], unit[1], unit[2, pl.ds(0, 32)]], 0)
        si = jnp.broadcast_to(unit[2, pl.ds(32, 1)], (B, B))
        sj = jnp.broadcast_to(unit[2, pl.ds(33, 1)], (B, B))
        si_c = jnp.broadcast_to(jnp.sum(jnp.where(eye, si, 0.0), axis=1, keepdims=True), (B, B))
        sj_c = jnp.broadcast_to(jnp.sum(jnp.where(eye, sj, 0.0), axis=1, keepdims=True), (B, B))
        s_sum = jnp.where(first, si_c, sj_c) + jnp.where(second, sj, si)
        dist = jnp.maximum(s_sum - 2.0 * g_u, 0.0)
        k_u = jnp.exp(-dist / kern_width)
        z_u = unit[2, pl.ds(40, 8)]
        pieces = (k_u[:48], k_u[48:96], jnp.concatenate([k_u[96:], z_u, jnp.zeros_like(z_u)], 0))
        own = [chip_index(k, me) for k in range(3)]
        for k in range(3):
            ag[k, own[k]] = pieces[k].astype(BF16)

        active = []
        for k in range(3):
            d = perms[k][2]
            if sizes[d] == 1:
                continue
            for by in range(1, 4):
                m = copy(("ag", 2, k, by), ag.at[k, own[k]], ag.at[k, own[k]], shifted(d, by))
                m.start()
                active.append(m)
        for m in active:
            m.wait_recv()
        pending += active
        swaps = []

        def swap(key, ref_of):
            m = copy(("sw",) + key, ref_of(ag), ref_of(ag_par), partner)
            m.start()
            swaps.append(m)

        for ph in (1, 0):
            active = []
            for k in range(3):
                p = perms[k]
                d = p[ph]
                n = sizes[p[2]] * (sizes[p[1]] if ph == 0 else 1)
                top = me[p[0]] * sizes[p[1]] * sizes[p[2]] if ph == 1 else 0
                base = [top + rem(me[d] + s, sizes[d]) * n for s in range(sizes[d])]
                if ph == 0:
                    swap((k, 6), lambda ref: ref.at[k, pl.ds(base[0], n)])
                if sizes[d] == 1:
                    continue
                ha, hb = split(n, True)
                right, left = shifted(d, 1), shifted(d, 3)
                key = ("ag", ph, k)

                def send(tag, b, h, to):
                    return copy(key + (tag,), part_of(ag, k, b, h), part_of(ag, k, b, h), to)
                n1p, n1m = send(0, base[0], ha, right), send(1, base[0], hb, left)
                n2p, n2m = send(2, base[0], hb, right), send(3, base[0], ha, left)
                for m in (n1p, n1m, n2p, n2m):
                    m.start()
                n3p, n3m = send(4, base[3], ha, right), send(5, base[1], hb, left)
                active.append((k, n, base, ha, hb, n1p, n1m, n2p, n2m, n3p, n3m))
            for k, n, base, ha, hb, n1p, n1m, n2p, n2m, n3p, n3m in active:
                n1p.wait_recv()
                n3p.start()
                n1m.wait_recv()
                n3m.start()
                if ph == 0:
                    swap((k, 0), lambda ref: part_of(ref, k, base[3], ha))
                    swap((k, 1), lambda ref: part_of(ref, k, base[1], hb))
            for k, n, base, ha, hb, n1p, n1m, n2p, n2m, n3p, n3m in active:
                got = ((n2p, base[3], hb), (n2m, base[1], ha), (n3p, base[2], ha), (n3m, base[2], hb))
                for t, (m, b, h) in enumerate(got):
                    m.wait_recv()
                    if ph == 0:
                        swap((k, 2 + t), lambda ref: part_of(ref, k, b, h))
                pending += [n1p, n1m, n2p, n2m, n3p, n3m]

        def assemble(ref, c):
            def body(q, cc):
                u, i, j, packed = unit_of(c, q)
                coord = coords_of(q)
                i0, i1, i2 = (chip_index(k, coord) for k in range(3))
                tail = ref[2, i2].astype(F32)
                m = jnp.concatenate([ref[0, i0].astype(F32), ref[1, i1].astype(F32), tail[:32]], 0)
                zt_b[pl.ds(pl.multiple_of(u // nb * 8, 8), 8), blk(i)] = tail[32:40]
                mt = m.T

                @pl.when(jnp.logical_not(packed))
                def _():
                    kfull[blk(i), blk(j)] = m.astype(BF16)
                    kfull[blk(j), blk(i)] = mt.astype(BF16)

                @pl.when(packed)
                def _():
                    kfull[blk(i), blk(i)] = jnp.where(eye, 1.0, jnp.where(low, m, mt)).astype(BF16)
                    kfull[blk(j), blk(j)] = jnp.where(eye, 1.0, jnp.where(low, mt, m)).astype(BF16)
                    zero = jnp.zeros((B, B), BF16)
                return cc
            lax.fori_loop(0, n_chip, body, 0)
        assemble(ag, core)
        for m in swaps:
            m.wait_recv()
        assemble(ag_par, 1 - core)

        def grads(r, cc):
            rows = pl.ds(pl.multiple_of(r * 256, 256), 256)
            lowt = lax.dot_general(zt_b[:, rows].astype(BF16), fact_ref[...], TN, preferred_element_type=F32)
            a_buf[rows] = (-((out_ref[rows] - mu_ref[...]) * lam_ref[...] + lowt)).astype(BF16)
            return cc
        lax.fori_loop(0, n_total // 256, grads, 0)

        def update(r, cc):
            rows = pl.ds(pl.multiple_of(r * 256, 256), 256)
            kr = kfull[rows]
            mass = jnp.sum(kr.astype(F32), axis=1, keepdims=True)
            drive = jnp.dot(kr, a_buf[...], preferred_element_type=F32)
            pull = jnp.dot(kr, t_own[...], preferred_element_type=F32)
            upd = (drive + (2.0 / kern_width) * (mass * t_own[rows].astype(F32) - pull)) / n_total
            out_ref[rows] = out_ref[rows] + step_size * upd
            return cc
        lax.fori_loop(0, n_total // 256, update, 0)
        for m in pending + swaps:
            m.wait_send()
        return carry

    lax.fori_loop(0, NUM_STEPS, one_step, 0)


def run_steps(theta, lam, mu, fac, sizes, kern_width, step_size):
    n_total, fcol = theta.shape
    rank = fac.shape[1]
    nb = n_total // B
    n_chip = sizes[0] * sizes[1] * sizes[2]
    assert nb * nb == 4 * n_chip and rank == 4 * nb
    cfg = dict(sizes=sizes, nb=nb, kern_width=kern_width, step_size=step_size)
    n1, n2 = n_chip, n_chip
    vmem = pl.BlockSpec(memory_space=pltpu.VMEM)
    most1 = max(n_chip // sizes[k] for k in range(3))
    most2 = max(sizes)
    scratch = [
        pltpu.VMEM((n_total, fcol), BF16),
        pltpu.VMEM((n_total, fcol), BF16),
        pltpu.VMEM((n_total, fcol), BF16),
        pltpu.VMEM((rank, n_total), F32),
        pltpu.VMEM((rank // 2, n_total), F32),
        pltpu.VMEM((rank, n_total), F32),
        pltpu.VMEM((nb, 8, B), F32),
        pltpu.VMEM((3, n_chip, PIECE, B), F32),
        pltpu.VMEM((3, 4, most1, PIECE, B), F32),
        pltpu.VMEM((3, 4, most2, PIECE, B), F32),
        pltpu.VMEM((3, 4, PIECE, B), F32),
        pltpu.VMEM((3, most1, PIECE, B), F32),
        pltpu.VMEM((3, most2, PIECE, B), F32),
        pltpu.VMEM((3, PIECE, B), F32),
        pltpu.VMEM((3, n_chip, PIECE, B), BF16),
        pltpu.VMEM((3, n_chip, PIECE, B), BF16),
        pltpu.VMEM((n_total, n_total), BF16),
        pltpu.SemaphoreType.DMA((NUM_SEMS,)),
        pltpu.SemaphoreType.DMA((NUM_SEMS,)),
    ]
    return pl.pallas_call(
        functools.partial(steps_kernel, cfg),
        out_shape=jax.ShapeDtypeStruct(theta.shape, F32),
        in_specs=[vmem] * 5,
        out_specs=vmem,
        scratch_shapes=scratch,
        compiler_params=pltpu.CompilerParams(collective_id=0, has_side_effects=True, vmem_limit_bytes=60 * 1024 * 1024),
        name="svgd_steps",
    )(theta, lam[None], mu[None], fac, fac.T)


def solution(mesh, sizes=(4, 4, 4)):
    part_size = mesh.shape["part"]
    feat_size = mesh.shape["feat"]

    def local_steps(local_theta, prec_loc, mean_loc, factor_loc):
        rows_loc, feat_loc = local_theta.shape
        n_total = rows_loc * part_size
        feat_total = feat_loc * feat_size
        kern_width = 2.0 * feat_total / math.log(n_total)
        step_size = 0.15 * n_total * feat_total / math.log(n_total)
        part_idx = lax.axis_index("part")
        fcol = feat_loc // part_size
        theta = lax.all_to_all(local_theta, "part", split_axis=1, concat_axis=0, tiled=True)
        lam = lax.dynamic_slice_in_dim(prec_loc, part_idx * fcol, fcol)
        mu = lax.dynamic_slice_in_dim(mean_loc, part_idx * fcol, fcol)
        fac = lax.dynamic_slice_in_dim(factor_loc, part_idx * fcol, fcol)
        theta = run_steps(theta, lam, mu, fac, sizes, kern_width, step_size)
        return lax.all_to_all(theta, "part", split_axis=0, concat_axis=1, tiled=True)

    row_spec = P(("ens", "part"), "feat")
    vec_spec = P(("ens", "feat"))
    fac_spec = P(("ens", "feat"), None)
    return jax.shard_map(local_steps, mesh=mesh, in_specs=(row_spec, vec_spec, vec_spec, fac_spec), out_specs=row_spec, check_vma=False)
```

```python
import functools
import math
import jax
import jax.numpy as jnp
from jax import lax
from jax.experimental import pallas as pl
from jax.experimental.pallas import tpu as pltpu
from jax.sharding import PartitionSpec as P

NUM_STEPS = 3
B = 128
PIECE = 48
F32 = jnp.float32
BF16 = jnp.bfloat16
NT = (((1,), (1,)), ((), ()))
TN = (((0,), (0,)), ((), ()))
NUM_SEMS = 160
PANEL = 256


def rem(a, n):
    return lax.rem(a, jnp.int32(n))


def div(a, n):
    return lax.div(a, jnp.int32(n))


def unrolled(count, by, body):
    def several(r, cc):
        for t in range(by):
            body(r * by + t)
        return cc
    lax.fori_loop(0, count // by, several, 0)


def steps_kernel(cfg, theta_ref, lam_ref, mu_ref, fac_ref, fact_ref, out_ref, t_own, t_par, a_buf, zt, zt_par, zt_b,
                 s_all, d_all, g, ring1, ring2, dir3, acc2, acc3, unit, ag, ag_par, kfull, send_sems, recv_sems):
    sizes, nb, kern_width, step_size = cfg["sizes"], cfg["nb"], cfg["kern_width"], cfg["step_size"]
    nx, ny, nz = sizes
    n_total = nb * B
    n_chip = nx * ny * nz
    part, feat = lax.axis_index("part"), lax.axis_index("feat")
    core = rem(feat, 2)
    me = (feat // 2, rem(part, ny), part // ny)

    def dev(coord, c):
        return {"part": coord[2] * ny + coord[1], "feat": coord[0] * 2 + c}

    def shifted(dim, by):
        c = list(me)
        c[dim] = rem(me[dim] + by, sizes[dim])
        return dev(c, core)

    partner = dev(me, 1 - core)
    perms = [(k, (k + 1) % 3, (k + 2) % 3) for k in range(3)]

    ids = {}

    def copy(key, src, dst, to):
        idx = ids.setdefault(key, len(ids))
        assert idx < NUM_SEMS - 8
        return pltpu.make_async_remote_copy(
            src_ref=src, dst_ref=dst, send_sem=send_sems.at[idx], recv_sem=recv_sems.at[idx],
            device_id=to, device_id_type=pl.DeviceIdType.MESH)

    barrier = pltpu.get_barrier_semaphore()
    peers = [partner] + [shifted(d, by) for d in range(3) if sizes[d] > 1 for by in range(1, sizes[d])]
    for peer in peers:
        pl.semaphore_signal(barrier, inc=1, device_id=peer, device_id_type=pl.DeviceIdType.MESH)
    pl.semaphore_wait(barrier, len(peers))

    row = lax.broadcasted_iota(jnp.int32, (B, B), 0)
    col = lax.broadcasted_iota(jnp.int32, (B, B), 1)
    low, eye = row >= col, row == col

    def blk(i):
        return pl.ds(pl.multiple_of(i * B, B), B)

    def unit_of(c, q):
        u = c * n_chip + q
        i = rem(u, nb)
        return u, i, rem(i + div(u, nb) + 1, nb), u >= 2 * n_chip - nb // 2

    def chip_index(k, coord):
        p = perms[k]
        return (coord[p[0]] * sizes[p[1]] + coord[p[1]]) * sizes[p[2]] + coord[p[2]]

    def coords_of(q):
        return (div(q, ny * nz), rem(div(q, nz), ny), rem(q, nz))

    def split(n, wide):
        if n > 1:
            return (0, n // 2, 0, PIECE), (n // 2, n // 2, 0, PIECE)
        r = 32 if wide else 24
        return (0, 1, 0, r), (0, 1, r, PIECE - r)

    def part_of(ref, lead, base, half):
        return ref.at[lead, pl.ds(base + half[0], half[1]), pl.ds(half[2], half[3])]

    zh = zt.shape[0] // 2
    kc = nb // 4
    n_panels = n_total // PANEL

    def panel(r):
        return pl.ds(pl.multiple_of(r * PANEL, PANEL), PANEL)

    def swap_t(r, slot):
        return pltpu.make_async_remote_copy(
            src_ref=t_own.at[slot, panel(r)], dst_ref=t_par.at[panel(r)], send_sem=send_sems.at[NUM_SEMS - 1 - r],
            recv_sem=recv_sems.at[NUM_SEMS - 1 - r], device_id=partner, device_id_type=pl.DeviceIdType.MESH)

    def swap_z():
        return copy("z", zt.at[pl.ds(pl.multiple_of((1 - core) * zh, 8), zh)], zt_par, partner)

    def prepare(r, th, slot):
        t_own[slot, panel(r)] = th.astype(BF16)
        swap_t(r, slot).start()
        xb = (th - mu_ref[...]).astype(BF16)
        zt[:, panel(r)] = lax.dot_general(fact_ref[...], xb, NT, preferred_element_type=F32)

    def first_prep(r, cc):
        th = theta_ref[panel(r)]
        out_ref[panel(r)] = th
        prepare(r, th, 0)
        return cc
    with jax.named_scope("prep"):
        lax.fori_loop(0, n_panels, first_prep, 0)
        swap_z().start()

    def one_step(step, carry):
        slot = rem(step, 2)
        with jax.named_scope("twait"):
            for r in range(n_panels):
                swap_t(r, slot).wait()
            swap_z().wait()

        def products(rows, cols):
            return (lax.dot_general(jnp.concatenate([t_own[slot, r] for r in rows], 0), t_own[slot, cols], NT,
                                    preferred_element_type=F32)
                    + lax.dot_general(jnp.concatenate([t_par[r] for r in rows], 0), t_par[cols], NT,
                                      preferred_element_type=F32))

        def put(m, q):
            coord = coords_of(q)
            g[0, chip_index(0, coord)] = m[:48]
            g[1, chip_index(1, coord)] = m[48:96]
            g[2, chip_index(2, coord), pl.ds(0, 32)] = m[96:]

        def form(h, cc):
            i = h * 2
            cols = pl.ds(pl.multiple_of(i * B, 2 * B), 2 * B)
            dg = products([cols], cols)
            for t in range(2):
                dt = dg[t * B:(t + 1) * B, t * B:(t + 1) * B]
                d_all[i + t] = dt
                s_all[i + t] = jnp.broadcast_to(jnp.sum(jnp.where(eye, dt, 0.0), axis=0, keepdims=True), (8, B))
            m = products([blk(rem(i + core * kc + 1 + t, nb)) for t in range(kc + 1)], cols)
            for t in range(kc + 1):
                if t < kc:
                    put(m[t * B:(t + 1) * B, :B], t * nb + i)
                if t > 0:
                    put(m[t * B:(t + 1) * B, B:], (t - 1) * nb + i + 1)
            return cc
        with jax.named_scope("form"):
            lax.fori_loop(0, nb // 2, form, 0)

        row8 = lax.broadcasted_iota(jnp.int32, (8, B), 0)

        def tails(q):
            u, i, j, packed = unit_of(core, q)
            zrow = div(u, nb) * 8
            at = chip_index(2, coords_of(q))
            g[2, at, pl.ds(32, 8)] = jnp.where(row8 == 0, s_all[j], s_all[i])
            g[2, at, pl.ds(40, 8)] = (zt[pl.ds(pl.multiple_of(zrow, 8), 8), blk(i)]
                                      + zt_par[pl.ds(pl.multiple_of(zrow - core * zh, 8), 8), blk(i)])
        with jax.named_scope("tails"):
            unrolled(n_chip, 4, tails)

            @pl.when(core == 1)
            def _():
                def pair(t, cc):
                    i = t + nb // 2
                    put(jnp.where(low, d_all[i], d_all[t]), n_chip - nb // 2 + t)
                    return cc
                lax.fori_loop(0, nb // 2, pair, 0)

        pending = []
        for ph in (0, 1):
          with jax.named_scope("rs%d" % ph):
            src = (g, acc2)[ph]
            bufs = (ring1, ring2)[ph]
            dstacc = (acc2, acc3)[ph]
            active = []
            for k in range(3):
                p = perms[k]
                d = p[ph]
                n = sizes[p[2]] * (sizes[p[1]] if ph == 0 else 1)
                if sizes[d] == 1:
                    dstacc[k, pl.ds(0, n)] = src[k, pl.ds(0, n)]
                    continue
                base = [rem(me[d] + s, 4) * n for s in range(4)]
                ha, hb = split(n, False)
                key = ("rs", ph, k)
                right, left = shifted(d, 1), shifted(d, 3)
                m1p = copy(key + (0,), part_of(src, k, base[2], ha), bufs.at[k, 0, pl.ds(0, ha[1]), pl.ds(0, ha[3])], right)
                m1m = copy(key + (1,), part_of(src, k, base[2], hb), bufs.at[k, 1, pl.ds(0, hb[1]), pl.ds(0, hb[3])], left)
                m2p = copy(key + (2,), part_of(src, k, base[1], hb), part_of(bufs.at[k], 2, 0, hb), right)
                m2m = copy(key + (3,), part_of(src, k, base[3], ha), part_of(bufs.at[k], 3, 0, ha), left)
                m3p = copy(key + (4,), part_of(src, k, base[1], ha), part_of(bufs.at[k], 2, 0, ha), right)
                m3m = copy(key + (5,), part_of(src, k, base[3], hb), part_of(bufs.at[k], 3, 0, hb), left)
                for m in (m1p, m1m, m2p, m2m):
                    m.start()
                active.append((k, n, base, ha, hb, m1p, m1m, m2p, m2m, m3p, m3m))
            for k, n, base, ha, hb, m1p, m1m, m2p, m2m, m3p, m3m in active:
                m1p.wait_recv()
                part_of(src, k, base[1], ha)[...] += bufs[k, 0, pl.ds(0, ha[1]), pl.ds(0, ha[3])]
                m3p.start()
                m1m.wait_recv()
                part_of(src, k, base[3], hb)[...] += bufs[k, 1, pl.ds(0, hb[1]), pl.ds(0, hb[3])]
                m3m.start()
            for k, n, base, ha, hb, m1p, m1m, m2p, m2m, m3p, m3m in active:
                for m in (m2p, m2m, m3p, m3m):
                    m.wait_recv()

                def add(v, cc):
                    dstacc[k, v] = src[k, base[0] + v] + bufs[k, 2, v] + bufs[k, 3, v]
                    return cc
                lax.fori_loop(0, n, add, 0)
                pending += [m1p, m1m, m2p, m2m, m3p, m3m]
        with jax.named_scope("rs2"):
            active = []
            for k in range(3):
                d = perms[k][2]
                if sizes[d] == 1:
                    active.append((k, d, []))
                    continue
                ms = []
                for by in range(1, 4):
                    m = copy(("rs", 2, k, by), acc3.at[k, rem(me[d] + by, 4)], dir3.at[k, by], shifted(d, by))
                    m.start()
                    ms.append(m)
                active.append((k, d, ms))
                pending += ms
            for k, d, ms in active:
                tot = acc3[k, me[d] if ms else 0]
                for m in ms:
                    m.wait_recv()
                for by in range(1, len(ms) + 1):
                    tot = tot + dir3[k, by]
                unit[k] = tot

        with jax.named_scope("kunit"):
            packed = unit_of(core, (me[0] * ny + me[1]) * nz + me[2])[3]
            g_u = jnp.concatenate([unit[0], unit[1], unit[2, pl.ds(0, 32)]], 0)
            sj = jnp.broadcast_to(unit[2, pl.ds(32, 1)], (B, B))
            si = jnp.broadcast_to(unit[2, pl.ds(33, 1)], (B, B))
            si_c = jnp.broadcast_to(jnp.sum(jnp.where(eye, si, 0.0), axis=1, keepdims=True), (B, B))
            sj_c = jnp.broadcast_to(jnp.sum(jnp.where(eye, sj, 0.0), axis=1, keepdims=True), (B, B))
            lower = jnp.logical_and(packed, low)
            upper = jnp.logical_and(packed, jnp.logical_not(low))
            s_sum = jnp.where(lower, si_c, sj_c) + jnp.where(upper, sj, si)
            dist = jnp.maximum(s_sum - 2.0 * g_u, 0.0)
            k_u = jnp.exp(-dist / kern_width)
            z_u = unit[2, pl.ds(40, 8)]
            pieces = (k_u[:48], k_u[48:96], jnp.concatenate([k_u[96:], z_u, jnp.zeros_like(z_u)], 0))
            own = [chip_index(k, me) for k in range(3)]
            for k in range(3):
                ag[k, own[k]] = pieces[k].astype(BF16)

        with jax.named_scope("ag2"):
            active = []
            for k in range(3):
                d = perms[k][2]
                if sizes[d] == 1:
                    continue
                for by in range(1, 4):
                    m = copy(("ag", 2, k, by), ag.at[k, own[k]], ag.at[k, own[k]], shifted(d, by))
                    m.start()
                    active.append(m)
            for m in active:
                m.wait_recv()
            pending += active
        swaps = []

        def swap(key, ref_of):
            m = copy(("sw",) + key, ref_of(ag), ref_of(ag_par), partner)
            m.start()
            swaps.append(m)

        for ph in (1, 0):
          with jax.named_scope("ag%d" % ph):
            active = []
            for k in range(3):
                p = perms[k]
                d = p[ph]
                n = sizes[p[2]] * (sizes[p[1]] if ph == 0 else 1)
                top = me[p[0]] * sizes[p[1]] * sizes[p[2]] if ph == 1 else 0
                base = [top + rem(me[d] + s, sizes[d]) * n for s in range(sizes[d])]
                if ph == 0:
                    swap((k, 6), lambda ref: ref.at[k, pl.ds(base[0], n)])
                if sizes[d] == 1:
                    continue
                ha, hb = split(n, True)
                right, left = shifted(d, 1), shifted(d, 3)
                key = ("ag", ph, k)

                def send(tag, b, h, to):
                    return copy(key + (tag,), part_of(ag, k, b, h), part_of(ag, k, b, h), to)
                n1p, n1m = send(0, base[0], ha, right), send(1, base[0], hb, left)
                n2p, n2m = send(2, base[0], hb, right), send(3, base[0], ha, left)
                for m in (n1p, n1m, n2p, n2m):
                    m.start()
                n3p, n3m = send(4, base[3], ha, right), send(5, base[1], hb, left)
                active.append((k, n, base, ha, hb, n1p, n1m, n2p, n2m, n3p, n3m))
            for k, n, base, ha, hb, n1p, n1m, n2p, n2m, n3p, n3m in active:
                n1p.wait_recv()
                n3p.start()
                n1m.wait_recv()
                n3m.start()
                if ph == 0:
                    swap((k, 0), lambda ref: part_of(ref, k, base[3], ha))
                    swap((k, 1), lambda ref: part_of(ref, k, base[1], hb))
            for k, n, base, ha, hb, n1p, n1m, n2p, n2m, n3p, n3m in active:
                got = ((n2p, base[3], hb), (n2m, base[1], ha), (n3p, base[2], ha), (n3m, base[2], hb))
                for t, (m, b, h) in enumerate(got):
                    m.wait_recv()
                    if ph == 0:
                        swap((k, 2 + t), lambda ref: part_of(ref, k, b, h))
                pending += [n1p, n1m, n2p, n2m, n3p, n3m]

        def place(ref, c, q):
            u, i, j, packed = unit_of(c, q)
            coord = coords_of(q)
            base = (j + div(u, 2 * n_chip - nb // 2) * (nb // 2)) * B
            for k, n in ((0, 48), (1, 48), (2, 32)):
                kfull[pl.ds(pl.multiple_of(base + 48 * k, 16), n), blk(i)] = ref[k, chip_index(k, coord), pl.ds(0, n)]
            tail = ref[2, chip_index(2, coord), pl.ds(32, 16)].astype(F32)
            zt_b[pl.ds(pl.multiple_of(div(u, nb) * 8, 8), 8), blk(i)] = tail[:8]
        with jax.named_scope("place1"):
            unrolled(n_chip, 4, functools.partial(place, ag, core))
        with jax.named_scope("swapwait"):
            for m in swaps:
                m.wait_recv()
        with jax.named_scope("place2"):
            unrolled(n_chip, 4, functools.partial(place, ag_par, 1 - core))

        per = 4 if nb > 4 else 2

        def mirror(r, cc):
            at = []
            for t in range(per):
                c = div(r * per + t, n_chip)
                u, i, j, packed = unit_of(c, r * per + t - c * n_chip)
                at.append((i, j, kfull[blk(j), blk(i)].T))
            for i, j, m in at:
                kfull[blk(i), blk(j)] = m
            return cc

        def unpack(t, cc):
            i = t + nb // 2
            m = kfull[blk(i), blk(i)].astype(F32)
            mt = m.T
            kfull[blk(i), blk(i)] = jnp.where(eye, 1.0, jnp.where(low, m, mt)).astype(BF16)
            kfull[blk(t), blk(t)] = jnp.where(eye, 1.0, jnp.where(low, mt, m)).astype(BF16)
            return cc
        with jax.named_scope("mirror"):
            lax.fori_loop(0, (2 * n_chip - nb // 2) // per, mirror, 0)
            lax.fori_loop(0, nb // 2, unpack, 0)

        def grads(r, cc):
            lowt = lax.dot_general(zt_b[:, panel(r)].astype(BF16), fact_ref[...], TN, preferred_element_type=F32)
            a_buf[panel(r)] = (-((out_ref[panel(r)] - mu_ref[...]) * lam_ref[...] + lowt)).astype(BF16)
            return cc
        with jax.named_scope("grads"):
            lax.fori_loop(0, n_panels, grads, 0)

        def update(r, cc):
            kr = kfull[panel(r)]
            mass = jnp.sum(kr.astype(F32), axis=1, keepdims=True)
            drive = jnp.dot(kr, a_buf[...], preferred_element_type=F32)
            pull = jnp.dot(kr, t_own[slot], preferred_element_type=F32)
            upd = (drive + (2.0 / kern_width) * (mass * t_own[slot, panel(r)].astype(F32) - pull)) / n_total
            th = out_ref[panel(r)] + step_size * upd
            out_ref[panel(r)] = th

            @pl.when(step < NUM_STEPS - 1)
            def _():
                prepare(r, th, 1 - slot)
            return cc
        with jax.named_scope("update"):
            lax.fori_loop(0, n_panels, update, 0)

            @pl.when(step < NUM_STEPS - 1)
            def _():
                swap_z().start()
        for m in pending + swaps:
            m.wait_send()
        return carry

    lax.fori_loop(0, NUM_STEPS, one_step, 0)


def run_steps(theta, lam, mu, fac, sizes, kern_width, step_size):
    n_total, fcol = theta.shape
    rank = fac.shape[1]
    nb = n_total // B
    n_chip = sizes[0] * sizes[1] * sizes[2]
    assert nb * nb == 4 * n_chip and rank == 4 * nb
    cfg = dict(sizes=sizes, nb=nb, kern_width=kern_width, step_size=step_size)
    n1, n2 = n_chip, n_chip
    vmem = pl.BlockSpec(memory_space=pltpu.VMEM)
    most1 = max(n_chip // sizes[k] for k in range(3))
    most2 = max(sizes)
    scratch = [
        pltpu.VMEM((2, n_total, fcol), BF16),
        pltpu.VMEM((n_total, fcol), BF16),
        pltpu.VMEM((n_total, fcol), BF16),
        pltpu.VMEM((rank, n_total), F32),
        pltpu.VMEM((rank // 2, n_total), F32),
        pltpu.VMEM((rank, n_total), F32),
        pltpu.VMEM((nb, 8, B), F32),
        pltpu.VMEM((nb, B, B), F32),
        pltpu.VMEM((3, n_chip, PIECE, B), F32),
        pltpu.VMEM((3, 4, most1, PIECE, B), F32),
        pltpu.VMEM((3, 4, most2, PIECE, B), F32),
        pltpu.VMEM((3, 4, PIECE, B), F32),
        pltpu.VMEM((3, most1, PIECE, B), F32),
        pltpu.VMEM((3, most2, PIECE, B), F32),
        pltpu.VMEM((3, PIECE, B), F32),
        pltpu.VMEM((3, n_chip, PIECE, B), BF16),
        pltpu.VMEM((3, n_chip, PIECE, B), BF16),
        pltpu.VMEM((n_total, n_total), BF16),
        pltpu.SemaphoreType.DMA((NUM_SEMS,)),
        pltpu.SemaphoreType.DMA((NUM_SEMS,)),
    ]
    return pl.pallas_call(
        functools.partial(steps_kernel, cfg),
        out_shape=jax.ShapeDtypeStruct(theta.shape, F32),
        in_specs=[vmem] * 5,
        out_specs=vmem,
        scratch_shapes=scratch,
        compiler_params=pltpu.CompilerParams(collective_id=0, has_side_effects=True, vmem_limit_bytes=60 * 1024 * 1024),
        name="svgd_steps",
    )(theta, lam[None], mu[None], fac, fac.T)


def solution(mesh, sizes=(4, 4, 4)):
    part_size = mesh.shape["part"]
    feat_size = mesh.shape["feat"]

    def local_steps(local_theta, prec_loc, mean_loc, factor_loc):
        rows_loc, feat_loc = local_theta.shape
        n_total = rows_loc * part_size
        feat_total = feat_loc * feat_size
        kern_width = 2.0 * feat_total / math.log(n_total)
        step_size = 0.15 * n_total * feat_total / math.log(n_total)
        part_idx = lax.axis_index("part")
        fcol = feat_loc // part_size
        theta = lax.all_to_all(local_theta, "part", split_axis=1, concat_axis=0, tiled=True)
        lam = lax.dynamic_slice_in_dim(prec_loc, part_idx * fcol, fcol)
        mu = lax.dynamic_slice_in_dim(mean_loc, part_idx * fcol, fcol)
        fac = lax.dynamic_slice_in_dim(factor_loc, part_idx * fcol, fcol)
        theta = run_steps(theta, lam, mu, fac, sizes, kern_width, step_size)
        return lax.all_to_all(theta, "part", split_axis=0, concat_axis=1, tiled=True)

    row_spec = P(("ens", "part"), "feat")
    vec_spec = P(("ens", "feat"))
    fac_spec = P(("ens", "feat"), None)
    return jax.shard_map(local_steps, mesh=mesh, in_specs=(row_spec, vec_spec, vec_spec, fac_spec), out_specs=row_spec, check_vma=False)
```

```python
import functools
import math
import jax
import jax.numpy as jnp
from jax import lax
from jax.experimental import pallas as pl
from jax.experimental.pallas import tpu as pltpu
from jax.sharding import PartitionSpec as P

NUM_STEPS = 3
B = 128
PIECE = 48
F32 = jnp.float32
BF16 = jnp.bfloat16
NT = (((1,), (1,)), ((), ()))
TN = (((0,), (0,)), ((), ()))
NUM_SEMS = 288
PANEL = 256


def rem(a, n):
    return lax.rem(a, jnp.int32(n))


def div(a, n):
    return lax.div(a, jnp.int32(n))


def unrolled(count, by, body):
    def several(r, cc):
        for t in range(by):
            body(r * by + t)
        return cc
    lax.fori_loop(0, count // by, several, 0)


def steps_kernel(cfg, theta_ref, lam_ref, mu_ref, fac_ref, fact_ref, out_ref, t_own, t_par, a_buf, zt, zt_par, zt_b,
                 s_all, d_all, g, ring1, dirb, dir3, acc2, acc3, unit, ag, ag_par, kfull, send_sems, recv_sems):
    sizes, nb, kern_width, step_size = cfg["sizes"], cfg["nb"], cfg["kern_width"], cfg["step_size"]
    nx, ny, nz = sizes
    n_total = nb * B
    n_chip = nx * ny * nz
    part, feat = lax.axis_index("part"), lax.axis_index("feat")
    core = rem(feat, 2)
    me = (feat // 2, rem(part, ny), part // ny)

    def dev(coord, c):
        return {"part": coord[2] * ny + coord[1], "feat": coord[0] * 2 + c}

    def shifted(dim, by):
        c = list(me)
        c[dim] = rem(me[dim] + by, sizes[dim])
        return dev(c, core)

    partner = dev(me, 1 - core)
    perms = [(k, (k + 1) % 3, (k + 2) % 3) for k in range(3)]

    ids = {}

    def copy(key, src, dst, to):
        idx = ids.setdefault(key, len(ids))
        assert idx < NUM_SEMS - 8
        return pltpu.make_async_remote_copy(
            src_ref=src, dst_ref=dst, send_sem=send_sems.at[idx], recv_sem=recv_sems.at[idx],
            device_id=to, device_id_type=pl.DeviceIdType.MESH)

    barrier = pltpu.get_barrier_semaphore()
    peers = [partner] + [shifted(d, by) for d in range(3) if sizes[d] > 1 for by in range(1, sizes[d])]
    for peer in peers:
        pl.semaphore_signal(barrier, inc=1, device_id=peer, device_id_type=pl.DeviceIdType.MESH)
    pl.semaphore_wait(barrier, len(peers))

    row = lax.broadcasted_iota(jnp.int32, (B, B), 0)
    col = lax.broadcasted_iota(jnp.int32, (B, B), 1)
    low, eye = row >= col, row == col

    def blk(i):
        return pl.ds(pl.multiple_of(i * B, B), B)

    def unit_of(c, q):
        u = c * n_chip + q
        i = rem(u, nb)
        return u, i, rem(i + div(u, nb) + 1, nb), u >= 2 * n_chip - nb // 2

    def chip_index(k, coord):
        p = perms[k]
        return (coord[p[0]] * sizes[p[1]] + coord[p[1]]) * sizes[p[2]] + coord[p[2]]

    def coords_of(q):
        return (div(q, ny * nz), rem(div(q, nz), ny), rem(q, nz))

    def split(n, wide):
        if n > 1:
            return (0, n // 2, 0, PIECE), (n // 2, n // 2, 0, PIECE)
        r = 32 if wide else 24
        return (0, 1, 0, r), (0, 1, r, PIECE - r)

    def part_of(ref, lead, base, half):
        return ref.at[lead, pl.ds(base + half[0], half[1]), pl.ds(half[2], half[3])]

    zh = zt.shape[0] // 2
    kc = nb // 4
    n_panels = n_total // PANEL

    def panel(r):
        return pl.ds(pl.multiple_of(r * PANEL, PANEL), PANEL)

    def swap_t(r, slot):
        return pltpu.make_async_remote_copy(
            src_ref=t_own.at[slot, panel(r)], dst_ref=t_par.at[panel(r)], send_sem=send_sems.at[NUM_SEMS - 1 - r],
            recv_sem=recv_sems.at[NUM_SEMS - 1 - r], device_id=partner, device_id_type=pl.DeviceIdType.MESH)

    def swap_z():
        return copy("z", zt.at[pl.ds(pl.multiple_of((1 - core) * zh, 8), zh)], zt_par, partner)

    def prepare(r, th, slot):
        t_own[slot, panel(r)] = th.astype(BF16)
        swap_t(r, slot).start()
        xb = (th - mu_ref[...]).astype(BF16)
        zt[:, panel(r)] = lax.dot_general(fact_ref[...], xb, NT, preferred_element_type=F32)

    def first_prep(r, cc):
        th = theta_ref[panel(r)]
        out_ref[panel(r)] = th
        prepare(r, th, 0)
        return cc
    with jax.named_scope("prep"):
        lax.fori_loop(0, n_panels, first_prep, 0)
        swap_z().start()

    def one_step(step, carry):
        slot = rem(step, 2)
        with jax.named_scope("twait"):
            for r in range(n_panels):
                swap_t(r, slot).wait()
            swap_z().wait()

        def products(rows, cols):
            return (lax.dot_general(jnp.concatenate([t_own[slot, r] for r in rows], 0), t_own[slot, cols], NT,
                                    preferred_element_type=F32)
                    + lax.dot_general(jnp.concatenate([t_par[r] for r in rows], 0), t_par[cols], NT,
                                      preferred_element_type=F32))

        def put(m, q):
            coord = coords_of(q)
            g[0, chip_index(0, coord)] = m[:48]
            g[1, chip_index(1, coord)] = m[48:96]
            g[2, chip_index(2, coord), pl.ds(0, 32)] = m[96:]

        def form(h, cc):
            i = h * 2
            cols = pl.ds(pl.multiple_of(i * B, 2 * B), 2 * B)
            dg = products([cols], cols)
            for t in range(2):
                dt = dg[t * B:(t + 1) * B, t * B:(t + 1) * B]
                d_all[i + t] = dt
                s_all[i + t] = jnp.broadcast_to(jnp.sum(jnp.where(eye, dt, 0.0), axis=0, keepdims=True), (8, B))
            m = products([blk(rem(i + core * kc + 1 + t, nb)) for t in range(kc + 1)], cols)
            for t in range(kc + 1):
                if t < kc:
                    put(m[t * B:(t + 1) * B, :B], t * nb + i)
                if t > 0:
                    put(m[t * B:(t + 1) * B, B:], (t - 1) * nb + i + 1)
            return cc
        with jax.named_scope("form"):
            lax.fori_loop(0, nb // 2, form, 0)

        row8 = lax.broadcasted_iota(jnp.int32, (8, B), 0)

        def tails(q):
            u, i, j, packed = unit_of(core, q)
            zrow = div(u, nb) * 8
            at = chip_index(2, coords_of(q))
            g[2, at, pl.ds(32, 8)] = jnp.where(row8 == 0, s_all[j], s_all[i])
            g[2, at, pl.ds(40, 8)] = (zt[pl.ds(pl.multiple_of(zrow, 8), 8), blk(i)]
                                      + zt_par[pl.ds(pl.multiple_of(zrow - core * zh, 8), 8), blk(i)])
        with jax.named_scope("tails"):
            unrolled(n_chip, 4, tails)

            @pl.when(core == 1)
            def _():
                def pair(t, cc):
                    i = t + nb // 2
                    put(jnp.where(low, d_all[i], d_all[t]), n_chip - nb // 2 + t)
                    return cc
                lax.fori_loop(0, nb // 2, pair, 0)

        pending = []

        def wave(k, s):
            p = perms[k]
            n = sizes[p[2]]
            order = (2, 1, 3, 0) if sizes[p[1]] > 1 else (0,)
            b = rem(me[p[1]] + order[s], sizes[p[1]])
            base = [(rem(me[p[0]] + t, sizes[p[0]]) * sizes[p[1]] + b) * n for t in range(4)]
            return p, n, order[s], base

        def n_waves(k):
            return sizes[perms[k][1]]

        def ring_copy(k, s, tag):
            p, n, by, base = wave(k, s)
            ha, hb = split(n, False)
            at, half, kind, to = {
                "m1p": (2, ha, 0, 1), "m1m": (2, hb, 1, 3), "m2p": (1, hb, 2, 1), "m2m": (3, ha, 3, 3),
                "m3p": (1, ha, 2, 1), "m3m": (3, hb, 3, 3)}[tag]
            return copy(("rs", k, s, tag), part_of(g, k, base[at], half), part_of(ring1.at[k], kind, s * n, half),
                        shifted(p[0], to))

        def ring_start(s, tags):
            for tag in tags:
                for k in range(3):
                    if s < n_waves(k) and sizes[perms[k][0]] > 1:
                        m = ring_copy(k, s, tag)
                        m.start()
                        pending.append(m)

        def ring_merge(s):
            for k in range(3):
                if s >= n_waves(k) or sizes[perms[k][0]] == 1:
                    continue
                p, n, by, base = wave(k, s)
                ha, hb = split(n, False)
                for got, out, at, half, kind in (("m1p", "m3p", 1, ha, 0), ("m1m", "m3m", 3, hb, 1)):
                    ring_copy(k, s, got).wait_recv()
                    part_of(g, k, base[at], half)[...] += part_of(ring1.at[k], kind, s * n, half)[...]
                    m = ring_copy(k, s, out)
                    m.start()
                    pending.append(m)

        def owner_copy(k, by, s, n):
            return copy(("rb", k, by), acc2.at[k, pl.ds(s * n, n)], dirb.at[k, by], shifted(perms[k][1], by))

        def ring_finish(s):
            for k in range(3):
                if s >= n_waves(k):
                    continue
                p, n, by, base = wave(k, s)
                ringed = sizes[p[0]] > 1
                if ringed:
                    for tag in ("m2p", "m2m", "m3p", "m3m"):
                        ring_copy(k, s, tag).wait_recv()
                for v in range(n):
                    tot = g[k, base[0] + v]
                    if ringed:
                        tot = tot + ring1[k, 2, s * n + v] + ring1[k, 3, s * n + v]
                    acc2[k, s * n + v] = tot
                if by:
                    m = owner_copy(k, by, s, n)
                    m.start()
                    pending.append(m)

        most = max(n_waves(k) for k in range(3))
        with jax.named_scope("rs0"):
            ring_start(0, ("m1p", "m1m", "m2p", "m2m"))
            ring_start(1, ("m1p", "m1m"))
            for s in range(most):
                ring_merge(s)
                ring_start(s + 1, ("m2p", "m2m"))
                ring_start(s + 2, ("m1p", "m1m"))
                if s:
                    ring_finish(s - 1)
            ring_finish(most - 1)
        last = []
        with jax.named_scope("rs1"):
            for k in range(3):
                p = perms[k]
                n = sizes[p[2]]
                s = n_waves(k) - 1
                bys = range(1, sizes[p[1]])
                for by in bys:
                    owner_copy(k, by, 0, n).wait_recv()
                for v in range(n):
                    tot = acc2[k, s * n + v]
                    for by in bys:
                        tot = tot + dirb[k, by, v]
                    acc3[k, v] = tot
                ms = []
                for by in range(1, sizes[p[2]]):
                    m = copy(("rc", k, by), acc3.at[k, rem(me[p[2]] + by, sizes[p[2]])], dir3.at[k, by],
                             shifted(p[2], by))
                    m.start()
                    ms.append(m)
                last.append(ms)
                pending += ms
        with jax.named_scope("rs2"):
            for k in range(3):
                tot = acc3[k, me[perms[k][2]]]
                for m in last[k]:
                    m.wait_recv()
                for by in range(1, len(last[k]) + 1):
                    tot = tot + dir3[k, by]
                unit[k] = tot

        with jax.named_scope("kunit"):
            packed = unit_of(core, (me[0] * ny + me[1]) * nz + me[2])[3]
            g_u = jnp.concatenate([unit[0], unit[1], unit[2, pl.ds(0, 32)]], 0)
            sj = jnp.broadcast_to(unit[2, pl.ds(32, 1)], (B, B))
            si = jnp.broadcast_to(unit[2, pl.ds(33, 1)], (B, B))
            si_c = jnp.broadcast_to(jnp.sum(jnp.where(eye, si, 0.0), axis=1, keepdims=True), (B, B))
            sj_c = jnp.broadcast_to(jnp.sum(jnp.where(eye, sj, 0.0), axis=1, keepdims=True), (B, B))
            lower = jnp.logical_and(packed, low)
            upper = jnp.logical_and(packed, jnp.logical_not(low))
            s_sum = jnp.where(lower, si_c, sj_c) + jnp.where(upper, sj, si)
            dist = jnp.maximum(s_sum - 2.0 * g_u, 0.0)
            k_u = jnp.exp(-dist / kern_width)
            z_u = unit[2, pl.ds(40, 8)]
            pieces = (k_u[:48], k_u[48:96], jnp.concatenate([k_u[96:], z_u, jnp.zeros_like(z_u)], 0))
            own = [chip_index(k, me) for k in range(3)]
            for k in range(3):
                ag[k, own[k]] = pieces[k].astype(BF16)

        def place(ref, c, k, a, b):
            p = perms[k]
            for v in range(sizes[p[2]]):
                coord = [0, 0, 0]
                coord[p[0]], coord[p[1]], coord[p[2]] = a, b, v
                q = (coord[0] * ny + coord[1]) * nz + coord[2]
                u, i, j, packed = unit_of(c, q)
                top = (j + div(u, 2 * n_chip - nb // 2) * (nb // 2)) * B + 48 * k
                at = (a * sizes[p[1]] + b) * sizes[p[2]] + v
                n = (48, 48, 32)[k]
                kfull[pl.ds(pl.multiple_of(top, 16), n), blk(i)] = ref[k, at, pl.ds(0, n)]
                if k == 2:
                    tail = ref[k, at, pl.ds(32, 16)].astype(F32)
                    zt_b[pl.ds(pl.multiple_of(div(u, nb) * 8, 8), 8), blk(i)] = tail[:8]

        def chunk(k, ta, tb):
            p = perms[k]
            a, b = rem(me[p[0]] + ta, sizes[p[0]]), rem(me[p[1]] + tb, sizes[p[1]])
            return a, b, (a * sizes[p[1]] + b) * sizes[p[2]], sizes[p[2]]

        def swap(k, ta, tb):
            a, b, at, n = chunk(k, ta, tb)
            return copy(("sw", k, ta, tb), ag.at[k, pl.ds(at, n)], ag_par.at[k, pl.ds(at, n)], partner)

        swaps = []

        def have(k, ta, tb):
            swap(k, ta, tb).start()
            swaps.append((k, ta, tb))
            a, b, at, n = chunk(k, ta, tb)
            place(ag, core, k, a, b)

        def unit_copy(stage, k, by, tc, start):
            p = perms[k]
            a, b, at, n = chunk(k, 0, 0)
            at = at + rem(me[p[2]] + tc, n)
            m = copy(("u", stage, k, by, tc), ag.at[k, at], ag.at[k, at], shifted(p[stage], by))
            if start:
                m.start()
                pending.append(m)
            return m

        def a_copy(k, tb, tag, start=False):
            p = perms[k]
            ta, h, to = {"n1p": (0, 0, 1), "n1m": (0, 1, 3), "n2p": (0, 1, 1), "n2m": (0, 0, 3), "n3p": (3, 0, 1),
                         "n3m": (1, 1, 3)}[tag]
            a, b, at, n = chunk(k, ta, tb)
            half = split(n, True)[h]
            m = copy(("a", k, tb, tag), part_of(ag, k, at, half), part_of(ag, k, at, half), shifted(p[0], to))
            if start:
                m.start()
                pending.append(m)
            return m

        def a_launch(k, tb):
            if sizes[perms[k][0]] > 1:
                for tag in ("n1p", "n1m", "n2p", "n2m"):
                    a_copy(k, tb, tag, True)
            have(k, 0, tb)

        def a_relay(tb):
            for k in range(3):
                if sizes[perms[k][0]] > 1 and (tb == 0 or sizes[perms[k][1]] > 1):
                    for got, out in (("n1p", "n3p"), ("n1m", "n3m")):
                        a_copy(k, tb, got).wait_recv()
                        a_copy(k, tb, out, True)

        def a_near(tb):
            for k in range(3):
                if sizes[perms[k][0]] > 1 and (tb == 0 or sizes[perms[k][1]] > 1):
                    for got, ta in (("n2p", 3), ("n2m", 1)):
                        a_copy(k, tb, got).wait_recv()
                        have(k, ta, tb)

        def a_far(tb):
            for k in range(3):
                if sizes[perms[k][0]] > 1 and (tb == 0 or sizes[perms[k][1]] > 1):
                    for got in ("n3p", "n3m"):
                        a_copy(k, tb, got).wait_recv()
                    have(k, 2, tb)

        with jax.named_scope("ag2"):
            for k in range(3):
                for by in range(1, sizes[perms[k][2]]):
                    unit_copy(2, k, by, 0, True)
            for k in range(3):
                for by in range(1, sizes[perms[k][1]]):
                    unit_copy(1, k, by, 0, True)
            for k in range(3):
                p = perms[k]
                for by in range(1, sizes[p[2]]):
                    unit_copy(2, k, by, 0, False).wait_recv()
                    for bb in range(1, sizes[p[1]]):
                        unit_copy(1, k, bb, sizes[p[2]] - by, True)
                a_launch(k, 0)

        def b_arrivals(bb):
            for k in range(3):
                p = perms[k]
                if sizes[p[1]] > 1:
                    for tc in range(sizes[p[2]]):
                        unit_copy(1, k, bb, tc, False).wait_recv()
                    a_launch(k, sizes[p[1]] - bb)

        with jax.named_scope("ag1"):
            b_arrivals(1)
            a_relay(0)
            b_arrivals(3)
            a_relay(3)
            b_arrivals(2)
            a_near(0)
            a_relay(1)
            a_near(3)
            a_relay(2)
        with jax.named_scope("ag0"):
            a_far(0)
            a_near(1)
            a_far(3)
            a_near(2)
            a_far(1)
            a_far(2)

        per = 4 if nb > 4 else 2

        def mirror(c, r, cc):
            at = []
            for t in range(per):
                u, i, j, packed = unit_of(c, r * per + t)
                at.append((i, j, kfull[blk(j), blk(i)].T))
            for i, j, m in at:
                kfull[blk(i), blk(j)] = m
            return cc

        def unpack(t, cc):
            i = t + nb // 2
            m = kfull[blk(i), blk(i)].astype(F32)
            mt = m.T
            kfull[blk(i), blk(i)] = jnp.where(eye, 1.0, jnp.where(low, m, mt)).astype(BF16)
            kfull[blk(t), blk(t)] = jnp.where(eye, 1.0, jnp.where(low, mt, m)).astype(BF16)
            return cc
        with jax.named_scope("mirror1"):
            lax.fori_loop(0, div(n_chip - core * (nb // 2), per), functools.partial(mirror, core), 0)
        with jax.named_scope("swapwait"):
            for k, ta, tb in swaps:
                swap(k, ta, tb).wait_recv()
                a, b, at, n = chunk(k, ta, tb)
                place(ag_par, 1 - core, k, a, b)
        with jax.named_scope("mirror2"):
            lax.fori_loop(0, div(n_chip - (1 - core) * (nb // 2), per), functools.partial(mirror, 1 - core), 0)
            lax.fori_loop(0, nb // 2, unpack, 0)

        def grads(r, cc):
            lowt = lax.dot_general(zt_b[:, panel(r)].astype(BF16), fact_ref[...], TN, preferred_element_type=F32)
            a_buf[panel(r)] = (-((out_ref[panel(r)] - mu_ref[...]) * lam_ref[...] + lowt)).astype(BF16)
            return cc
        with jax.named_scope("grads"):
            lax.fori_loop(0, n_panels, grads, 0)

        def update(r, cc):
            kr = kfull[panel(r)]
            mass = jnp.sum(kr.astype(F32), axis=1, keepdims=True)
            drive = jnp.dot(kr, a_buf[...], preferred_element_type=F32)
            pull = jnp.dot(kr, t_own[slot], preferred_element_type=F32)
            upd = (drive + (2.0 / kern_width) * (mass * t_own[slot, panel(r)].astype(F32) - pull)) / n_total
            th = out_ref[panel(r)] + step_size * upd
            out_ref[panel(r)] = th

            @pl.when(step < NUM_STEPS - 1)
            def _():
                prepare(r, th, 1 - slot)
            return cc
        with jax.named_scope("update"):
            lax.fori_loop(0, n_panels, update, 0)

            @pl.when(step < NUM_STEPS - 1)
            def _():
                swap_z().start()
        with jax.named_scope("sendwait"):
            for m in pending:
                m.wait_send()
            for k, ta, tb in swaps:
                swap(k, ta, tb).wait_send()
        return carry

    lax.fori_loop(0, NUM_STEPS, one_step, 0)


def run_steps(theta, lam, mu, fac, sizes, kern_width, step_size):
    n_total, fcol = theta.shape
    rank = fac.shape[1]
    nb = n_total // B
    n_chip = sizes[0] * sizes[1] * sizes[2]
    assert nb * nb == 4 * n_chip and rank == 4 * nb
    cfg = dict(sizes=sizes, nb=nb, kern_width=kern_width, step_size=step_size)
    n1, n2 = n_chip, n_chip
    vmem = pl.BlockSpec(memory_space=pltpu.VMEM)
    most1 = max(n_chip // sizes[k] for k in range(3))
    most2 = max(sizes)
    scratch = [
        pltpu.VMEM((2, n_total, fcol), BF16),
        pltpu.VMEM((n_total, fcol), BF16),
        pltpu.VMEM((n_total, fcol), BF16),
        pltpu.VMEM((rank, n_total), F32),
        pltpu.VMEM((rank // 2, n_total), F32),
        pltpu.VMEM((rank, n_total), F32),
        pltpu.VMEM((nb, 8, B), F32),
        pltpu.VMEM((nb, B, B), F32),
        pltpu.VMEM((3, n_chip, PIECE, B), F32),
        pltpu.VMEM((3, 4, most1, PIECE, B), F32),
        pltpu.VMEM((3, 4, most2, PIECE, B), F32),
        pltpu.VMEM((3, 4, PIECE, B), F32),
        pltpu.VMEM((3, most1, PIECE, B), F32),
        pltpu.VMEM((3, most2, PIECE, B), F32),
        pltpu.VMEM((3, PIECE, B), F32),
        pltpu.VMEM((3, n_chip, PIECE, B), BF16),
        pltpu.VMEM((3, n_chip, PIECE, B), BF16),
        pltpu.VMEM((n_total, n_total), BF16),
        pltpu.SemaphoreType.DMA((NUM_SEMS,)),
        pltpu.SemaphoreType.DMA((NUM_SEMS,)),
    ]
    return pl.pallas_call(
        functools.partial(steps_kernel, cfg),
        out_shape=jax.ShapeDtypeStruct(theta.shape, F32),
        in_specs=[vmem] * 5,
        out_specs=vmem,
        scratch_shapes=scratch,
        compiler_params=pltpu.CompilerParams(collective_id=0, has_side_effects=True, vmem_limit_bytes=60 * 1024 * 1024),
        name="svgd_steps",
    )(theta, lam[None], mu[None], fac, fac.T)


def solution(mesh, sizes=(4, 4, 4)):
    part_size = mesh.shape["part"]
    feat_size = mesh.shape["feat"]

    def local_steps(local_theta, prec_loc, mean_loc, factor_loc):
        rows_loc, feat_loc = local_theta.shape
        n_total = rows_loc * part_size
        feat_total = feat_loc * feat_size
        kern_width = 2.0 * feat_total / math.log(n_total)
        step_size = 0.15 * n_total * feat_total / math.log(n_total)
        part_idx = lax.axis_index("part")
        fcol = feat_loc // part_size
        theta = lax.all_to_all(local_theta, "part", split_axis=1, concat_axis=0, tiled=True)
        lam = lax.dynamic_slice_in_dim(prec_loc, part_idx * fcol, fcol)
        mu = lax.dynamic_slice_in_dim(mean_loc, part_idx * fcol, fcol)
        fac = lax.dynamic_slice_in_dim(factor_loc, part_idx * fcol, fcol)
        theta = run_steps(theta, lam, mu, fac, sizes, kern_width, step_size)
        return lax.all_to_all(theta, "part", split_axis=0, concat_axis=1, tiled=True)

    row_spec = P(("ens", "part"), "feat")
    vec_spec = P(("ens", "feat"))
    fac_spec = P(("ens", "feat"), None)
    return jax.shard_map(local_steps, mesh=mesh, in_specs=(row_spec, vec_spec, vec_spec, fac_spec), out_specs=row_spec, check_vma=False)
```

```python
import functools
import math
import jax
import jax.numpy as jnp
from jax import lax
from jax.experimental import pallas as pl
from jax.experimental.pallas import tpu as pltpu
from jax.sharding import PartitionSpec as P

NUM_STEPS = 3
B = 128
PIECE = 48
F32 = jnp.float32
BF16 = jnp.bfloat16
NT = (((1,), (1,)), ((), ()))
TN = (((0,), (0,)), ((), ()))
NUM_SEMS = 288
MOVE_SEMS = 96
PANEL = 256


def rem(a, n):
    return lax.rem(a, jnp.int32(n))


def div(a, n):
    return lax.div(a, jnp.int32(n))


def unrolled(count, by, body):
    def several(r, cc):
        for t in range(by):
            body(r * by + t)
        return cc
    lax.fori_loop(0, count // by, several, 0)


def steps_kernel(cfg, theta_ref, lam_ref, mu_ref, fac_ref, fact_ref, out_ref, th, t_own, t_par, a_buf, zt, zt_par, zt_b,
                 s_all, d_all, g, ring1, dirb, dir3, acc2, acc3, unit, ag, ag_par, kfull, send_sems, recv_sems):
    sizes, nb, kern_width, step_size = cfg["sizes"], cfg["nb"], cfg["kern_width"], cfg["step_size"]
    nx, ny, nz = sizes
    n_total = nb * B
    n_chip = nx * ny * nz
    part, feat = lax.axis_index("part"), lax.axis_index("feat")
    core = rem(feat, 2)
    me = (feat // 2, rem(part, ny), part // ny)

    def dev(coord, c):
        return {"part": coord[2] * ny + coord[1], "feat": coord[0] * 2 + c}

    def shifted(dim, by):
        c = list(me)
        c[dim] = rem(me[dim] + by, sizes[dim])
        return dev(c, core)

    partner = dev(me, 1 - core)
    perms = [(k, (k + 1) % 3, (k + 2) % 3) for k in range(3)]

    ids = {}

    def copy(key, src, dst, to):
        idx = ids.setdefault(key, len(ids))
        assert idx < NUM_SEMS - 8, idx
        return pltpu.make_async_remote_copy(
            src_ref=src, dst_ref=dst, send_sem=send_sems.at[idx], recv_sem=recv_sems.at[idx],
            device_id=to, device_id_type=pl.DeviceIdType.MESH)

    barrier = pltpu.get_barrier_semaphore()
    peers = [partner] + [shifted(d, by) for d in range(3) if sizes[d] > 1 for by in range(1, sizes[d])]
    for peer in peers:
        pl.semaphore_signal(barrier, inc=1, device_id=peer, device_id_type=pl.DeviceIdType.MESH)
    pl.semaphore_wait(barrier, len(peers))

    row = lax.broadcasted_iota(jnp.int32, (B, B), 0)
    col = lax.broadcasted_iota(jnp.int32, (B, B), 1)
    low, eye = row >= col, row == col

    def blk(i):
        return pl.ds(pl.multiple_of(i * B, B), B)

    def unit_of(c, q):
        u = c * n_chip + q
        i = rem(u, nb)
        return u, i, rem(i + div(u, nb) + 1, nb), u >= 2 * n_chip - nb // 2

    def chip_index(k, coord):
        p = perms[k]
        return (coord[p[0]] * sizes[p[1]] + coord[p[1]]) * sizes[p[2]] + coord[p[2]]

    def coords_of(q):
        return (div(q, ny * nz), rem(div(q, nz), ny), rem(q, nz))

    def split(n, wide):
        if n > 1:
            return (0, n // 2, 0, PIECE), (n // 2, n // 2, 0, PIECE)
        r = 32 if wide else 24
        return (0, 1, 0, r), (0, 1, r, PIECE - r)

    def part_of(ref, lead, base, half):
        return ref.at[lead, pl.ds(base + half[0], half[1]), pl.ds(half[2], half[3])]

    zh = zt.shape[0] // 2
    kc = nb // 4
    n_panels = n_total // PANEL

    def panel(r):
        return pl.ds(pl.multiple_of(r * PANEL, PANEL), PANEL)

    def swap_t(r, slot):
        return pltpu.make_async_remote_copy(
            src_ref=t_own.at[slot, panel(r)], dst_ref=t_par.at[panel(r)], send_sem=send_sems.at[NUM_SEMS - 1 - r],
            recv_sem=recv_sems.at[NUM_SEMS - 1 - r], device_id=partner, device_id_type=pl.DeviceIdType.MESH)

    def swap_z():
        return copy("z", zt.at[pl.ds(pl.multiple_of((1 - core) * zh, 8), zh)], zt_par, partner)

    def prepare(r, theta, slot):
        t_own[slot, panel(r)] = theta.astype(BF16)
        swap_t(r, slot).start()
        xb = (theta - mu_ref[...]).astype(BF16)
        zt[:, panel(r)] = lax.dot_general(fact_ref[...], xb, NT, preferred_element_type=F32)

    def get_rows(r):
        return jnp.concatenate([th[div(r, 2), 2 * rem(r, 2)], th[div(r, 2), 2 * rem(r, 2) + 1]], 0)

    def first_prep(r, cc):
        for v in range(2):
            th[div(r, 2), 2 * rem(r, 2) + v] = theta_ref[div(r, 2), 2 * rem(r, 2) + v]
        prepare(r, get_rows(r), 0)
        return cc
    fcol = fac_ref.shape[0]
    with jax.named_scope("prep"):
        lax.fori_loop(0, n_panels, first_prep, 0)
        swap_z().start()

    def one_step(step, carry):
        slot = rem(step, 2)
        with jax.named_scope("twait"):
            for r in range(n_panels):
                swap_t(r, slot).wait()
            swap_z().wait()

        def products(rows, cols):
            return (lax.dot_general(jnp.concatenate([t_own[slot, r] for r in rows], 0), t_own[slot, cols], NT,
                                    preferred_element_type=F32)
                    + lax.dot_general(jnp.concatenate([t_par[r] for r in rows], 0), t_par[cols], NT,
                                      preferred_element_type=F32))

        def put(m, q):
            coord = coords_of(q)
            g[0, chip_index(0, coord)] = m[:48]
            g[1, chip_index(1, coord)] = m[48:96]
            g[2, chip_index(2, coord), pl.ds(0, 32)] = m[96:]

        def form(h, cc):
            i = h * 2
            cols = pl.ds(pl.multiple_of(i * B, 2 * B), 2 * B)
            dg = products([cols], cols)
            for t in range(2):
                dt = dg[t * B:(t + 1) * B, t * B:(t + 1) * B]
                d_all[i + t] = dt
                s_all[i + t] = jnp.broadcast_to(jnp.sum(jnp.where(eye, dt, 0.0), axis=0, keepdims=True), (8, B))
            m = products([blk(rem(i + core * kc + 1 + t, nb)) for t in range(kc + 1)], cols)
            for t in range(kc + 1):
                if t < kc:
                    put(m[t * B:(t + 1) * B, :B], t * nb + i)
                if t > 0:
                    put(m[t * B:(t + 1) * B, B:], (t - 1) * nb + i + 1)
            return cc
        with jax.named_scope("form"):
            lax.fori_loop(0, nb // 2, form, 0)

        row8 = lax.broadcasted_iota(jnp.int32, (8, B), 0)

        def tails(q):
            u, i, j, packed = unit_of(core, q)
            zrow = div(u, nb) * 8
            at = chip_index(2, coords_of(q))
            g[2, at, pl.ds(32, 8)] = jnp.where(row8 == 0, s_all[j], s_all[i])
            g[2, at, pl.ds(40, 8)] = (zt[pl.ds(pl.multiple_of(zrow, 8), 8), blk(i)]
                                      + zt_par[pl.ds(pl.multiple_of(zrow - core * zh, 8), 8), blk(i)])
        with jax.named_scope("tails"):
            unrolled(n_chip, 4, tails)

            @pl.when(core == 1)
            def _():
                def pair(t, cc):
                    i = t + nb // 2
                    put(jnp.where(low, d_all[i], d_all[t]), n_chip - nb // 2 + t)
                    return cc
                lax.fori_loop(0, nb // 2, pair, 0)

        pending = []

        def wave(k, s):
            p = perms[k]
            n = sizes[p[2]]
            order = (2, 1, 3, 0) if sizes[p[1]] > 1 else (0,)
            b = rem(me[p[1]] + order[s], sizes[p[1]])
            base = [(rem(me[p[0]] + t, sizes[p[0]]) * sizes[p[1]] + b) * n for t in range(4)]
            return p, n, order[s], base

        def n_waves(k):
            return sizes[perms[k][1]]

        def ring_copy(k, s, tag):
            p, n, by, base = wave(k, s)
            ha, hb = split(n, False)
            at, half, kind, to = {
                "m1p": (2, ha, 0, 1), "m1m": (2, hb, 1, 3), "m2p": (1, hb, 2, 1), "m2m": (3, ha, 3, 3),
                "m3p": (1, ha, 2, 1), "m3m": (3, hb, 3, 3)}[tag]
            return copy(("rs", k, s, tag), part_of(g, k, base[at], half), part_of(ring1.at[k], kind, s * n, half),
                        shifted(p[0], to))

        def ring_start(s, tags):
            for tag in tags:
                for k in range(3):
                    if s < n_waves(k) and sizes[perms[k][0]] > 1:
                        m = ring_copy(k, s, tag)
                        m.start()
                        pending.append(m)

        def ring_merge(s):
            for k in range(3):
                if s >= n_waves(k) or sizes[perms[k][0]] == 1:
                    continue
                p, n, by, base = wave(k, s)
                ha, hb = split(n, False)
                for got, out, at, half, kind in (("m1p", "m3p", 1, ha, 0), ("m1m", "m3m", 3, hb, 1)):
                    ring_copy(k, s, got).wait_recv()
                    part_of(g, k, base[at], half)[...] += part_of(ring1.at[k], kind, s * n, half)[...]
                    m = ring_copy(k, s, out)
                    m.start()
                    pending.append(m)

        def owner_copy(k, by, s, n):
            return copy(("rb", k, by), acc2.at[k, pl.ds(s * n, n)], dirb.at[k, by], shifted(perms[k][1], by))

        def ring_finish(s):
            for k in range(3):
                if s >= n_waves(k):
                    continue
                p, n, by, base = wave(k, s)
                ringed = sizes[p[0]] > 1
                if ringed:
                    for tag in ("m2p", "m2m", "m3p", "m3m"):
                        ring_copy(k, s, tag).wait_recv()
                for v in range(n):
                    tot = g[k, base[0] + v]
                    if ringed:
                        tot = tot + ring1[k, 2, s * n + v] + ring1[k, 3, s * n + v]
                    acc2[k, s * n + v] = tot
                if by:
                    m = owner_copy(k, by, s, n)
                    m.start()
                    pending.append(m)

        most = max(n_waves(k) for k in range(3))
        with jax.named_scope("rs0"):
            ring_start(0, ("m1p", "m1m", "m2p", "m2m"))
            ring_start(1, ("m1p", "m1m"))
            for s in range(most):
                ring_merge(s)
                ring_start(s + 1, ("m2p", "m2m"))
                ring_start(s + 2, ("m1p", "m1m"))
                if s:
                    ring_finish(s - 1)
            ring_finish(most - 1)
        last = []
        with jax.named_scope("rs1"):
            for k in range(3):
                p = perms[k]
                n = sizes[p[2]]
                s = n_waves(k) - 1
                bys = range(1, sizes[p[1]])
                for by in bys:
                    owner_copy(k, by, 0, n).wait_recv()
                for v in range(n):
                    tot = acc2[k, s * n + v]
                    for by in bys:
                        tot = tot + dirb[k, by, v]
                    acc3[k, v] = tot
                ms = []
                for by in range(1, sizes[p[2]]):
                    m = copy(("rc", k, by), acc3.at[k, rem(me[p[2]] + by, sizes[p[2]])], dir3.at[k, by],
                             shifted(p[2], by))
                    m.start()
                    ms.append(m)
                last.append(ms)
                pending += ms
        with jax.named_scope("rs2"):
            for k in range(3):
                tot = acc3[k, me[perms[k][2]]]
                for m in last[k]:
                    m.wait_recv()
                for by in range(1, len(last[k]) + 1):
                    tot = tot + dir3[k, by]
                unit[k] = tot

        with jax.named_scope("kunit"):
            packed = unit_of(core, (me[0] * ny + me[1]) * nz + me[2])[3]
            g_u = jnp.concatenate([unit[0], unit[1], unit[2, pl.ds(0, 32)]], 0)
            sj = jnp.broadcast_to(unit[2, pl.ds(32, 1)], (B, B))
            si = jnp.broadcast_to(unit[2, pl.ds(33, 1)], (B, B))
            si_c = jnp.broadcast_to(jnp.sum(jnp.where(eye, si, 0.0), axis=1, keepdims=True), (B, B))
            sj_c = jnp.broadcast_to(jnp.sum(jnp.where(eye, sj, 0.0), axis=1, keepdims=True), (B, B))
            lower = jnp.logical_and(packed, low)
            upper = jnp.logical_and(packed, jnp.logical_not(low))
            s_sum = jnp.where(lower, si_c, sj_c) + jnp.where(upper, sj, si)
            dist = jnp.maximum(s_sum - 2.0 * g_u, 0.0)
            k_u = jnp.exp(-dist / kern_width)
            z_u = unit[2, pl.ds(40, 8)]
            pieces = (k_u[:48], k_u[48:96], jnp.concatenate([k_u[96:], z_u, jnp.zeros_like(z_u)], 0))
            own = [chip_index(k, me) for k in range(3)]
            for k in range(3):
                ag[k, own[k]] = pieces[k].astype(BF16)

        def place(ref, c, k, a, b):
            p = perms[k]
            for v in range(sizes[p[2]]):
                coord = [0, 0, 0]
                coord[p[0]], coord[p[1]], coord[p[2]] = a, b, v
                q = (coord[0] * ny + coord[1]) * nz + coord[2]
                u, i, j, packed = unit_of(c, q)
                top = (j + div(u, 2 * n_chip - nb // 2) * (nb // 2)) * B + 48 * k
                at = (a * sizes[p[1]] + b) * sizes[p[2]] + v
                n = (48, 48, 32)[k]
                kfull[pl.ds(pl.multiple_of(top, 16), n), blk(i)] = ref[k, at, pl.ds(0, n)]
                if k == 2:
                    tail = ref[k, at, pl.ds(32, 16)].astype(F32)
                    zt_b[pl.ds(pl.multiple_of(div(u, nb) * 8, 8), 8), blk(i)] = tail[:8]

        def chunk(k, ta, tb):
            p = perms[k]
            a, b = rem(me[p[0]] + ta, sizes[p[0]]), rem(me[p[1]] + tb, sizes[p[1]])
            return a, b, (a * sizes[p[1]] + b) * sizes[p[2]], sizes[p[2]]

        def swap(k, ta, tb):
            a, b, at, n = chunk(k, ta, tb)
            return copy(("sw", k, ta, tb), ag.at[k, pl.ds(at, n)], ag_par.at[k, pl.ds(at, n)], partner)

        swaps = []

        def have(k, ta, tb):
            swap(k, ta, tb).start()
            swaps.append((k, ta, tb))
            a, b, at, n = chunk(k, ta, tb)
            place(ag, core, k, a, b)

        def unit_copy(stage, k, by, tc, start):
            p = perms[k]
            a, b, at, n = chunk(k, 0, 0)
            at = at + rem(me[p[2]] + tc, n)
            m = copy(("u", stage, k, by, tc), ag.at[k, at], ag.at[k, at], shifted(p[stage], by))
            if start:
                m.start()
                pending.append(m)
            return m

        def a_copy(k, tb, tag, start=False):
            p = perms[k]
            ta, h, to = {"n1p": (0, 0, 1), "n1m": (0, 1, 3), "n2p": (0, 1, 1), "n2m": (0, 0, 3), "n3p": (3, 0, 1),
                         "n3m": (1, 1, 3)}[tag]
            a, b, at, n = chunk(k, ta, tb)
            half = split(n, True)[h]
            m = copy(("a", k, tb, tag), part_of(ag, k, at, half), part_of(ag, k, at, half), shifted(p[0], to))
            if start:
                m.start()
                pending.append(m)
            return m

        def a_launch(k, tb):
            if sizes[perms[k][0]] > 1:
                for tag in ("n1p", "n1m", "n2p", "n2m"):
                    a_copy(k, tb, tag, True)
            have(k, 0, tb)

        def a_relay(tb):
            for k in range(3):
                if sizes[perms[k][0]] > 1 and (tb == 0 or sizes[perms[k][1]] > 1):
                    for got, out in (("n1p", "n3p"), ("n1m", "n3m")):
                        a_copy(k, tb, got).wait_recv()
                        a_copy(k, tb, out, True)

        def a_near(tb):
            for k in range(3):
                if sizes[perms[k][0]] > 1 and (tb == 0 or sizes[perms[k][1]] > 1):
                    for got, ta in (("n2p", 3), ("n2m", 1)):
                        a_copy(k, tb, got).wait_recv()
                        have(k, ta, tb)

        def a_far(tb):
            for k in range(3):
                if sizes[perms[k][0]] > 1 and (tb == 0 or sizes[perms[k][1]] > 1):
                    for got in ("n3p", "n3m"):
                        a_copy(k, tb, got).wait_recv()
                    have(k, 2, tb)

        with jax.named_scope("ag2"):
            for k in range(3):
                for by in range(1, sizes[perms[k][2]]):
                    unit_copy(2, k, by, 0, True)
            for k in range(3):
                for by in range(1, sizes[perms[k][1]]):
                    unit_copy(1, k, by, 0, True)
            for k in range(3):
                p = perms[k]
                for by in range(1, sizes[p[2]]):
                    unit_copy(2, k, by, 0, False).wait_recv()
                    for bb in range(1, sizes[p[1]]):
                        unit_copy(1, k, bb, sizes[p[2]] - by, True)
                a_launch(k, 0)

        def b_arrivals(bb):
            for k in range(3):
                p = perms[k]
                if sizes[p[1]] > 1:
                    for tc in range(sizes[p[2]]):
                        unit_copy(1, k, bb, tc, False).wait_recv()
                    a_launch(k, sizes[p[1]] - bb)

        with jax.named_scope("ag1"):
            b_arrivals(1)
            a_relay(0)
            b_arrivals(3)
            a_relay(3)
            b_arrivals(2)
            a_near(0)
            a_relay(1)
            a_near(3)
            a_relay(2)
        with jax.named_scope("ag0"):
            a_far(0)
            a_near(1)
            a_far(3)
            a_near(2)
            a_far(1)
            a_far(2)

        per = 4 if nb > 4 else 2

        def mirror(c, r, cc):
            at = []
            for t in range(per):
                u, i, j, packed = unit_of(c, r * per + t)
                at.append((i, j, kfull[blk(j), blk(i)].T))
            for i, j, m in at:
                kfull[blk(i), blk(j)] = m
            return cc

        def unpack(t, cc):
            i = t + nb // 2
            m = kfull[blk(i), blk(i)].astype(F32)
            mt = m.T
            kfull[blk(i), blk(i)] = jnp.where(eye, 1.0, jnp.where(low, m, mt)).astype(BF16)
            kfull[blk(t), blk(t)] = jnp.where(eye, 1.0, jnp.where(low, mt, m)).astype(BF16)
            return cc
        with jax.named_scope("mirror1"):
            lax.fori_loop(0, div(n_chip - core * (nb // 2), per), functools.partial(mirror, core), 0)
        with jax.named_scope("swapwait"):
            for k, ta, tb in swaps:
                swap(k, ta, tb).wait_recv()
                a, b, at, n = chunk(k, ta, tb)
                place(ag_par, 1 - core, k, a, b)
        with jax.named_scope("mirror2"):
            lax.fori_loop(0, div(n_chip - (1 - core) * (nb // 2), per), functools.partial(mirror, 1 - core), 0)
            lax.fori_loop(0, nb // 2, unpack, 0)

        def grads(r, cc):
            lowt = lax.dot_general(zt_b[:, panel(r)].astype(BF16), fact_ref[...], TN, preferred_element_type=F32)
            a_buf[panel(r)] = (-((get_rows(r) - mu_ref[...]) * lam_ref[...] + lowt)).astype(BF16)
            return cc
        with jax.named_scope("grads"):
            lax.fori_loop(0, n_panels, grads, 0)

        def update(r, cc):
            kr = kfull[panel(r)]
            mass = jnp.sum(kr.astype(F32), axis=1, keepdims=True)
            drive = jnp.dot(kr, a_buf[...], preferred_element_type=F32)
            pull = jnp.dot(kr, t_own[slot], preferred_element_type=F32)
            upd = (drive + (2.0 / kern_width) * (mass * t_own[slot, panel(r)].astype(F32) - pull)) / n_total
            theta = get_rows(r) + step_size * upd
            for v in range(2):
                th[div(r, 2), 2 * rem(r, 2) + v] = theta[v * B:(v + 1) * B]

            @pl.when(step < NUM_STEPS - 1)
            def _():
                prepare(r, theta, 1 - slot)
            return cc
        with jax.named_scope("update"):
            lax.fori_loop(0, n_panels, update, 0)

            @pl.when(step < NUM_STEPS - 1)
            def _():
                swap_z().start()
        with jax.named_scope("sendwait"):
            for m in pending:
                m.wait_send()
            for k, ta, tb in swaps:
                swap(k, ta, tb).wait_send()
        return carry

    lax.fori_loop(0, NUM_STEPS, one_step, 0)

    with jax.named_scope("finish"):
        out_ref[...] = th[...]


def mover(cfg, fcol, send_sems, recv_sems):
    nx, ny, nz = cfg["sizes"]
    part, feat = lax.axis_index("part"), lax.axis_index("feat")
    me = (div(feat, 2), rem(part, ny), div(part, ny))
    ids = {}

    def shifted(dim, by):
        c = list(me)
        c[dim] = rem(me[dim] + by, 4)
        return {"part": c[2] * ny + c[1], "feat": feat}

    def copy(key, src, dst, to):
        idx = ids.setdefault(key, len(ids))
        assert idx < MOVE_SEMS
        return pltpu.make_async_remote_copy(
            src_ref=src, dst_ref=dst, send_sem=send_sems.at[idx], recv_sem=recv_sems.at[idx],
            device_id=to, device_id_type=pl.DeviceIdType.MESH)

    barrier = pltpu.get_barrier_semaphore()
    for d in (1, 2):
        for by in (1, 3):
            pl.semaphore_signal(barrier, inc=1, device_id=shifted(d, by), device_id_type=pl.DeviceIdType.MESH)
    pl.semaphore_wait(barrier, 4)

    my = pl.ds(pl.multiple_of((me[1] * nz + me[2]) * fcol, fcol), fcol)

    def cols(y, z, n=1):
        return pl.ds(pl.multiple_of((y * nz + z) * fcol, fcol), n * fcol)

    def side(d, by):
        return rem(me[d] + by, 4)

    def relayed(key, d, sends):
        def copies(tag):
            return [copy((key, tag, t), src, dst, shifted(d, 1 if tag[1] == "+" else 3))
                    for t, (src, dst) in enumerate(sends(tag))]
        started = []

        def go(tags):
            for tag in tags:
                for m in copies(tag):
                    m.start()
                    started.append(m)

        def relay():
            for got, out in (("r+", "f+"), ("r-", "f-")):
                for m in copies(got):
                    m.wait_recv()
                go((out,))

        def finish():
            for tag in ("d+", "d-", "f+", "f-"):
                for m in copies(tag):
                    m.wait_recv()
        go(("r+", "r-", "d+", "d-"))
        return relay, finish, started

    def halves(tag):
        if tag[0] == "d":
            return (0, 1, 2, 3)
        return (0, 1) if tag[1] == "+" else (2, 3)

    return me, my, cols, side, relayed, halves


def mine(ref, h, v, src_at):
    hb = B // 2
    return ref.at[src_at, v, pl.ds(0, hb)] if h == 0 else ref.at[v, src_at, pl.ds(hb, hb)]


def in_kernel(cfg, theta_ref, lam_all, mu_all, fac_all, out_ref, lam_ref, mu_ref, fac_ref, fact_ref, th, l1, rel1, rel2,
              send_sems, recv_sems):
    fcol, hb = fac_ref.shape[0], B // 2
    nx, ny, nz = cfg["sizes"]
    me, my, cols, side, relayed, halves = mover(cfg, fcol, send_sems, recv_sems)

    def in_first(h):
        d = 1 + h

        def sends(tag):
            r0, nr = {"r+": (0, hb // 2), "r-": (hb // 2, hb // 2)}.get(tag, (0, hb))
            way = tag[1] == "+"
            if tag[0] == "f":
                b = 0 if way else 1
                return [(rel1.at[h, b], l1.at[h, side(d, 3 if way else 1), pl.ds(b * (hb // 2), hb // 2)])]
            to = side(d, {"r": 2, "d": 1 if way else 3}[tag[0]])
            rows = pl.ds(h * hb + r0, nr)

            def dst(y, n):
                at = pl.ds(y * fcol, n * fcol)
                if tag[0] == "d":
                    return l1.at[h, me[d], pl.ds(0, nr), at]
                return rel1.at[h, 0 if way else 1, pl.ds(0, nr), at]
            if h == 0:
                return [(theta_ref.at[rows, cols(to, 0, 4)], dst(0, 4))]
            return [(theta_ref.at[rows, cols(y, to)], dst(y, 1)) for y in range(4)]
        return relayed(("in1", h), d, sends)

    def in_second(h):
        d = 2 - h

        def sends(tag):
            way = tag[1] == "+"
            b = 0 if way else 1
            if tag[0] == "f":
                return [(rel2.at[h, b, v % 2], mine(th, h, v, side(d, 3 if way else 1))) for v in halves(tag)]
            to = side(d, {"r": 2, "d": 1 if way else 3}[tag[0]])
            at = pl.ds(pl.multiple_of(to * fcol, fcol), fcol)
            return [(l1.at[h, v, pl.ds(0, hb), at], mine(th, h, v, me[d]) if tag[0] == "d" else rel2.at[h, b, v % 2])
                    for v in halves(tag)]
        return relayed(("in2", h), d, sends)

    with jax.named_scope("in1"):
        fac_ref[...] = fac_all[my]
        first = [in_first(h) for h in range(2)]
        lam_ref[...] = lam_all[pl.ds(0, 1), my]
        mu_ref[...] = mu_all[pl.ds(0, 1), my]
        fact_ref[...] = fac_ref[...].astype(F32).T.astype(BF16)
        l1[0, me[1]] = theta_ref[pl.ds(0, hb), cols(me[1], 0, 4)]
        for y in range(4):
            l1[1, me[2], pl.ds(0, hb), pl.ds(y * fcol, fcol)] = theta_ref[pl.ds(hb, hb), cols(y, me[2])]
        for relay, finish, started in first:
            relay()
    with jax.named_scope("in2"):
        second = []
        for h, (relay, finish, started) in enumerate(first):
            finish()
            second.append(in_second(h))
        for v in range(4):
            th[me[2], v, pl.ds(0, hb)] = l1[0, v, pl.ds(0, hb), pl.ds(pl.multiple_of(me[2] * fcol, fcol), fcol)]
            th[v, me[1], pl.ds(hb, hb)] = l1[1, v, pl.ds(0, hb), pl.ds(pl.multiple_of(me[1] * fcol, fcol), fcol)]
        for relay, finish, started in second:
            relay()
        for relay, finish, started in second:
            finish()
        for relay, finish, started in first + second:
            for m in started:
                m.wait_send()
    out_ref[...] = th[...]


def out_kernel(cfg, th, out_ref, land, m1, rel2, rel3, send_sems, recv_sems):
    fcol, hb = th.shape[3], B // 2
    nx, ny, nz = cfg["sizes"]
    me, my, cols, side, relayed, halves = mover(cfg, fcol, send_sems, recv_sems)

    def out_first(h):
        d = 2 - h

        def sends(tag):
            way = tag[1] == "+"
            b = 0 if way else 1
            if tag[0] == "f":
                return [(rel2.at[h, b, v % 2], m1.at[h, side(d, 3 if way else 1), v]) for v in halves(tag)]
            to = side(d, {"r": 2, "d": 1 if way else 3}[tag[0]])
            return [(mine(th, h, v, to), m1.at[h, me[d], v] if tag[0] == "d" else rel2.at[h, b, v % 2])
                    for v in halves(tag)]
        return relayed(("out1", h), d, sends)

    def out_second(h):
        d = 1 + h

        def place_of(src_at, v):
            return land.at[pl.ds(h * hb, hb), cols(src_at, v) if h == 0 else cols(v, src_at)]

        def sends(tag):
            way = tag[1] == "+"
            b = 0 if way else 1
            if tag[0] == "f":
                return [(rel3.at[h, b, t], place_of(side(d, 3 if way else 1), 2 * b + t)) for t in range(2)]
            to = side(d, {"r": 2, "d": 1 if way else 3}[tag[0]])
            if tag[0] == "r":
                return [(m1.at[h, v, to], rel3.at[h, b, v % 2]) for v in halves(tag)]
            return [(m1.at[h, v, to], place_of(me[d], v)) for v in range(4)]
        return relayed(("out2", h), d, sends)

    with jax.named_scope("out1"):
        first = [out_first(h) for h in range(2)]
        for v in range(4):
            m1[0, me[2], v] = th[me[2], v, pl.ds(0, hb)]
            m1[1, me[1], v] = th[v, me[1], pl.ds(hb, hb)]
        for relay, finish, started in first:
            relay()
    with jax.named_scope("out2"):
        second = []
        for h, (relay, finish, started) in enumerate(first):
            finish()
            second.append(out_second(h))
        for v in range(4):
            land[pl.ds(0, hb), cols(me[1], v)] = m1[0, v, me[1]]
            land[pl.ds(hb, hb), cols(v, me[2])] = m1[1, v, me[2]]
        for relay, finish, started in second:
            relay()
        for relay, finish, started in second:
            finish()
        for relay, finish, started in first + second:
            for m in started:
                m.wait_send()
    out_ref[...] = land[...]


def run_steps(theta, lam, mu, fac, sizes, kern_width, step_size):
    n_total, fcol = theta.shape[0] * sizes[1] * sizes[2], theta.shape[1] // (sizes[1] * sizes[2])
    rank = fac.shape[1]
    nb = n_total // B
    n_chip = sizes[0] * sizes[1] * sizes[2]
    assert nb * nb == 4 * n_chip and rank == 4 * nb
    hb = B // 2
    cfg = dict(sizes=sizes, nb=nb, kern_width=kern_width, step_size=step_size)
    n1, n2 = n_chip, n_chip
    vmem = pl.BlockSpec(memory_space=pltpu.VMEM)
    most1 = max(n_chip // sizes[k] for k in range(3))
    most2 = max(sizes)
    params = dict(has_side_effects=True, vmem_limit_bytes=60 * 1024 * 1024)
    blocks = (4, 4, B, fcol)
    move_sems = [pltpu.SemaphoreType.DMA((MOVE_SEMS,)), pltpu.SemaphoreType.DMA((MOVE_SEMS,))]
    th, lam, mu, fac, fact = pl.pallas_call(
        functools.partial(in_kernel, cfg),
        out_shape=[jax.ShapeDtypeStruct(blocks, F32), jax.ShapeDtypeStruct((1, fcol), F32),
                   jax.ShapeDtypeStruct((1, fcol), F32), jax.ShapeDtypeStruct((fcol, rank), BF16),
                   jax.ShapeDtypeStruct((rank, fcol), BF16)],
        in_specs=[vmem] * 4,
        out_specs=[vmem] * 5,
        scratch_shapes=[
            pltpu.VMEM(blocks, F32),
            pltpu.VMEM((2, 4, hb, 4 * fcol), F32),
            pltpu.VMEM((2, 2, hb // 2, 4 * fcol), F32),
            pltpu.VMEM((2, 2, 2, hb, fcol), F32),
        ] + move_sems,
        compiler_params=pltpu.CompilerParams(collective_id=1, **params),
        name="particles_in",
    )(theta, lam[None], mu[None], fac)
    scratch = [
        pltpu.VMEM(blocks, F32),
        pltpu.VMEM((2, n_total, fcol), BF16),
        pltpu.VMEM((n_total, fcol), BF16),
        pltpu.VMEM((n_total, fcol), BF16),
        pltpu.VMEM((rank, n_total), F32),
        pltpu.VMEM((rank // 2, n_total), F32),
        pltpu.VMEM((rank, n_total), F32),
        pltpu.VMEM((nb, 8, B), F32),
        pltpu.VMEM((nb, B, B), F32),
        pltpu.VMEM((3, n_chip, PIECE, B), F32),
        pltpu.VMEM((3, 4, most1, PIECE, B), F32),
        pltpu.VMEM((3, 4, most2, PIECE, B), F32),
        pltpu.VMEM((3, 4, PIECE, B), F32),
        pltpu.VMEM((3, most1, PIECE, B), F32),
        pltpu.VMEM((3, most2, PIECE, B), F32),
        pltpu.VMEM((3, PIECE, B), F32),
        pltpu.VMEM((3, n_chip, PIECE, B), BF16),
        pltpu.VMEM((3, n_chip, PIECE, B), BF16),
        pltpu.VMEM((n_total, n_total), BF16),
        pltpu.SemaphoreType.DMA((NUM_SEMS,)),
        pltpu.SemaphoreType.DMA((NUM_SEMS,)),
    ]
    th = pl.pallas_call(
        functools.partial(steps_kernel, cfg),
        out_shape=jax.ShapeDtypeStruct(blocks, F32),
        in_specs=[vmem] * 5,
        out_specs=vmem,
        scratch_shapes=scratch,
        compiler_params=pltpu.CompilerParams(collective_id=0, **params),
        name="svgd_steps",
    )(th, lam, mu, fac, fact)
    return pl.pallas_call(
        functools.partial(out_kernel, cfg),
        out_shape=jax.ShapeDtypeStruct(theta.shape, F32),
        in_specs=[vmem],
        out_specs=vmem,
        scratch_shapes=[
            pltpu.VMEM(theta.shape, F32),
            pltpu.VMEM((2, 4, 4, hb, fcol), F32),
            pltpu.VMEM((2, 2, 2, hb, fcol), F32),
            pltpu.VMEM((2, 2, 2, hb, fcol), F32),
        ] + move_sems,
        compiler_params=pltpu.CompilerParams(collective_id=2, **params),
        name="particles_out",
    )(th)


def solution(mesh, sizes=(4, 4, 4)):
    part_size = mesh.shape["part"]
    feat_size = mesh.shape["feat"]

    def local_steps(local_theta, prec_loc, mean_loc, factor_loc):
        rows_loc, feat_loc = local_theta.shape
        n_total = rows_loc * part_size
        feat_total = feat_loc * feat_size
        kern_width = 2.0 * feat_total / math.log(n_total)
        step_size = 0.15 * n_total * feat_total / math.log(n_total)
        return run_steps(local_theta, prec_loc, mean_loc, factor_loc, sizes, kern_width, step_size)

    row_spec = P(("ens", "part"), "feat")
    vec_spec = P(("ens", "feat"))
    fac_spec = P(("ens", "feat"), None)
    return jax.shard_map(local_steps, mesh=mesh, in_specs=(row_spec, vec_spec, vec_spec, fac_spec), out_specs=row_spec, check_vma=False)
```

```python
import functools
import math
import jax
import jax.numpy as jnp
from jax import lax
from jax.experimental import pallas as pl
from jax.experimental.pallas import tpu as pltpu
from jax.sharding import PartitionSpec as P

NUM_STEPS = 3
B = 128
PIECE = 48
F32 = jnp.float32
BF16 = jnp.bfloat16
NT = (((1,), (1,)), ((), ()))
TN = (((0,), (0,)), ((), ()))
NUM_SEMS = 288
MOVE_SEMS = 96
PANEL = 512


def rem(a, n):
    return lax.rem(a, jnp.int32(n))


def div(a, n):
    return lax.div(a, jnp.int32(n))


def unrolled(count, by, body):
    def several(r, cc):
        for t in range(by):
            body(r * by + t)
        return cc
    lax.fori_loop(0, count // by, several, 0)


def steps_kernel(cfg, theta_ref, lam_ref, mu_ref, fact_ref, out_ref, th, t_own, t_par, a_buf, zt, zt_par, zt_b,
                 s_all, d_all, g, ring1, dirb, dir3, acc2, acc3, unit, ag, ag_par, kfull, send_sems, recv_sems):
    sizes, nb, kern_width, step_size = cfg["sizes"], cfg["nb"], cfg["kern_width"], cfg["step_size"]
    nx, ny, nz = sizes
    n_total = nb * B
    n_chip = nx * ny * nz
    part, feat = lax.axis_index("part"), lax.axis_index("feat")
    core = rem(feat, 2)
    me = (feat // 2, rem(part, ny), part // ny)

    def dev(coord, c):
        return {"part": coord[2] * ny + coord[1], "feat": coord[0] * 2 + c}

    def shifted(dim, by):
        c = list(me)
        c[dim] = rem(me[dim] + by, sizes[dim])
        return dev(c, core)

    partner = dev(me, 1 - core)
    perms = [(k, (k + 1) % 3, (k + 2) % 3) for k in range(3)]

    ids = {}

    def copy(key, src, dst, to):
        idx = ids.setdefault(key, len(ids))
        assert idx < NUM_SEMS - 8, idx
        return pltpu.make_async_remote_copy(
            src_ref=src, dst_ref=dst, send_sem=send_sems.at[idx], recv_sem=recv_sems.at[idx],
            device_id=to, device_id_type=pl.DeviceIdType.MESH)

    barrier = pltpu.get_barrier_semaphore()
    peers = [partner] + [shifted(d, by) for d in range(3) if sizes[d] > 1 for by in range(1, sizes[d])]
    for peer in peers:
        pl.semaphore_signal(barrier, inc=1, device_id=peer, device_id_type=pl.DeviceIdType.MESH)
    pl.semaphore_wait(barrier, len(peers))

    row = lax.broadcasted_iota(jnp.int32, (B, B), 0)
    col = lax.broadcasted_iota(jnp.int32, (B, B), 1)
    low, eye = row >= col, row == col

    def blk(i):
        return pl.ds(pl.multiple_of(i * B, B), B)

    def unit_of(c, q):
        u = c * n_chip + q
        i = rem(u, nb)
        return u, i, rem(i + div(u, nb) + 1, nb), u >= 2 * n_chip - nb // 2

    def chip_index(k, coord):
        p = perms[k]
        return (coord[p[0]] * sizes[p[1]] + coord[p[1]]) * sizes[p[2]] + coord[p[2]]

    def coords_of(q):
        return (div(q, ny * nz), rem(div(q, nz), ny), rem(q, nz))

    def split(n, wide):
        if n > 1:
            return (0, n // 2, 0, PIECE), (n // 2, n // 2, 0, PIECE)
        r = 32 if wide else 24
        return (0, 1, 0, r), (0, 1, r, PIECE - r)

    def part_of(ref, lead, base, half):
        return ref.at[lead, pl.ds(base + half[0], half[1]), pl.ds(half[2], half[3])]

    zh = zt.shape[0] // 2
    kc = nb // 4
    n_panels = n_total // PANEL

    def panel(r):
        return pl.ds(pl.multiple_of(r * PANEL, PANEL), PANEL)

    def swap_t(r, slot):
        return pltpu.make_async_remote_copy(
            src_ref=t_own.at[slot, panel(r)], dst_ref=t_par.at[panel(r)], send_sem=send_sems.at[NUM_SEMS - 1 - r],
            recv_sem=recv_sems.at[NUM_SEMS - 1 - r], device_id=partner, device_id_type=pl.DeviceIdType.MESH)

    def swap_z():
        return copy("z", zt.at[pl.ds(pl.multiple_of((1 - core) * zh, 8), zh)], zt_par, partner)

    def prepare(r, theta, slot):
        t_own[slot, panel(r)] = theta.astype(BF16)
        swap_t(r, slot).start()
        xb = (theta - mu_ref[...]).astype(BF16)
        zt[:, panel(r)] = lax.dot_general(fact_ref[...], xb, NT, preferred_element_type=F32)

    def get_rows(r):
        return jnp.concatenate([th[r, v] for v in range(4)], 0)

    def first_prep(r, cc):
        th[r] = theta_ref[r]
        prepare(r, get_rows(r), 0)
        return cc
    fcol = fact_ref.shape[1]
    with jax.named_scope("prep"):
        lax.fori_loop(0, n_panels, first_prep, 0)
        swap_z().start()

    def one_step(step, carry):
        slot = rem(step, 2)
        with jax.named_scope("twait"):
            for r in range(n_panels):
                swap_t(r, slot).wait()
            swap_z().wait()

        def products(rows, cols):
            return (lax.dot_general(jnp.concatenate([t_own[slot, r] for r in rows], 0), t_own[slot, cols], NT,
                                    preferred_element_type=F32)
                    + lax.dot_general(jnp.concatenate([t_par[r] for r in rows], 0), t_par[cols], NT,
                                      preferred_element_type=F32))

        def put(m, q):
            coord = coords_of(q)
            g[0, chip_index(0, coord)] = m[:48]
            g[1, chip_index(1, coord)] = m[48:96]
            g[2, chip_index(2, coord), pl.ds(0, 32)] = m[96:]

        def form(h, cc):
            i = h * 2
            cols = pl.ds(pl.multiple_of(i * B, 2 * B), 2 * B)
            dg = products([cols], cols)
            for t in range(2):
                dt = dg[t * B:(t + 1) * B, t * B:(t + 1) * B]
                d_all[i + t] = dt
                s_all[i + t] = jnp.broadcast_to(jnp.sum(jnp.where(eye, dt, 0.0), axis=0, keepdims=True), (8, B))
            m = products([blk(rem(i + core * kc + 1 + t, nb)) for t in range(kc + 1)], cols)
            for t in range(kc + 1):
                if t < kc:
                    put(m[t * B:(t + 1) * B, :B], t * nb + i)
                if t > 0:
                    put(m[t * B:(t + 1) * B, B:], (t - 1) * nb + i + 1)
            return cc
        with jax.named_scope("form"):
            lax.fori_loop(0, nb // 2, form, 0)

        row8 = lax.broadcasted_iota(jnp.int32, (8, B), 0)

        def tails(q):
            u, i, j, packed = unit_of(core, q)
            zrow = div(u, nb) * 8
            at = chip_index(2, coords_of(q))
            g[2, at, pl.ds(32, 8)] = jnp.where(row8 == 0, s_all[j], s_all[i])
            g[2, at, pl.ds(40, 8)] = (zt[pl.ds(pl.multiple_of(zrow, 8), 8), blk(i)]
                                      + zt_par[pl.ds(pl.multiple_of(zrow - core * zh, 8), 8), blk(i)])
        with jax.named_scope("tails"):
            unrolled(n_chip, 4, tails)

            @pl.when(core == 1)
            def _():
                def pair(t, cc):
                    i = t + nb // 2
                    put(jnp.where(low, d_all[i], d_all[t]), n_chip - nb // 2 + t)
                    return cc
                lax.fori_loop(0, nb // 2, pair, 0)

        pending = []

        def wave(k, s):
            p = perms[k]
            n = sizes[p[2]]
            order = (2, 1, 3, 0) if sizes[p[1]] > 1 else (0,)
            b = rem(me[p[1]] + order[s], sizes[p[1]])
            base = [(rem(me[p[0]] + t, sizes[p[0]]) * sizes[p[1]] + b) * n for t in range(4)]
            return p, n, order[s], base

        def n_waves(k):
            return sizes[perms[k][1]]

        def ring_copy(k, s, tag):
            p, n, by, base = wave(k, s)
            ha, hb = split(n, False)
            at, half, kind, to = {
                "m1p": (2, ha, 0, 1), "m1m": (2, hb, 1, 3), "m2p": (1, hb, 2, 1), "m2m": (3, ha, 3, 3),
                "m3p": (1, ha, 2, 1), "m3m": (3, hb, 3, 3)}[tag]
            return copy(("rs", k, s, tag), part_of(g, k, base[at], half), part_of(ring1.at[k], kind, s * n, half),
                        shifted(p[0], to))

        def ring_start(s, tags):
            for tag in tags:
                for k in range(3):
                    if s < n_waves(k) and sizes[perms[k][0]] > 1:
                        m = ring_copy(k, s, tag)
                        m.start()
                        pending.append(m)

        def ring_merge(s):
            for k in range(3):
                if s >= n_waves(k) or sizes[perms[k][0]] == 1:
                    continue
                p, n, by, base = wave(k, s)
                ha, hb = split(n, False)
                for got, out, at, half, kind in (("m1p", "m3p", 1, ha, 0), ("m1m", "m3m", 3, hb, 1)):
                    ring_copy(k, s, got).wait_recv()
                    part_of(g, k, base[at], half)[...] += part_of(ring1.at[k], kind, s * n, half)[...]
                    m = ring_copy(k, s, out)
                    m.start()
                    pending.append(m)

        def owner_copy(k, by, s, n):
            return copy(("rb", k, by), acc2.at[k, pl.ds(s * n, n)], dirb.at[k, by], shifted(perms[k][1], by))

        def ring_finish(s):
            for k in range(3):
                if s >= n_waves(k):
                    continue
                p, n, by, base = wave(k, s)
                ringed = sizes[p[0]] > 1
                if ringed:
                    for tag in ("m2p", "m2m", "m3p", "m3m"):
                        ring_copy(k, s, tag).wait_recv()
                for v in range(n):
                    tot = g[k, base[0] + v]
                    if ringed:
                        tot = tot + ring1[k, 2, s * n + v] + ring1[k, 3, s * n + v]
                    acc2[k, s * n + v] = tot
                if by:
                    m = owner_copy(k, by, s, n)
                    m.start()
                    pending.append(m)

        most = max(n_waves(k) for k in range(3))
        with jax.named_scope("rs0"):
            ring_start(0, ("m1p", "m1m", "m2p", "m2m"))
            ring_start(1, ("m1p", "m1m"))
            for s in range(most):
                ring_merge(s)
                ring_start(s + 1, ("m2p", "m2m"))
                ring_start(s + 2, ("m1p", "m1m"))
                if s:
                    ring_finish(s - 1)
            ring_finish(most - 1)
        last = []
        with jax.named_scope("rs1"):
            for k in range(3):
                p = perms[k]
                n = sizes[p[2]]
                s = n_waves(k) - 1
                bys = range(1, sizes[p[1]])
                for by in bys:
                    owner_copy(k, by, 0, n).wait_recv()
                for v in range(n):
                    tot = acc2[k, s * n + v]
                    for by in bys:
                        tot = tot + dirb[k, by, v]
                    acc3[k, v] = tot
                ms = []
                for by in range(1, sizes[p[2]]):
                    m = copy(("rc", k, by), acc3.at[k, rem(me[p[2]] + by, sizes[p[2]])], dir3.at[k, by],
                             shifted(p[2], by))
                    m.start()
                    ms.append(m)
                last.append(ms)
                pending += ms
        with jax.named_scope("rs2"):
            for k in range(3):
                tot = acc3[k, me[perms[k][2]]]
                for m in last[k]:
                    m.wait_recv()
                for by in range(1, len(last[k]) + 1):
                    tot = tot + dir3[k, by]
                unit[k] = tot

        with jax.named_scope("kunit"):
            packed = unit_of(core, (me[0] * ny + me[1]) * nz + me[2])[3]
            g_u = jnp.concatenate([unit[0], unit[1], unit[2, pl.ds(0, 32)]], 0)
            sj = jnp.broadcast_to(unit[2, pl.ds(32, 1)], (B, B))
            si = jnp.broadcast_to(unit[2, pl.ds(33, 1)], (B, B))
            si_c = jnp.broadcast_to(jnp.sum(jnp.where(eye, si, 0.0), axis=1, keepdims=True), (B, B))
            sj_c = jnp.broadcast_to(jnp.sum(jnp.where(eye, sj, 0.0), axis=1, keepdims=True), (B, B))
            lower = jnp.logical_and(packed, low)
            upper = jnp.logical_and(packed, jnp.logical_not(low))
            s_sum = jnp.where(lower, si_c, sj_c) + jnp.where(upper, sj, si)
            dist = jnp.maximum(s_sum - 2.0 * g_u, 0.0)
            k_u = jnp.exp(-dist / kern_width)
            z_u = unit[2, pl.ds(40, 8)]
            pieces = (k_u[:48], k_u[48:96], jnp.concatenate([k_u[96:], z_u, jnp.zeros_like(z_u)], 0))
            own = [chip_index(k, me) for k in range(3)]
            for k in range(3):
                ag[k, own[k]] = pieces[k].astype(BF16)

        def place(ref, c, k, a, b):
            p = perms[k]
            for v in range(sizes[p[2]]):
                coord = [0, 0, 0]
                coord[p[0]], coord[p[1]], coord[p[2]] = a, b, v
                q = (coord[0] * ny + coord[1]) * nz + coord[2]
                u, i, j, packed = unit_of(c, q)
                top = (j + div(u, 2 * n_chip - nb // 2) * (nb // 2)) * B + 48 * k
                at = (a * sizes[p[1]] + b) * sizes[p[2]] + v
                n = (48, 48, 32)[k]
                kfull[pl.ds(pl.multiple_of(top, 16), n), blk(i)] = ref[k, at, pl.ds(0, n)]
                if k == 2:
                    tail = ref[k, at, pl.ds(32, 16)].astype(F32)
                    zt_b[pl.ds(pl.multiple_of(div(u, nb) * 8, 8), 8), blk(i)] = tail[:8]

        def chunk(k, ta, tb):
            p = perms[k]
            a, b = rem(me[p[0]] + ta, sizes[p[0]]), rem(me[p[1]] + tb, sizes[p[1]])
            return a, b, (a * sizes[p[1]] + b) * sizes[p[2]], sizes[p[2]]

        def swap(k, ta, tb):
            a, b, at, n = chunk(k, ta, tb)
            return copy(("sw", k, ta, tb), ag.at[k, pl.ds(at, n)], ag_par.at[k, pl.ds(at, n)], partner)

        swaps = []
        placed = []

        def take(upto):
            while len(placed) < upto:
                k, ta, tb = swaps[len(placed)]
                swap(k, ta, tb).wait_recv()
                a, b, at, n = chunk(k, ta, tb)
                place(ag_par, 1 - core, k, a, b)
                placed.append((k, ta, tb))

        def have(k, ta, tb):
            swap(k, ta, tb).start()
            swaps.append((k, ta, tb))
            a, b, at, n = chunk(k, ta, tb)
            place(ag, core, k, a, b)

        def unit_copy(stage, k, by, tc, start):
            p = perms[k]
            a, b, at, n = chunk(k, 0, 0)
            at = at + rem(me[p[2]] + tc, n)
            m = copy(("u", stage, k, by, tc), ag.at[k, at], ag.at[k, at], shifted(p[stage], by))
            if start:
                m.start()
                pending.append(m)
            return m

        def a_copy(k, tb, tag, start=False):
            p = perms[k]
            ta, h, to = {"n1p": (0, 0, 1), "n1m": (0, 1, 3), "n2p": (0, 1, 1), "n2m": (0, 0, 3), "n3p": (3, 0, 1),
                         "n3m": (1, 1, 3)}[tag]
            a, b, at, n = chunk(k, ta, tb)
            half = split(n, True)[h]
            m = copy(("a", k, tb, tag), part_of(ag, k, at, half), part_of(ag, k, at, half), shifted(p[0], to))
            if start:
                m.start()
                pending.append(m)
            return m

        def a_launch(k, tb):
            if sizes[perms[k][0]] > 1:
                for tag in ("n1p", "n1m", "n2p", "n2m"):
                    a_copy(k, tb, tag, True)
            have(k, 0, tb)

        def a_relay(tb):
            for k in range(3):
                if sizes[perms[k][0]] > 1 and (tb == 0 or sizes[perms[k][1]] > 1):
                    for got, out in (("n1p", "n3p"), ("n1m", "n3m")):
                        a_copy(k, tb, got).wait_recv()
                        a_copy(k, tb, out, True)

        def a_near(tb):
            for k in range(3):
                if sizes[perms[k][0]] > 1 and (tb == 0 or sizes[perms[k][1]] > 1):
                    for got, ta in (("n2p", 3), ("n2m", 1)):
                        a_copy(k, tb, got).wait_recv()
                        have(k, ta, tb)

        def a_far(tb):
            for k in range(3):
                if sizes[perms[k][0]] > 1 and (tb == 0 or sizes[perms[k][1]] > 1):
                    for got in ("n3p", "n3m"):
                        a_copy(k, tb, got).wait_recv()
                    have(k, 2, tb)

        with jax.named_scope("ag2"):
            for k in range(3):
                for by in range(1, sizes[perms[k][2]]):
                    unit_copy(2, k, by, 0, True)
            for k in range(3):
                for by in range(1, sizes[perms[k][1]]):
                    unit_copy(1, k, by, 0, True)
            for k in range(3):
                p = perms[k]
                for by in range(1, sizes[p[2]]):
                    unit_copy(2, k, by, 0, False).wait_recv()
                    for bb in range(1, sizes[p[1]]):
                        unit_copy(1, k, bb, sizes[p[2]] - by, True)
                a_launch(k, 0)

        def b_arrivals(bb):
            for k in range(3):
                p = perms[k]
                if sizes[p[1]] > 1:
                    for tc in range(sizes[p[2]]):
                        unit_copy(1, k, bb, tc, False).wait_recv()
                    a_launch(k, sizes[p[1]] - bb)

        with jax.named_scope("ag1"):
            for name, stage, at in (("b1", b_arrivals, 1), ("r0", a_relay, 0), ("b3", b_arrivals, 3), ("r3", a_relay, 3),
                                    ("b2", b_arrivals, 2), ("n0", a_near, 0), ("r1", a_relay, 1), ("n3", a_near, 3),
                                    ("r2", a_relay, 2)):
                with jax.named_scope("ag1_" + name):
                    stage(at)
        with jax.named_scope("ag0"):
            for stage, tb in ((a_far, 0), (a_near, 1), (a_far, 3), (a_near, 2), (a_far, 1), (a_far, 2)):
                before = len(swaps)
                with jax.named_scope("ag0_%s%d" % (stage.__name__, tb)):
                    stage(tb)
                take(before - 12)

        per = 4 if nb > 4 else 2

        def mirror(c, r, cc):
            at = []
            for t in range(per):
                u, i, j, packed = unit_of(c, r * per + t)
                at.append((i, j, kfull[blk(j), blk(i)].T))
            for i, j, m in at:
                kfull[blk(i), blk(j)] = m
            return cc

        def unpack(t, cc):
            i = t + nb // 2
            m = kfull[blk(i), blk(i)].astype(F32)
            mt = m.T
            kfull[blk(i), blk(i)] = jnp.where(eye, 1.0, jnp.where(low, m, mt)).astype(BF16)
            kfull[blk(t), blk(t)] = jnp.where(eye, 1.0, jnp.where(low, mt, m)).astype(BF16)
            return cc
        with jax.named_scope("mirror1"):
            lax.fori_loop(0, div(n_chip - core * (nb // 2), per), functools.partial(mirror, core), 0)
        with jax.named_scope("swapwait"):
            take(len(swaps))
        with jax.named_scope("mirror2"):
            lax.fori_loop(0, div(n_chip - (1 - core) * (nb // 2), per), functools.partial(mirror, 1 - core), 0)
            lax.fori_loop(0, nb // 2, unpack, 0)

        def grads(r, cc):
            lowt = lax.dot_general(zt_b[:, panel(r)].astype(BF16), fact_ref[...], TN, preferred_element_type=F32)
            a_buf[panel(r)] = (-((get_rows(r) - mu_ref[...]) * lam_ref[...] + lowt)).astype(BF16)
            return cc
        with jax.named_scope("grads"):
            lax.fori_loop(0, n_panels, grads, 0)

        def update(r, cc):
            kr = kfull[panel(r)]
            mass = jnp.sum(kr.astype(F32), axis=1, keepdims=True)
            drive = jnp.dot(kr, a_buf[...], preferred_element_type=F32)
            pull = jnp.dot(kr, t_own[slot], preferred_element_type=F32)
            upd = (drive + (2.0 / kern_width) * (mass * t_own[slot, panel(r)].astype(F32) - pull)) / n_total
            theta = get_rows(r) + step_size * upd
            for v in range(4):
                th[r, v] = theta[v * B:(v + 1) * B]

            @pl.when(step < NUM_STEPS - 1)
            def _():
                prepare(r, theta, 1 - slot)
            return cc
        with jax.named_scope("update"):
            lax.fori_loop(0, n_panels, update, 0)

            @pl.when(step < NUM_STEPS - 1)
            def _():
                swap_z().start()
        with jax.named_scope("sendwait"):
            for m in pending:
                m.wait_send()
            for k, ta, tb in swaps:
                swap(k, ta, tb).wait_send()
        return carry

    lax.fori_loop(0, NUM_STEPS, one_step, 0)

    with jax.named_scope("finish"):
        out_ref[...] = th[...]


def mover(cfg, fcol, send_sems, recv_sems):
    nx, ny, nz = cfg["sizes"]
    part, feat = lax.axis_index("part"), lax.axis_index("feat")
    me = (div(feat, 2), rem(part, ny), div(part, ny))
    ids = {}

    def shifted(dim, by):
        c = list(me)
        c[dim] = rem(me[dim] + by, 4)
        return {"part": c[2] * ny + c[1], "feat": feat}

    def copy(key, src, dst, to):
        idx = ids.setdefault(key, len(ids))
        assert idx < MOVE_SEMS
        return pltpu.make_async_remote_copy(
            src_ref=src, dst_ref=dst, send_sem=send_sems.at[idx], recv_sem=recv_sems.at[idx],
            device_id=to, device_id_type=pl.DeviceIdType.MESH)

    barrier = pltpu.get_barrier_semaphore()
    for d in (1, 2):
        for by in (1, 3):
            pl.semaphore_signal(barrier, inc=1, device_id=shifted(d, by), device_id_type=pl.DeviceIdType.MESH)
    pl.semaphore_wait(barrier, 4)

    my = pl.ds(pl.multiple_of((me[1] * nz + me[2]) * fcol, fcol), fcol)

    def cols(y, z, n=1):
        return pl.ds(pl.multiple_of((y * nz + z) * fcol, fcol), n * fcol)

    def side(d, by):
        return rem(me[d] + by, 4)

    def relayed(key, d, sends):
        def copies(tag):
            return [copy((key, tag, t), src, dst, shifted(d, 1 if tag[1] == "+" else 3))
                    for t, (src, dst) in enumerate(sends(tag))]
        started = []

        def go(tags):
            for tag in tags:
                for m in copies(tag):
                    m.start()
                    started.append(m)

        def relay():
            for got, out in (("r+", "f+"), ("r-", "f-")):
                for m in copies(got):
                    m.wait_recv()
                go((out,))

        def finish():
            for tag in ("d+", "d-", "f+", "f-"):
                for m in copies(tag):
                    m.wait_recv()
        go(("r+", "r-", "d+", "d-"))
        return relay, finish, started

    def halves(tag):
        if tag[0] == "d":
            return (0, 1, 2, 3)
        return (0, 1) if tag[1] == "+" else (2, 3)

    return me, my, cols, side, relayed, halves


def mine(ref, h, v, src_at):
    hb = B // 2
    return ref.at[src_at, v, pl.ds(0, hb)] if h == 0 else ref.at[v, src_at, pl.ds(hb, hb)]


def in_kernel(cfg, theta_ref, lam_all, mu_all, fact_all, out_ref, lam_ref, mu_ref, fact_ref, th, l1, rel1, rel2,
              send_sems, recv_sems):
    fcol, hb = fact_ref.shape[1], B // 2
    nx, ny, nz = cfg["sizes"]
    me, my, cols, side, relayed, halves = mover(cfg, fcol, send_sems, recv_sems)

    def in_first(h):
        d = 1 + h

        def sends(tag):
            r0, nr = {"r+": (0, hb // 2), "r-": (hb // 2, hb // 2)}.get(tag, (0, hb))
            way = tag[1] == "+"
            if tag[0] == "f":
                b = 0 if way else 1
                return [(rel1.at[h, b], l1.at[h, side(d, 3 if way else 1), pl.ds(b * (hb // 2), hb // 2)])]
            to = side(d, {"r": 2, "d": 1 if way else 3}[tag[0]])
            rows = pl.ds(h * hb + r0, nr)

            def dst(y, n):
                at = pl.ds(y * fcol, n * fcol)
                if tag[0] == "d":
                    return l1.at[h, me[d], pl.ds(0, nr), at]
                return rel1.at[h, 0 if way else 1, pl.ds(0, nr), at]
            if h == 0:
                return [(theta_ref.at[rows, cols(to, 0, 4)], dst(0, 4))]
            return [(theta_ref.at[rows, cols(y, to)], dst(y, 1)) for y in range(4)]
        return relayed(("in1", h), d, sends)

    def in_second(h):
        d = 2 - h

        def sends(tag):
            way = tag[1] == "+"
            b = 0 if way else 1
            if tag[0] == "f":
                return [(rel2.at[h, b, v % 2], mine(th, h, v, side(d, 3 if way else 1))) for v in halves(tag)]
            to = side(d, {"r": 2, "d": 1 if way else 3}[tag[0]])
            at = pl.ds(pl.multiple_of(to * fcol, fcol), fcol)
            return [(l1.at[h, v, pl.ds(0, hb), at], mine(th, h, v, me[d]) if tag[0] == "d" else rel2.at[h, b, v % 2])
                    for v in halves(tag)]
        return relayed(("in2", h), d, sends)

    with jax.named_scope("in1"):
        first = [in_first(h) for h in range(2)]
        lam_ref[...] = lam_all[pl.ds(0, 1), my]
        mu_ref[...] = mu_all[pl.ds(0, 1), my]
        fact_ref[...] = fact_all[pl.ds(0, fact_ref.shape[0]), my]
        l1[0, me[1]] = theta_ref[pl.ds(0, hb), cols(me[1], 0, 4)]
        for y in range(4):
            l1[1, me[2], pl.ds(0, hb), pl.ds(y * fcol, fcol)] = theta_ref[pl.ds(hb, hb), cols(y, me[2])]
        for relay, finish, started in first:
            relay()
    with jax.named_scope("in2"):
        second = []
        for h, (relay, finish, started) in enumerate(first):
            finish()
            second.append(in_second(h))
        for v in range(4):
            th[me[2], v, pl.ds(0, hb)] = l1[0, v, pl.ds(0, hb), pl.ds(pl.multiple_of(me[2] * fcol, fcol), fcol)]
            th[v, me[1], pl.ds(hb, hb)] = l1[1, v, pl.ds(0, hb), pl.ds(pl.multiple_of(me[1] * fcol, fcol), fcol)]
        for relay, finish, started in second:
            relay()
        for relay, finish, started in second:
            finish()
        for relay, finish, started in first + second:
            for m in started:
                m.wait_send()
    out_ref[...] = th[...]


def out_kernel(cfg, th, out_ref, land, m1, rel2, rel3, send_sems, recv_sems):
    fcol, hb = th.shape[3], B // 2
    nx, ny, nz = cfg["sizes"]
    me, my, cols, side, relayed, halves = mover(cfg, fcol, send_sems, recv_sems)

    def out_first(h):
        d = 2 - h

        def sends(tag):
            way = tag[1] == "+"
            b = 0 if way else 1
            if tag[0] == "f":
                return [(rel2.at[h, b, v % 2], m1.at[h, side(d, 3 if way else 1), v]) for v in halves(tag)]
            to = side(d, {"r": 2, "d": 1 if way else 3}[tag[0]])
            return [(mine(th, h, v, to), m1.at[h, me[d], v] if tag[0] == "d" else rel2.at[h, b, v % 2])
                    for v in halves(tag)]
        return relayed(("out1", h), d, sends)

    def out_second(h):
        d = 1 + h

        def place_of(src_at, v):
            return land.at[pl.ds(h * hb, hb), cols(src_at, v) if h == 0 else cols(v, src_at)]

        def sends(tag):
            way = tag[1] == "+"
            b = 0 if way else 1
            if tag[0] == "f":
                return [(rel3.at[h, b, t], place_of(side(d, 3 if way else 1), 2 * b + t)) for t in range(2)]
            to = side(d, {"r": 2, "d": 1 if way else 3}[tag[0]])
            if tag[0] == "r":
                return [(m1.at[h, v, to], rel3.at[h, b, v % 2]) for v in halves(tag)]
            return [(m1.at[h, v, to], place_of(me[d], v)) for v in range(4)]
        return relayed(("out2", h), d, sends)

    with jax.named_scope("out1"):
        first = [out_first(h) for h in range(2)]
        for v in range(4):
            m1[0, me[2], v] = th[me[2], v, pl.ds(0, hb)]
            m1[1, me[1], v] = th[v, me[1], pl.ds(hb, hb)]
        for relay, finish, started in first:
            relay()
    with jax.named_scope("out2"):
        second = []
        for h, (relay, finish, started) in enumerate(first):
            finish()
            second.append(out_second(h))
        for v in range(4):
            land[pl.ds(0, hb), cols(me[1], v)] = m1[0, v, me[1]]
            land[pl.ds(hb, hb), cols(v, me[2])] = m1[1, v, me[2]]
        for relay, finish, started in second:
            relay()
        for relay, finish, started in second:
            finish()
        for relay, finish, started in first + second:
            for m in started:
                m.wait_send()
    out_ref[...] = land[...]


def run_steps(theta, lam, mu, fac, sizes, kern_width, step_size):
    n_total, fcol = theta.shape[0] * sizes[1] * sizes[2], theta.shape[1] // (sizes[1] * sizes[2])
    rank = fac.shape[1]
    nb = n_total // B
    n_chip = sizes[0] * sizes[1] * sizes[2]
    assert nb * nb == 4 * n_chip and rank == 4 * nb
    hb = B // 2
    cfg = dict(sizes=sizes, nb=nb, kern_width=kern_width, step_size=step_size)
    n1, n2 = n_chip, n_chip
    vmem = pl.BlockSpec(memory_space=pltpu.VMEM)
    most1 = max(n_chip // sizes[k] for k in range(3))
    most2 = max(sizes)
    params = dict(has_side_effects=True, vmem_limit_bytes=60 * 1024 * 1024)
    blocks = (4, 4, B, fcol)
    move_sems = [pltpu.SemaphoreType.DMA((MOVE_SEMS,)), pltpu.SemaphoreType.DMA((MOVE_SEMS,))]
    th, lam, mu, fact = pl.pallas_call(
        functools.partial(in_kernel, cfg),
        out_shape=[jax.ShapeDtypeStruct(blocks, F32), jax.ShapeDtypeStruct((1, fcol), F32),
                   jax.ShapeDtypeStruct((1, fcol), F32), jax.ShapeDtypeStruct((rank, fcol), BF16)],
        in_specs=[vmem] * 4,
        out_specs=[vmem] * 4,
        scratch_shapes=[
            pltpu.VMEM(blocks, F32),
            pltpu.VMEM((2, 4, hb, 4 * fcol), F32),
            pltpu.VMEM((2, 2, hb // 2, 4 * fcol), F32),
            pltpu.VMEM((2, 2, 2, hb, fcol), F32),
        ] + move_sems,
        compiler_params=pltpu.CompilerParams(collective_id=1, **params),
        name="particles_in",
    )(theta, lam[None], mu[None], fac.T)
    scratch = [
        pltpu.VMEM(blocks, F32),
        pltpu.VMEM((2, n_total, fcol), BF16),
        pltpu.VMEM((n_total, fcol), BF16),
        pltpu.VMEM((n_total, fcol), BF16),
        pltpu.VMEM((rank, n_total), F32),
        pltpu.VMEM((rank // 2, n_total), F32),
        pltpu.VMEM((rank, n_total), F32),
        pltpu.VMEM((nb, 8, B), F32),
        pltpu.VMEM((nb, B, B), F32),
        pltpu.VMEM((3, n_chip, PIECE, B), F32),
        pltpu.VMEM((3, 4, most1, PIECE, B), F32),
        pltpu.VMEM((3, 4, most2, PIECE, B), F32),
        pltpu.VMEM((3, 4, PIECE, B), F32),
        pltpu.VMEM((3, most1, PIECE, B), F32),
        pltpu.VMEM((3, most2, PIECE, B), F32),
        pltpu.VMEM((3, PIECE, B), F32),
        pltpu.VMEM((3, n_chip, PIECE, B), BF16),
        pltpu.VMEM((3, n_chip, PIECE, B), BF16),
        pltpu.VMEM((n_total, n_total), BF16),
        pltpu.SemaphoreType.DMA((NUM_SEMS,)),
        pltpu.SemaphoreType.DMA((NUM_SEMS,)),
    ]
    th = pl.pallas_call(
        functools.partial(steps_kernel, cfg),
        out_shape=jax.ShapeDtypeStruct(blocks, F32),
        in_specs=[vmem] * 4,
        out_specs=vmem,
        scratch_shapes=scratch,
        compiler_params=pltpu.CompilerParams(collective_id=0, **params),
        name="svgd_steps",
    )(th, lam, mu, fact)
    return pl.pallas_call(
        functools.partial(out_kernel, cfg),
        out_shape=jax.ShapeDtypeStruct(theta.shape, F32),
        in_specs=[vmem],
        out_specs=vmem,
        scratch_shapes=[
            pltpu.VMEM(theta.shape, F32),
            pltpu.VMEM((2, 4, 4, hb, fcol), F32),
            pltpu.VMEM((2, 2, 2, hb, fcol), F32),
            pltpu.VMEM((2, 2, 2, hb, fcol), F32),
        ] + move_sems,
        compiler_params=pltpu.CompilerParams(collective_id=2, **params),
        name="particles_out",
    )(th)


def solution(mesh, sizes=(4, 4, 4)):
    part_size = mesh.shape["part"]
    feat_size = mesh.shape["feat"]

    def local_steps(local_theta, prec_loc, mean_loc, factor_loc):
        rows_loc, feat_loc = local_theta.shape
        n_total = rows_loc * part_size
        feat_total = feat_loc * feat_size
        kern_width = 2.0 * feat_total / math.log(n_total)
        step_size = 0.15 * n_total * feat_total / math.log(n_total)
        return run_steps(local_theta, prec_loc, mean_loc, factor_loc, sizes, kern_width, step_size)

    row_spec = P(("ens", "part"), "feat")
    vec_spec = P(("ens", "feat"))
    fac_spec = P(("ens", "feat"), None)
    return jax.shard_map(local_steps, mesh=mesh, in_specs=(row_spec, vec_spec, vec_spec, fac_spec), out_specs=row_spec, check_vma=False)
```

```python
import functools
import math
import jax
import jax.numpy as jnp
from jax import lax
from jax.experimental import pallas as pl
from jax.experimental.pallas import tpu as pltpu
from jax.sharding import PartitionSpec as P

NUM_STEPS = 3
B = 128
PIECE = 48
F32 = jnp.float32
BF16 = jnp.bfloat16
NT = (((1,), (1,)), ((), ()))
TN = (((0,), (0,)), ((), ()))
NUM_SEMS = 416
PANEL = 512


def rem(a, n):
    return lax.rem(a, jnp.int32(n))


def div(a, n):
    return lax.div(a, jnp.int32(n))


def unrolled(count, by, body):
    def several(r, cc):
        for t in range(by):
            body(r * by + t)
        return cc
    lax.fori_loop(0, count // by, several, 0)


def mine(ref, h, v, src_at):
    hb = B // 2
    return ref.at[src_at, v, pl.ds(0, hb)] if h == 0 else ref.at[v, src_at, pl.ds(hb, hb)]


def steps_kernel(cfg, theta_ref, lam_all, mu_all, fact_all, out_ref, th, l1, m1, rel1, rel2, rel3, lam_ref, mu_ref, fact_ref,
                 t_own, t_par, a_buf, zt, zt_par, zt_b, s_all, d_all, g, ring1, relb, dirb, dir3, acc2, acc3, unit, ag,
                 ag_par, kfull, send_sems, recv_sems):
    nb, kern_width, step_size = cfg["nb"], cfg["kern_width"], cfg["step_size"]
    n_total = nb * B
    n_chip = 64
    part, feat = lax.axis_index("part"), lax.axis_index("feat")
    core = rem(feat, 2)
    me = (div(feat, 2), rem(part, 4), div(part, 4))
    near = [[me[d]] + [rem(me[d] + by, 4) for by in (1, 2, 3)] for d in range(3)]

    def dev(coord, c):
        return {"part": coord[2] * 4 + coord[1], "feat": coord[0] * 2 + c}

    def device_at(dim, by):
        c = list(me)
        c[dim] = near[dim][by]
        return dev(c, core)

    around = [[device_at(d, by) for by in range(4)] for d in range(3)]

    def shifted(dim, by):
        return around[dim][by]

    partner = dev(me, 1 - core)
    perms = [(k, (k + 1) % 3, (k + 2) % 3) for k in range(3)]

    ids = {}

    def slot_of(key):
        idx = ids.setdefault(key, len(ids))
        assert idx < NUM_SEMS - 8
        return idx

    def copy(key, src, dst, to):
        idx = slot_of(key)
        return pltpu.make_async_remote_copy(
            src_ref=src, dst_ref=dst, send_sem=send_sems.at[idx], recv_sem=recv_sems.at[idx],
            device_id=to, device_id_type=pl.DeviceIdType.MESH)

    def local(key, src, dst):
        return pltpu.make_async_copy(src, dst, send_sems.at[slot_of(key)])

    barrier = pltpu.get_barrier_semaphore()
    peers = [partner] + [shifted(d, by) for d in range(3) for by in (1, 2, 3)]
    for peer in peers:
        pl.semaphore_signal(barrier, inc=1, device_id=peer, device_id_type=pl.DeviceIdType.MESH)
    pl.semaphore_wait(barrier, len(peers))

    row = lax.broadcasted_iota(jnp.int32, (B, B), 0)
    col = lax.broadcasted_iota(jnp.int32, (B, B), 1)
    low, eye = row >= col, row == col

    def blk(i):
        return pl.ds(pl.multiple_of(i * B, B), B)

    def unit_of(c, q):
        u = c * n_chip + q
        i = rem(u, nb)
        return u, i, rem(i + div(u, nb) + 1, nb), u >= 2 * n_chip - nb // 2

    def chip_index(k, x, y, z):
        p = perms[k]
        c = (x, y, z)
        return (c[p[0]] * 4 + c[p[1]]) * 4 + c[p[2]]

    def split(n, wide):
        if n > 1:
            return (0, n // 2, 0, PIECE), (n // 2, n // 2, 0, PIECE)
        r = 32 if wide else 24
        return (0, 1, 0, r), (0, 1, r, PIECE - r)

    def part_of(ref, lead, base, half):
        return ref.at[lead, pl.ds(base + half[0], half[1]), pl.ds(half[2], half[3])]

    zh = zt.shape[0] // 2
    kc = nb // 4
    n_panels = n_total // PANEL

    def panel(r):
        return pl.ds(pl.multiple_of(r * PANEL, PANEL), PANEL)

    def swap_t(r, slot):
        return pltpu.make_async_remote_copy(
            src_ref=t_own.at[slot, panel(r)], dst_ref=t_par.at[panel(r)], send_sem=send_sems.at[NUM_SEMS - 1 - r],
            recv_sem=recv_sems.at[NUM_SEMS - 1 - r], device_id=partner, device_id_type=pl.DeviceIdType.MESH)

    def swap_z():
        return copy("z", zt.at[pl.ds(pl.multiple_of((1 - core) * zh, 8), zh)], zt_par, partner)

    def prepare(r, theta, slot):
        t_own[slot, panel(r)] = theta.astype(BF16)
        swap_t(r, slot).start()
        xb = (theta - mu_ref[...]).astype(BF16)
        zt[:, panel(r)] = lax.dot_general(fact_ref[...], xb, NT, preferred_element_type=F32)

    def get_rows(r):
        return jnp.concatenate([th[r, v] for v in range(4)], 0)

    def first_prep(r, cc):
        prepare(r, get_rows(r), 0)
        return cc
    fcol, hb = fact_ref.shape[1], B // 2
    my = pl.ds(pl.multiple_of((me[1] * 4 + me[2]) * fcol, fcol), fcol)

    def cols(y, z, n=1):
        return pl.ds(pl.multiple_of((y * 4 + z) * fcol, fcol), n * fcol)

    def side(d, by):
        return near[d][by]

    def relayed(key, d, sends):
        def copies(tag):
            return [copy((key, tag, t), src, dst, shifted(d, 1 if tag[1] == "+" else 3))
                    for t, (src, dst) in enumerate(sends(tag))]
        started = []

        def go(tags):
            for tag in tags:
                for m in copies(tag):
                    m.start()
                    started.append(m)

        def relay():
            for got, out in (("r+", "f+"), ("r-", "f-")):
                for m in copies(got):
                    m.wait_recv()
                go((out,))

        def finish():
            for tag in ("d+", "d-", "f+", "f-"):
                for m in copies(tag):
                    m.wait_recv()
        go(("r+", "r-", "d+", "d-"))
        return relay, finish, started

    def halves(tag):
        if tag[0] == "d":
            return (0, 1, 2, 3)
        return (0, 1) if tag[1] == "+" else (2, 3)

    def in_first(h):
        d = 1 + h

        def sends(tag):
            r0, nr = {"r+": (0, hb // 2), "r-": (hb // 2, hb // 2)}.get(tag, (0, hb))
            way = tag[1] == "+"
            if tag[0] == "f":
                b = 0 if way else 1
                return [(rel1.at[h, b], l1.at[h, side(d, 3 if way else 1), pl.ds(b * (hb // 2), hb // 2)])]
            to = side(d, {"r": 2, "d": 1 if way else 3}[tag[0]])
            rows = pl.ds(h * hb + r0, nr)

            def dst(y, n):
                at = pl.ds(y * fcol, n * fcol)
                if tag[0] == "d":
                    return l1.at[h, me[d], pl.ds(0, nr), at]
                return rel1.at[h, 0 if way else 1, pl.ds(0, nr), at]
            if h == 0:
                return [(theta_ref.at[rows, cols(to, 0, 4)], dst(0, 4))]
            return [(theta_ref.at[rows, cols(y, to)], dst(y, 1)) for y in range(4)]
        return relayed(("in1", h), d, sends)

    def in_second(h):
        d = 2 - h

        def sends(tag):
            way = tag[1] == "+"
            b = 0 if way else 1
            if tag[0] == "f":
                return [(rel2.at[h, b, v % 2], mine(th, h, v, side(d, 3 if way else 1))) for v in halves(tag)]
            to = side(d, {"r": 2, "d": 1 if way else 3}[tag[0]])
            at = pl.ds(pl.multiple_of(to * fcol, fcol), fcol)
            return [(l1.at[h, v, pl.ds(0, hb), at], mine(th, h, v, me[d]) if tag[0] == "d" else rel2.at[h, b, v % 2])
                    for v in halves(tag)]
        return relayed(("in2", h), d, sends)

    own_in = [local(("own", 0), theta_ref.at[pl.ds(0, hb), cols(me[1], 0, 4)], l1.at[0, me[1]])]
    own_in += [local(("own", 1 + y), theta_ref.at[pl.ds(hb, hb), cols(y, me[2])],
                     l1.at[1, me[2], pl.ds(0, hb), pl.ds(y * fcol, fcol)]) for y in range(4)]
    own_in.append(local(("own", 5), fact_all.at[pl.ds(0, fact_ref.shape[0]), my], fact_ref))

    with jax.named_scope("in1"):
        first = [in_first(h) for h in range(2)]
        for m in own_in:
            m.start()
        lam_ref[...] = lam_all[pl.ds(0, 1), my]
        mu_ref[...] = mu_all[pl.ds(0, 1), my]
        for relay, finish, started in first:
            relay()
    with jax.named_scope("in2"):
        for m in own_in:
            m.wait()
        second = []
        for h, (relay, finish, started) in enumerate(first):
            finish()
            second.append(in_second(h))
        for v in range(4):
            th[me[2], v, pl.ds(0, hb)] = l1[0, v, pl.ds(0, hb), pl.ds(pl.multiple_of(me[2] * fcol, fcol), fcol)]
            th[v, me[1], pl.ds(hb, hb)] = l1[1, v, pl.ds(0, hb), pl.ds(pl.multiple_of(me[1] * fcol, fcol), fcol)]
        for relay, finish, started in second:
            relay()
        for relay, finish, started in second:
            finish()
        for relay, finish, started in first + second:
            for m in started:
                m.wait_send()
    with jax.named_scope("prep"):
        lax.fori_loop(0, n_panels, first_prep, 0)
        swap_z().start()

    def one_step(step, carry):
        slot = rem(step, 2)
        with jax.named_scope("twait"):
            for r in range(n_panels):
                swap_t(r, slot).wait()
            swap_z().wait()

        def products(rows, cols):
            return (lax.dot_general(jnp.concatenate([t_own[slot, r] for r in rows], 0), t_own[slot, cols], NT,
                                    preferred_element_type=F32)
                    + lax.dot_general(jnp.concatenate([t_par[r] for r in rows], 0), t_par[cols], NT,
                                      preferred_element_type=F32))

        def put(m, x, y, z):
            g[0, chip_index(0, x, y, z)] = m[:48]
            g[1, chip_index(1, x, y, z)] = m[48:96]
            g[2, chip_index(2, x, y, z), pl.ds(0, 32)] = m[96:]

        def form(h, cc):
            i = h * 2
            cols = pl.ds(pl.multiple_of(i * B, 2 * B), 2 * B)
            dg = products([cols], cols)
            for t in range(2):
                dt = dg[t * B:(t + 1) * B, t * B:(t + 1) * B]
                d_all[i + t] = dt
                s_all[i + t] = jnp.broadcast_to(jnp.sum(jnp.where(eye, dt, 0.0), axis=0, keepdims=True), (8, B))
            m = products([blk(rem(i + core * kc + 1 + t, nb)) for t in range(kc + 1)], cols)
            y, z = div(h, 2), 2 * rem(h, 2)
            for t in range(kc + 1):
                if t < kc:
                    put(m[t * B:(t + 1) * B, :B], t, y, z)
                if t > 0:
                    put(m[t * B:(t + 1) * B, B:], t - 1, y, z + 1)
            return cc
        with jax.named_scope("form"):
            lax.fori_loop(0, nb // 2, form, 0)

        row8 = lax.broadcasted_iota(jnp.int32, (8, B), 0)

        def tails(i, cc):
            y, z = div(i, 4), rem(i, 4)
            for x in range(4):
                off = core * kc + x
                at = chip_index(2, x, y, z)
                g[2, at, pl.ds(32, 8)] = jnp.where(row8 == 0, s_all[rem(i + off + 1, nb)], s_all[i])
                g[2, at, pl.ds(40, 8)] = (zt[pl.ds(pl.multiple_of(off * 8, 8), 8), blk(i)]
                                          + zt_par[pl.ds(x * 8, 8), blk(i)])
            return cc
        with jax.named_scope("tails"):
            lax.fori_loop(0, nb, tails, 0)

            @pl.when(core == 1)
            def _():
                def pair(t, cc):
                    i = t + nb // 2
                    put(jnp.where(low, d_all[i], d_all[t]), 3, div(i, 4), rem(i, 4))
                    return cc
                lax.fori_loop(0, nb // 2, pair, 0)

        pending = []

        order = (2, 1, 3, 0)
        wave_base = [[[(near[perms[k][0]][t] * 4 + near[perms[k][1]][o]) * 4 for t in range(4)] for o in order]
                     for k in range(3)]

        def wave(k, s):
            return perms[k], 4, order[s], wave_base[k][s]

        def n_waves(k):
            return 4

        def ring_copy(k, s, tag):
            p, n, by, base = wave(k, s)
            ha, hb = split(n, False)
            at, half, kind, to = {
                "m1p": (2, ha, 0, 1), "m1m": (2, hb, 1, 3), "m2p": (1, hb, 2, 1), "m2m": (3, ha, 3, 3),
                "m3p": (1, ha, 2, 1), "m3m": (3, hb, 3, 3)}[tag]
            return copy(("rs", k, s, tag), part_of(g, k, base[at], half), part_of(ring1.at[k], kind, s * n, half),
                        shifted(p[0], to))

        def ring_start(s, tags):
            for tag in tags:
                for k in range(3):
                    if s < n_waves(k):
                        m = ring_copy(k, s, tag)
                        m.start()
                        pending.append(m)

        def ring_merge(s):
            for k in range(3):
                p, n, by, base = wave(k, s)
                ha, hb = split(n, False)
                for got, out, at, half, kind in (("m1p", "m3p", 1, ha, 0), ("m1m", "m3m", 3, hb, 1)):
                    ring_copy(k, s, got).wait_recv()
                    part_of(g, k, base[at], half)[...] += part_of(ring1.at[k], kind, s * n, half)[...]
                    m = ring_copy(k, s, out)
                    m.start()
                    pending.append(m)

        def owner_copy(k, by, s):
            return copy(("rb", k, by), acc2.at[k, pl.ds(s * 4, 4)], dirb.at[k, by], shifted(perms[k][1], by))

        def via_copy(k, b):
            return copy(("rv", k, b), acc2.at[k, pl.ds(2 * b, 2)], relb.at[k, b], shifted(perms[k][1], (1, 3)[b]))

        def ring_finish(s):
            for k in range(3):
                p, n, by, base = wave(k, s)
                for tag in ("m2p", "m2m", "m3p", "m3m"):
                    ring_copy(k, s, tag).wait_recv()
                if by in (1, 3):
                    via_copy(k, by // 2).wait_recv()
                for v in range(n):
                    tot = g[k, base[0] + v] + ring1[k, 2, s * n + v] + ring1[k, 3, s * n + v]
                    if by in (1, 3) and v // 2 == by // 2:
                        tot = tot + relb[k, by // 2, v % 2]
                    acc2[k, s * n + v] = tot
                ms = [via_copy(k, 0), via_copy(k, 1)] if by == 2 else [owner_copy(k, by, s)] if by else []
                for m in ms:
                    m.start()
                    pending.append(m)

        most = 4
        with jax.named_scope("rs0"):
            ring_start(0, ("m1p", "m1m", "m2p", "m2m"))
            ring_start(1, ("m1p", "m1m"))
            for s in range(most):
                ring_merge(s)
                ring_start(s + 1, ("m2p", "m2m"))
                ring_start(s + 2, ("m1p", "m1m"))
                if s:
                    ring_finish(s - 1)
            ring_finish(most - 1)
        last = []
        with jax.named_scope("rs1"):
            for k in range(3):
                p = perms[k]
                n, s = 4, 3
                bys = (1, 3)
                for by in bys:
                    owner_copy(k, by, 0).wait_recv()
                for v in range(n):
                    tot = acc2[k, s * n + v]
                    for by in bys:
                        tot = tot + dirb[k, by, v]
                    acc3[k, v] = tot
                ms = []
                for by in (1, 2, 3):
                    m = copy(("rc", k, by), acc3.at[k, near[p[2]][by]], dir3.at[k, by],
                             shifted(p[2], by))
                    m.start()
                    ms.append(m)
                last.append(ms)
                pending += ms
        with jax.named_scope("rs2"):
            for k in range(3):
                tot = acc3[k, me[perms[k][2]]]
                for m in last[k]:
                    m.wait_recv()
                for by in range(1, len(last[k]) + 1):
                    tot = tot + dir3[k, by]
                unit[k] = tot

        with jax.named_scope("kunit"):
            packed = unit_of(core, (me[0] * 4 + me[1]) * 4 + me[2])[3]
            g_u = jnp.concatenate([unit[0], unit[1], unit[2, pl.ds(0, 32)]], 0)
            sj = jnp.broadcast_to(unit[2, pl.ds(32, 1)], (B, B))
            si = jnp.broadcast_to(unit[2, pl.ds(33, 1)], (B, B))
            si_c = jnp.broadcast_to(jnp.sum(jnp.where(eye, si, 0.0), axis=1, keepdims=True), (B, B))
            sj_c = jnp.broadcast_to(jnp.sum(jnp.where(eye, sj, 0.0), axis=1, keepdims=True), (B, B))
            lower = jnp.logical_and(packed, low)
            upper = jnp.logical_and(packed, jnp.logical_not(low))
            s_sum = jnp.where(lower, si_c, sj_c) + jnp.where(upper, sj, si)
            dist = jnp.maximum(s_sum - 2.0 * g_u, 0.0)
            k_u = jnp.exp(-dist / kern_width)
            z_u = unit[2, pl.ds(40, 8)]
            pieces = (k_u[:48], k_u[48:96], jnp.concatenate([k_u[96:], z_u, jnp.zeros_like(z_u)], 0))
            own = [chip_index(k, *me) for k in range(3)]
            for k in range(3):
                ag[k, own[k]] = pieces[k].astype(BF16)

        def place(ref, c, k, a, b, at):
            for v in range(4):
                coord = [0, 0, 0]
                for d, t in zip(perms[k], (a, b, v)):
                    coord[d] = t
                off = c * kc + coord[0]
                i = coord[1] * 4 + coord[2]
                top = (rem(i + off + 1, nb) + div(off * nb + i, 2 * n_chip - nb // 2) * (nb // 2)) * B + 48 * k
                n = (48, 48, 32)[k]
                kfull[pl.ds(pl.multiple_of(top, 16), n), blk(i)] = ref[k, at + v, pl.ds(0, n)]
                if k == 2:
                    tail = ref[k, at + v, pl.ds(32, 16)].astype(F32)
                    zt_b[pl.ds(pl.multiple_of(off * 8, 8), 8), blk(i)] = tail[:8]

        chunks = {}

        def chunk(k, ta, tb):
            if (k, ta, tb) not in chunks:
                p = perms[k]
                a, b = near[p[0]][ta], near[p[1]][tb]
                chunks[k, ta, tb] = (a, b, (a * 4 + b) * 4, 4)
            return chunks[k, ta, tb]

        def swap(k, ta, tb):
            a, b, at, n = chunk(k, ta, tb)
            return copy(("sw", k, ta, tb), ag.at[k, pl.ds(at, n)], ag_par.at[k, pl.ds(at, n)], partner)

        swaps = []
        placed = []

        def take(upto):
            while len(placed) < upto:
                k, ta, tb = swaps[len(placed)]
                swap(k, ta, tb).wait_recv()
                a, b, at, n = chunk(k, ta, tb)
                place(ag_par, 1 - core, k, a, b, at)
                placed.append((k, ta, tb))

        def have(k, ta, tb):
            swap(k, ta, tb).start()
            swaps.append((k, ta, tb))
            a, b, at, n = chunk(k, ta, tb)
            place(ag, core, k, a, b, at)

        def unit_copy(stage, k, by, tc, start):
            p = perms[k]
            a, b, at, n = chunk(k, 0, 0)
            at = at + near[p[2]][tc]
            m = copy(("u", stage, k, by, tc), ag.at[k, at], ag.at[k, at], shifted(p[stage], by))
            if start:
                m.start()
                pending.append(m)
            return m

        def a_copy(k, tb, tag, start=False):
            p = perms[k]
            ta, h, to = {"n1p": (0, 0, 1), "n1m": (0, 1, 3), "n2p": (0, 1, 1), "n2m": (0, 0, 3), "n3p": (3, 0, 1),
                         "n3m": (1, 1, 3)}[tag]
            a, b, at, n = chunk(k, ta, tb)
            half = split(n, True)[h]
            m = copy(("a", k, tb, tag), part_of(ag, k, at, half), part_of(ag, k, at, half), shifted(p[0], to))
            if start:
                m.start()
                pending.append(m)
            return m

        def a_launch(k, tb):
            for tag in ("n1p", "n1m", "n2p", "n2m"):
                a_copy(k, tb, tag, True)
            have(k, 0, tb)

        def a_relay(tb):
            for k in range(3):
                if True:
                    for got, out in (("n1p", "n3p"), ("n1m", "n3m")):
                        a_copy(k, tb, got).wait_recv()
                        a_copy(k, tb, out, True)

        def a_near(tb):
            for k in range(3):
                if True:
                    for got, ta in (("n2p", 3), ("n2m", 1)):
                        a_copy(k, tb, got).wait_recv()
                        have(k, ta, tb)

        def a_far(tb):
            for k in range(3):
                if True:
                    for got in ("n3p", "n3m"):
                        a_copy(k, tb, got).wait_recv()
                    have(k, 2, tb)

        with jax.named_scope("ag2"):
            for k in range(3):
                for by in (1, 2, 3):
                    unit_copy(2, k, by, 0, True)
            for k in range(3):
                for by in (1, 2, 3):
                    unit_copy(1, k, by, 0, True)
            for k in range(3):
                p = perms[k]
                for by in (1, 2, 3):
                    unit_copy(2, k, by, 0, False).wait_recv()
                    for bb in (1, 2, 3):
                        unit_copy(1, k, bb, 4 - by, True)
                a_launch(k, 0)

        def b_arrivals(bb):
            for k in range(3):
                p = perms[k]
                if True:
                    for tc in range(4):
                        unit_copy(1, k, bb, tc, False).wait_recv()
                    a_launch(k, 4 - bb)

        with jax.named_scope("ag1"):
            for name, stage, at in (("b1", b_arrivals, 1), ("r0", a_relay, 0), ("b3", b_arrivals, 3), ("r3", a_relay, 3),
                                    ("b2", b_arrivals, 2), ("n0", a_near, 0), ("r1", a_relay, 1), ("n3", a_near, 3),
                                    ("r2", a_relay, 2)):
                with jax.named_scope("ag1_" + name):
                    stage(at)
        with jax.named_scope("ag0"):
            for stage, tb in ((a_far, 0), (a_near, 1), (a_far, 3), (a_near, 2), (a_far, 1), (a_far, 2)):
                before = len(swaps)
                with jax.named_scope("ag0_%s%d" % (stage.__name__, tb)):
                    stage(tb)
                take(before - 12)

        per = 4 if nb > 4 else 2

        def mirror(c, r, cc):
            at = []
            for t in range(per):
                u, i, j, packed = unit_of(c, r * per + t)
                at.append((i, j, kfull[blk(j), blk(i)].T))
            for i, j, m in at:
                kfull[blk(i), blk(j)] = m
            return cc

        def unpack(t, cc):
            i = t + nb // 2
            m = kfull[blk(i), blk(i)].astype(F32)
            mt = m.T
            kfull[blk(i), blk(i)] = jnp.where(eye, 1.0, jnp.where(low, m, mt)).astype(BF16)
            kfull[blk(t), blk(t)] = jnp.where(eye, 1.0, jnp.where(low, mt, m)).astype(BF16)
            return cc
        with jax.named_scope("mirror1"):
            lax.fori_loop(0, div(n_chip - core * (nb // 2), per), functools.partial(mirror, core), 0)
        with jax.named_scope("swapwait"):
            take(len(swaps))
        with jax.named_scope("mirror2"):
            lax.fori_loop(0, div(n_chip - (1 - core) * (nb // 2), per), functools.partial(mirror, 1 - core), 0)
            lax.fori_loop(0, nb // 2, unpack, 0)

        def grads(r, cc):
            lowt = lax.dot_general(zt_b[:, panel(r)].astype(BF16), fact_ref[...], TN, preferred_element_type=F32)
            a_buf[panel(r)] = (-((get_rows(r) - mu_ref[...]) * lam_ref[...] + lowt)).astype(BF16)
            return cc
        with jax.named_scope("grads"):
            lax.fori_loop(0, n_panels, grads, 0)

        def update(r, cc):
            kr = kfull[panel(r)]
            mass = jnp.sum(kr.astype(F32), axis=1, keepdims=True)
            drive = jnp.dot(kr, a_buf[...], preferred_element_type=F32)
            pull = jnp.dot(kr, t_own[slot], preferred_element_type=F32)
            upd = (drive + (2.0 / kern_width) * (mass * t_own[slot, panel(r)].astype(F32) - pull)) / n_total
            theta = get_rows(r) + step_size * upd
            for v in range(4):
                th[r, v] = theta[v * B:(v + 1) * B]

            @pl.when(step < NUM_STEPS - 1)
            def _():
                prepare(r, theta, 1 - slot)
            return cc
        with jax.named_scope("update"):
            lax.fori_loop(0, n_panels, update, 0)

            @pl.when(step < NUM_STEPS - 1)
            def _():
                swap_z().start()
        with jax.named_scope("sendwait"):
            for m in pending:
                m.wait_send()
            for k, ta, tb in swaps:
                swap(k, ta, tb).wait_send()
        return carry

    lax.fori_loop(0, NUM_STEPS, one_step, 0)

    def out_first(h):
        d = 2 - h

        def sends(tag):
            way = tag[1] == "+"
            b = 0 if way else 1
            if tag[0] == "f":
                return [(rel2.at[h, b, v % 2], m1.at[h, side(d, 3 if way else 1), v]) for v in halves(tag)]
            to = side(d, {"r": 2, "d": 1 if way else 3}[tag[0]])
            return [(mine(th, h, v, to), m1.at[h, me[d], v] if tag[0] == "d" else rel2.at[h, b, v % 2])
                    for v in halves(tag)]
        return relayed(("out1", h), d, sends)

    def out_second(h):
        d = 1 + h

        def place_of(src_at, v):
            return out_ref.at[pl.ds(h * hb, hb), cols(src_at, v) if h == 0 else cols(v, src_at)]

        def sends(tag):
            way = tag[1] == "+"
            b = 0 if way else 1
            if tag[0] == "f":
                return [(rel3.at[h, b, t], place_of(side(d, 3 if way else 1), 2 * b + t)) for t in range(2)]
            to = side(d, {"r": 2, "d": 1 if way else 3}[tag[0]])
            if tag[0] == "r":
                return [(m1.at[h, v, to], rel3.at[h, b, v % 2]) for v in halves(tag)]
            return [(m1.at[h, v, to], place_of(me[d], v)) for v in range(4)]
        return relayed(("out2", h), d, sends)

    with jax.named_scope("out1"):
        first = [out_first(h) for h in range(2)]
        for v in range(4):
            m1[0, me[2], v] = th[me[2], v, pl.ds(0, hb)]
            m1[1, me[1], v] = th[v, me[1], pl.ds(hb, hb)]
        for relay, finish, started in first:
            relay()
    with jax.named_scope("out2"):
        second = []
        for h, (relay, finish, started) in enumerate(first):
            finish()
            second.append(out_second(h))
        own_out = []
        for v in range(4):
            own_out.append(local(("back", v), m1.at[0, v, me[1]], out_ref.at[pl.ds(0, hb), cols(me[1], v)]))
            own_out.append(local(("back", 4 + v), m1.at[1, v, me[2]], out_ref.at[pl.ds(hb, hb), cols(v, me[2])]))
        for m in own_out:
            m.start()
        for relay, finish, started in second:
            relay()
        for relay, finish, started in second:
            finish()
        for relay, finish, started in first + second:
            for m in started:
                m.wait_send()
        for m in own_out:
            m.wait()


def run_steps(theta, lam, mu, fac, sizes, kern_width, step_size):
    n_total, fcol = theta.shape[0] * sizes[1] * sizes[2], theta.shape[1] // (sizes[1] * sizes[2])
    rank = fac.shape[1]
    nb = n_total // B
    n_chip = sizes[0] * sizes[1] * sizes[2]
    assert nb * nb == 4 * n_chip and rank == 4 * nb
    hb = B // 2
    cfg = dict(sizes=sizes, nb=nb, kern_width=kern_width, step_size=step_size)
    n1, n2 = n_chip, n_chip
    vmem = pl.BlockSpec(memory_space=pltpu.VMEM)
    most1 = max(n_chip // sizes[k] for k in range(3))
    most2 = max(sizes)
    blocks = (4, 4, B, fcol)
    scratch = [
        pltpu.VMEM(blocks, F32),
        pltpu.VMEM((2, 4, hb, 4 * fcol), F32),
        pltpu.VMEM((2, 4, 4, hb, fcol), F32),
        pltpu.VMEM((2, 2, hb // 2, 4 * fcol), F32),
        pltpu.VMEM((2, 2, 2, hb, fcol), F32),
        pltpu.VMEM((2, 2, 2, hb, fcol), F32),
        pltpu.VMEM((1, fcol), F32),
        pltpu.VMEM((1, fcol), F32),
        pltpu.VMEM((rank, fcol), BF16),
        pltpu.VMEM((2, n_total, fcol), BF16),
        pltpu.VMEM((n_total, fcol), BF16),
        pltpu.VMEM((n_total, fcol), BF16),
        pltpu.VMEM((rank, n_total), F32),
        pltpu.VMEM((rank // 2, n_total), F32),
        pltpu.VMEM((rank, n_total), F32),
        pltpu.VMEM((nb, 8, B), F32),
        pltpu.VMEM((nb, B, B), F32),
        pltpu.VMEM((3, n_chip, PIECE, B), F32),
        pltpu.VMEM((3, 4, most1, PIECE, B), F32),
        pltpu.VMEM((3, 2, 2, PIECE, B), F32),
        pltpu.VMEM((3, 4, most2, PIECE, B), F32),
        pltpu.VMEM((3, 4, PIECE, B), F32),
        pltpu.VMEM((3, most1, PIECE, B), F32),
        pltpu.VMEM((3, most2, PIECE, B), F32),
        pltpu.VMEM((3, PIECE, B), F32),
        pltpu.VMEM((3, n_chip, PIECE, B), BF16),
        pltpu.VMEM((3, n_chip, PIECE, B), BF16),
        pltpu.VMEM((n_total, n_total), BF16),
        pltpu.SemaphoreType.DMA((NUM_SEMS,)),
        pltpu.SemaphoreType.DMA((NUM_SEMS,)),
    ]
    hbm = pl.BlockSpec(memory_space=pltpu.HBM)
    return pl.pallas_call(
        functools.partial(steps_kernel, cfg),
        out_shape=jax.ShapeDtypeStruct(theta.shape, F32),
        in_specs=[hbm, vmem, vmem, hbm],
        out_specs=hbm,
        scratch_shapes=scratch,
        compiler_params=pltpu.CompilerParams(collective_id=0, has_side_effects=True, vmem_limit_bytes=60 * 1024 * 1024),
        name="svgd_steps",
    )(theta, lam[None], mu[None], fac.T)


def solution(mesh, sizes=(4, 4, 4)):
    part_size = mesh.shape["part"]
    feat_size = mesh.shape["feat"]

    def local_steps(local_theta, prec_loc, mean_loc, factor_loc):
        rows_loc, feat_loc = local_theta.shape
        n_total = rows_loc * part_size
        feat_total = feat_loc * feat_size
        kern_width = 2.0 * feat_total / math.log(n_total)
        step_size = 0.15 * n_total * feat_total / math.log(n_total)
        return run_steps(local_theta, prec_loc, mean_loc, factor_loc, sizes, kern_width, step_size)

    row_spec = P(("ens", "part"), "feat")
    vec_spec = P(("ens", "feat"))
    fac_spec = P(("ens", "feat"), None)
    return jax.shard_map(local_steps, mesh=mesh, in_specs=(row_spec, vec_spec, vec_spec, fac_spec), out_specs=row_spec, check_vma=False)
```

```python
import functools
import math
import jax
import jax.numpy as jnp
from jax import lax
from jax.experimental import pallas as pl
from jax.experimental.pallas import tpu as pltpu
from jax.sharding import PartitionSpec as P

NUM_STEPS = 3
B = 128
PIECE = 48
F32 = jnp.float32
BF16 = jnp.bfloat16
NT = (((1,), (1,)), ((), ()))
TN = (((0,), (0,)), ((), ()))
NUM_SEMS = 416
PANEL = 512


def rem(a, n):
    return lax.rem(a, jnp.int32(n))


def div(a, n):
    return lax.div(a, jnp.int32(n))


def unrolled(count, by, body):
    def several(r, cc):
        for t in range(by):
            body(r * by + t)
        return cc
    lax.fori_loop(0, count // by, several, 0)


def mine(ref, h, v, src_at):
    hb = B // 2
    return ref.at[src_at, v, pl.ds(0, hb)] if h == 0 else ref.at[v, src_at, pl.ds(hb, hb)]


def steps_kernel(cfg, theta_ref, lam_all, mu_all, fact_all, out_ref, th, l1, m1, rel1, rel2, rel3, lam_ref, mu_ref, fact_ref,
                 t_own, t_par, a_buf, zt, zt_par, zt_b, s_all, d_all, g, ring1, relb, dirb, dir3, acc2, acc3, unit, ag,
                 ag_par, kfull, send_sems, recv_sems):
    nb, kern_width, step_size = cfg["nb"], cfg["kern_width"], cfg["step_size"]
    n_total = nb * B
    n_chip = 64
    part, feat = lax.axis_index("part"), lax.axis_index("feat")
    core = rem(feat, 2)
    me = (div(feat, 2), rem(part, 4), div(part, 4))
    near = [[me[d]] + [rem(me[d] + by, 4) for by in (1, 2, 3)] for d in range(3)]

    def dev(coord, c):
        return {"part": coord[2] * 4 + coord[1], "feat": coord[0] * 2 + c}

    def device_at(dim, by):
        c = list(me)
        c[dim] = near[dim][by]
        return dev(c, core)

    around = [[device_at(d, by) for by in range(4)] for d in range(3)]

    def shifted(dim, by):
        return around[dim][by]

    partner = dev(me, 1 - core)
    perms = [(k, (k + 1) % 3, (k + 2) % 3) for k in range(3)]

    ids = {}

    def slot_of(key):
        idx = ids.setdefault(key, len(ids))
        assert idx < NUM_SEMS - 8
        return idx

    def copy(key, src, dst, to):
        idx = slot_of(key)
        return pltpu.make_async_remote_copy(
            src_ref=src, dst_ref=dst, send_sem=send_sems.at[idx], recv_sem=recv_sems.at[idx],
            device_id=to, device_id_type=pl.DeviceIdType.MESH)

    def local(key, src, dst):
        return pltpu.make_async_copy(src, dst, send_sems.at[slot_of(key)])

    barrier = pltpu.get_barrier_semaphore()
    peers = [partner] + [shifted(d, by) for d in range(3) for by in (1, 2, 3)]
    for peer in peers:
        pl.semaphore_signal(barrier, inc=1, device_id=peer, device_id_type=pl.DeviceIdType.MESH)
    pl.semaphore_wait(barrier, len(peers))

    row = lax.broadcasted_iota(jnp.int32, (B, B), 0)
    col = lax.broadcasted_iota(jnp.int32, (B, B), 1)
    low, eye = row >= col, row == col

    def blk(i):
        return pl.ds(pl.multiple_of(i * B, B), B)

    def unit_of(c, q):
        u = c * n_chip + q
        i = rem(u, nb)
        return u, i, rem(i + div(u, nb) + 1, nb), u >= 2 * n_chip - nb // 2

    def chip_index(k, x, y, z):
        p = perms[k]
        c = (x, y, z)
        return (c[p[0]] * 4 + c[p[1]]) * 4 + c[p[2]]

    def split(n, wide):
        if n > 1:
            return (0, n // 2, 0, PIECE), (n // 2, n // 2, 0, PIECE)
        r = 32 if wide else 24
        return (0, 1, 0, r), (0, 1, r, PIECE - r)

    def part_of(ref, lead, base, half):
        return ref.at[lead, pl.ds(base + half[0], half[1]), pl.ds(half[2], half[3])]

    zh = zt.shape[0] // 2
    kc = nb // 4
    n_panels = n_total // PANEL

    def panel(r):
        return pl.ds(pl.multiple_of(r * PANEL, PANEL), PANEL)

    def swap_t(r, slot):
        return pltpu.make_async_remote_copy(
            src_ref=t_own.at[slot, panel(r)], dst_ref=t_par.at[panel(r)], send_sem=send_sems.at[NUM_SEMS - 1 - r],
            recv_sem=recv_sems.at[NUM_SEMS - 1 - r], device_id=partner, device_id_type=pl.DeviceIdType.MESH)

    def swap_z(r):
        return pltpu.make_async_remote_copy(
            src_ref=zt.at[pl.ds(pl.multiple_of((1 - core) * zh, 8), zh), panel(r)], dst_ref=zt_par.at[pl.ds(0, zh), panel(r)],
            send_sem=send_sems.at[NUM_SEMS - 1 - n_panels - r], recv_sem=recv_sems.at[NUM_SEMS - 1 - n_panels - r],
            device_id=partner, device_id_type=pl.DeviceIdType.MESH)

    def prepare(r, theta, slot):
        t_own[slot, panel(r)] = theta.astype(BF16)
        swap_t(r, slot).start()
        xb = (theta - mu_ref[...]).astype(BF16)
        zt[:, panel(r)] = lax.dot_general(fact_ref[...], xb, NT, preferred_element_type=F32)
        swap_z(r).start()

    def get_rows(r):
        return jnp.concatenate([th[r, v] for v in range(4)], 0)

    def first_prep(r, cc):
        prepare(r, get_rows(r), 0)
        return cc
    fcol, hb = fact_ref.shape[1], B // 2
    my = pl.ds(pl.multiple_of((me[1] * 4 + me[2]) * fcol, fcol), fcol)

    def cols(y, z, n=1):
        return pl.ds(pl.multiple_of((y * 4 + z) * fcol, fcol), n * fcol)

    def side(d, by):
        return near[d][by]

    def relayed(key, d, sends):
        def copies(tag):
            return [copy((key, tag, t), src, dst, shifted(d, 1 if tag[1] == "+" else 3))
                    for t, (src, dst) in enumerate(sends(tag))]
        started = []

        def go(tags):
            for tag in tags:
                for m in copies(tag):
                    m.start()
                    started.append(m)

        def relay():
            for got, out in (("r+", "f+"), ("r-", "f-")):
                for m in copies(got):
                    m.wait_recv()
                go((out,))

        def finish():
            for tag in ("d+", "d-", "f+", "f-"):
                for m in copies(tag):
                    m.wait_recv()
        go(("r+", "r-", "d+", "d-"))
        return relay, finish, started

    def halves(tag):
        if tag[0] == "d":
            return (0, 1, 2, 3)
        return (0, 1) if tag[1] == "+" else (2, 3)

    def in_first(h):
        d = 1 + h

        def sends(tag):
            r0, nr = {"r+": (0, hb // 2), "r-": (hb // 2, hb // 2)}.get(tag, (0, hb))
            way = tag[1] == "+"
            if tag[0] == "f":
                b = 0 if way else 1
                return [(rel1.at[h, b], l1.at[h, side(d, 3 if way else 1), pl.ds(b * (hb // 2), hb // 2)])]
            to = side(d, {"r": 2, "d": 1 if way else 3}[tag[0]])
            rows = pl.ds(h * hb + r0, nr)

            def dst(y, n):
                at = pl.ds(y * fcol, n * fcol)
                if tag[0] == "d":
                    return l1.at[h, me[d], pl.ds(0, nr), at]
                return rel1.at[h, 0 if way else 1, pl.ds(0, nr), at]
            if h == 0:
                return [(theta_ref.at[rows, cols(to, 0, 4)], dst(0, 4))]
            return [(theta_ref.at[rows, cols(y, to)], dst(y, 1)) for y in range(4)]
        return relayed(("in1", h), d, sends)

    def in_second(h):
        d = 2 - h

        def sends(tag):
            way = tag[1] == "+"
            b = 0 if way else 1
            if tag[0] == "f":
                return [(rel2.at[h, b, v % 2], mine(th, h, v, side(d, 3 if way else 1))) for v in halves(tag)]
            to = side(d, {"r": 2, "d": 1 if way else 3}[tag[0]])
            at = pl.ds(pl.multiple_of(to * fcol, fcol), fcol)
            return [(l1.at[h, v, pl.ds(0, hb), at], mine(th, h, v, me[d]) if tag[0] == "d" else rel2.at[h, b, v % 2])
                    for v in halves(tag)]
        return relayed(("in2", h), d, sends)

    own_in = [local(("own", 0), theta_ref.at[pl.ds(0, hb), cols(me[1], 0, 4)], l1.at[0, me[1]])]
    own_in += [local(("own", 1 + y), theta_ref.at[pl.ds(hb, hb), cols(y, me[2])],
                     l1.at[1, me[2], pl.ds(0, hb), pl.ds(y * fcol, fcol)]) for y in range(4)]
    own_in.append(local(("own", 5), fact_all.at[pl.ds(0, fact_ref.shape[0]), my], fact_ref))

    with jax.named_scope("in1"):
        first = [in_first(h) for h in range(2)]
        for m in own_in:
            m.start()
        lam_ref[...] = lam_all[pl.ds(0, 1), my]
        mu_ref[...] = mu_all[pl.ds(0, 1), my]
        for relay, finish, started in first:
            relay()
    with jax.named_scope("in2"):
        for m in own_in:
            m.wait()
        second = []
        for h, (relay, finish, started) in enumerate(first):
            finish()
            second.append(in_second(h))
        for v in range(4):
            th[me[2], v, pl.ds(0, hb)] = l1[0, v, pl.ds(0, hb), pl.ds(pl.multiple_of(me[2] * fcol, fcol), fcol)]
            th[v, me[1], pl.ds(hb, hb)] = l1[1, v, pl.ds(0, hb), pl.ds(pl.multiple_of(me[1] * fcol, fcol), fcol)]
        for relay, finish, started in second:
            relay()
        for relay, finish, started in second:
            finish()
        for relay, finish, started in first + second:
            for m in started:
                m.wait_send()
    with jax.named_scope("prep"):
        lax.fori_loop(0, n_panels, first_prep, 0)

    def one_step(step, carry):
        slot = rem(step, 2)
        with jax.named_scope("twait"):
            for r in range(n_panels):
                swap_t(r, slot).wait()
                swap_z(r).wait()

        def products(rows, cols):
            return (lax.dot_general(jnp.concatenate([t_own[slot, r] for r in rows], 0), t_own[slot, cols], NT,
                                    preferred_element_type=F32)
                    + lax.dot_general(jnp.concatenate([t_par[r] for r in rows], 0), t_par[cols], NT,
                                      preferred_element_type=F32))

        def put(m, x, y, z):
            g[0, chip_index(0, x, y, z)] = m[:48]
            g[1, chip_index(1, x, y, z)] = m[48:96]
            g[2, chip_index(2, x, y, z), pl.ds(0, 32)] = m[96:]

        def form(h, cc):
            i = h * 2
            cols = pl.ds(pl.multiple_of(i * B, 2 * B), 2 * B)
            dg = products([cols], cols)
            for t in range(2):
                dt = dg[t * B:(t + 1) * B, t * B:(t + 1) * B]
                d_all[i + t] = dt
                s_all[i + t] = jnp.broadcast_to(jnp.sum(jnp.where(eye, dt, 0.0), axis=0, keepdims=True), (8, B))
            m = products([blk(rem(i + core * kc + 1 + t, nb)) for t in range(kc + 1)], cols)
            y, z = div(h, 2), 2 * rem(h, 2)
            for t in range(kc + 1):
                if t < kc:
                    put(m[t * B:(t + 1) * B, :B], t, y, z)
                if t > 0:
                    put(m[t * B:(t + 1) * B, B:], t - 1, y, z + 1)
            return cc
        with jax.named_scope("form"):
            lax.fori_loop(0, nb // 2, form, 0, unroll=2)

        row8 = lax.broadcasted_iota(jnp.int32, (8, B), 0)

        def tails(i, cc):
            y, z = div(i, 4), rem(i, 4)
            for x in range(4):
                off = core * kc + x
                at = chip_index(2, x, y, z)
                g[2, at, pl.ds(32, 8)] = jnp.where(row8 == 0, s_all[rem(i + off + 1, nb)], s_all[i])
                g[2, at, pl.ds(40, 8)] = (zt[pl.ds(pl.multiple_of(off * 8, 8), 8), blk(i)]
                                          + zt_par[pl.ds(x * 8, 8), blk(i)])
            return cc
        with jax.named_scope("tails"):
            lax.fori_loop(0, nb, tails, 0)

            @pl.when(core == 1)
            def _():
                def pair(t, cc):
                    i = t + nb // 2
                    put(jnp.where(low, d_all[i], d_all[t]), 3, div(i, 4), rem(i, 4))
                    return cc
                lax.fori_loop(0, nb // 2, pair, 0)

        pending = []

        order = (2, 1, 3, 0)
        wave_base = [[[(near[perms[k][0]][t] * 4 + near[perms[k][1]][o]) * 4 for t in range(4)] for o in order]
                     for k in range(3)]

        def wave(k, s):
            return perms[k], 4, order[s], wave_base[k][s]

        def n_waves(k):
            return 4

        def ring_copy(k, s, tag):
            p, n, by, base = wave(k, s)
            ha, hb = split(n, False)
            at, half, kind, to = {
                "m1p": (2, ha, 0, 1), "m1m": (2, hb, 1, 3), "m2p": (1, hb, 2, 1), "m2m": (3, ha, 3, 3),
                "m3p": (1, ha, 2, 1), "m3m": (3, hb, 3, 3)}[tag]
            return copy(("rs", k, s, tag), part_of(g, k, base[at], half), part_of(ring1.at[k], kind, s * n, half),
                        shifted(p[0], to))

        def ring_start(s, tags):
            for tag in tags:
                for k in range(3):
                    if s < n_waves(k):
                        m = ring_copy(k, s, tag)
                        m.start()
                        pending.append(m)

        def ring_merge(s):
            for k in range(3):
                p, n, by, base = wave(k, s)
                ha, hb = split(n, False)
                for got, out, at, half, kind in (("m1p", "m3p", 1, ha, 0), ("m1m", "m3m", 3, hb, 1)):
                    ring_copy(k, s, got).wait_recv()
                    part_of(g, k, base[at], half)[...] += part_of(ring1.at[k], kind, s * n, half)[...]
                    m = ring_copy(k, s, out)
                    m.start()
                    pending.append(m)

        def owner_copy(k, by, s):
            return copy(("rb", k, by), acc2.at[k, pl.ds(s * 4, 4)], dirb.at[k, by], shifted(perms[k][1], by))

        def via_copy(k, b):
            return copy(("rv", k, b), acc2.at[k, pl.ds(2 * b, 2)], relb.at[k, b], shifted(perms[k][1], (1, 3)[b]))

        def ring_finish(s):
            for k in range(3):
                p, n, by, base = wave(k, s)
                for tag in ("m2p", "m2m", "m3p", "m3m"):
                    ring_copy(k, s, tag).wait_recv()
                if by in (1, 3):
                    via_copy(k, by // 2).wait_recv()
                for v in range(n):
                    tot = g[k, base[0] + v] + ring1[k, 2, s * n + v] + ring1[k, 3, s * n + v]
                    if by in (1, 3) and v // 2 == by // 2:
                        tot = tot + relb[k, by // 2, v % 2]
                    acc2[k, s * n + v] = tot
                ms = [via_copy(k, 0), via_copy(k, 1)] if by == 2 else [owner_copy(k, by, s)] if by else []
                for m in ms:
                    m.start()
                    pending.append(m)

        most = 4
        with jax.named_scope("rs0"):
            ring_start(0, ("m1p", "m1m", "m2p", "m2m"))
            ring_start(1, ("m1p", "m1m"))
            for s in range(most):
                ring_merge(s)
                ring_start(s + 1, ("m2p", "m2m"))
                ring_start(s + 2, ("m1p", "m1m"))
                if s:
                    ring_finish(s - 1)
            ring_finish(most - 1)
        last = []
        with jax.named_scope("rs1"):
            for k in range(3):
                p = perms[k]
                n, s = 4, 3
                bys = (1, 3)
                for by in bys:
                    owner_copy(k, by, 0).wait_recv()
                for v in range(n):
                    tot = acc2[k, s * n + v]
                    for by in bys:
                        tot = tot + dirb[k, by, v]
                    acc3[k, v] = tot
                ms = []
                for by in (1, 2, 3):
                    m = copy(("rc", k, by), acc3.at[k, near[p[2]][by]], dir3.at[k, by],
                             shifted(p[2], by))
                    m.start()
                    ms.append(m)
                last.append(ms)
                pending += ms
        with jax.named_scope("rs2"):
            for k in range(3):
                tot = acc3[k, me[perms[k][2]]]
                for m in last[k]:
                    m.wait_recv()
                for by in range(1, len(last[k]) + 1):
                    tot = tot + dir3[k, by]
                unit[k] = tot

        with jax.named_scope("kunit"):
            packed = unit_of(core, (me[0] * 4 + me[1]) * 4 + me[2])[3]
            g_u = jnp.concatenate([unit[0], unit[1], unit[2, pl.ds(0, 32)]], 0)
            sj = jnp.broadcast_to(unit[2, pl.ds(32, 1)], (B, B))
            si = jnp.broadcast_to(unit[2, pl.ds(33, 1)], (B, B))
            si_c = jnp.broadcast_to(jnp.sum(jnp.where(eye, si, 0.0), axis=1, keepdims=True), (B, B))
            sj_c = jnp.broadcast_to(jnp.sum(jnp.where(eye, sj, 0.0), axis=1, keepdims=True), (B, B))
            lower = jnp.logical_and(packed, low)
            upper = jnp.logical_and(packed, jnp.logical_not(low))
            s_sum = jnp.where(lower, si_c, sj_c) + jnp.where(upper, sj, si)
            dist = jnp.maximum(s_sum - 2.0 * g_u, 0.0)
            k_u = jnp.exp(-dist / kern_width)
            z_u = unit[2, pl.ds(40, 8)]
            pieces = (k_u[:48], k_u[48:96], jnp.concatenate([k_u[96:], z_u, jnp.zeros_like(z_u)], 0))
            own = [chip_index(k, *me) for k in range(3)]
            for k in range(3):
                ag[k, own[k]] = pieces[k].astype(BF16)

        def place(ref, c, k, a, b, at):
            for v in range(4):
                coord = [0, 0, 0]
                for d, t in zip(perms[k], (a, b, v)):
                    coord[d] = t
                off = c * kc + coord[0]
                i = coord[1] * 4 + coord[2]
                top = (rem(i + off + 1, nb) + div(off * nb + i, 2 * n_chip - nb // 2) * (nb // 2)) * B + 48 * k
                n = (48, 48, 32)[k]
                kfull[pl.ds(pl.multiple_of(top, 16), n), blk(i)] = ref[k, at + v, pl.ds(0, n)]
                if k == 2:
                    tail = ref[k, at + v, pl.ds(32, 16)].astype(F32)
                    zt_b[pl.ds(pl.multiple_of(off * 8, 8), 8), blk(i)] = tail[:8]

        chunks = {}

        def chunk(k, ta, tb):
            if (k, ta, tb) not in chunks:
                p = perms[k]
                a, b = near[p[0]][ta], near[p[1]][tb]
                chunks[k, ta, tb] = (a, b, (a * 4 + b) * 4, 4)
            return chunks[k, ta, tb]

        def swap(k, ta, tb):
            a, b, at, n = chunk(k, ta, tb)
            return copy(("sw", k, ta, tb), ag.at[k, pl.ds(at, n)], ag_par.at[k, pl.ds(at, n)], partner)

        swaps = []
        placed = []

        def take(upto):
            while len(placed) < upto:
                k, ta, tb = swaps[len(placed)]
                swap(k, ta, tb).wait_recv()
                a, b, at, n = chunk(k, ta, tb)
                place(ag_par, 1 - core, k, a, b, at)
                placed.append((k, ta, tb))

        def have(k, ta, tb):
            swap(k, ta, tb).start()
            swaps.append((k, ta, tb))
            a, b, at, n = chunk(k, ta, tb)
            place(ag, core, k, a, b, at)

        def unit_copy(stage, k, by, tc, start):
            p = perms[k]
            a, b, at, n = chunk(k, 0, 0)
            at = at + near[p[2]][tc]
            m = copy(("u", stage, k, by, tc), ag.at[k, at], ag.at[k, at], shifted(p[stage], by))
            if start:
                m.start()
                pending.append(m)
            return m

        def a_copy(k, tb, tag, start=False):
            p = perms[k]
            ta, h, to = {"n1p": (0, 0, 1), "n1m": (0, 1, 3), "n2p": (0, 1, 1), "n2m": (0, 0, 3), "n3p": (3, 0, 1),
                         "n3m": (1, 1, 3)}[tag]
            a, b, at, n = chunk(k, ta, tb)
            half = split(n, True)[h]
            m = copy(("a", k, tb, tag), part_of(ag, k, at, half), part_of(ag, k, at, half), shifted(p[0], to))
            if start:
                m.start()
                pending.append(m)
            return m

        def a_launch(k, tb):
            for tag in ("n1p", "n1m", "n2p", "n2m"):
                a_copy(k, tb, tag, True)
            have(k, 0, tb)

        def a_relay(tb):
            for k in range(3):
                if True:
                    for got, out in (("n1p", "n3p"), ("n1m", "n3m")):
                        a_copy(k, tb, got).wait_recv()
                        a_copy(k, tb, out, True)

        def a_near(tb):
            for k in range(3):
                if True:
                    for got, ta in (("n2p", 3), ("n2m", 1)):
                        a_copy(k, tb, got).wait_recv()
                        have(k, ta, tb)

        def a_far(tb):
            for k in range(3):
                if True:
                    for got in ("n3p", "n3m"):
                        a_copy(k, tb, got).wait_recv()
                    have(k, 2, tb)

        with jax.named_scope("ag2"):
            for k in range(3):
                for by in (1, 2, 3):
                    unit_copy(2, k, by, 0, True)
            for k in range(3):
                for by in (1, 3):
                    unit_copy(1, k, by, 0, True)
            for k in range(3):
                p = perms[k]
                for by in (1, 2, 3):
                    unit_copy(2, k, by, 0, False).wait_recv()
                    for bb in (1, 3):
                        unit_copy(1, k, bb, 4 - by, True)
                a_launch(k, 0)

        def b_relay(k, b, tc, start):
            at = chunk(k, 0, (3, 1)[b])[2] + near[perms[k][2]][tc]
            m = copy(("ur", k, b, tc), ag.at[k, at], ag.at[k, at], shifted(perms[k][1], (1, 3)[b]))
            if start:
                m.start()
                pending.append(m)
            return m

        relay_tc = ((0, 2), (1, 3))

        def b_arrivals(bb):
            for k in range(3):
                if bb == 2:
                    for b in range(2):
                        for tc in relay_tc[b]:
                            b_relay(k, b, tc, False).wait_recv()
                else:
                    for tc in range(4):
                        unit_copy(1, k, bb, tc, False).wait_recv()
                        if tc in relay_tc[bb // 2]:
                            b_relay(k, bb // 2, tc, True)
                a_launch(k, 4 - bb)

        with jax.named_scope("ag1"):
            for name, stage, at, got in (("r0", a_relay, 0, 0), ("b1", b_arrivals, 1, 0), ("b3", b_arrivals, 3, 0),
                                         ("n0", a_near, 0, 3), ("b2", b_arrivals, 2, 6), ("r3", a_relay, 3, 9),
                                         ("r1", a_relay, 1, 12), ("n3", a_near, 3, 15), ("r2", a_relay, 2, 18)):
                with jax.named_scope("ag1_" + name):
                    stage(at)
                    take(min(got, len(swaps) - 3))
        with jax.named_scope("ag0"):
            for stage, tb in ((a_far, 0), (a_near, 1), (a_far, 3), (a_near, 2), (a_far, 1), (a_far, 2)):
                before = len(swaps)
                with jax.named_scope("ag0_%s%d" % (stage.__name__, tb)):
                    stage(tb)
                take(before - 12)

        per = 4 if nb > 4 else 2

        def mirror(c, r, cc):
            at = []
            for t in range(per):
                u, i, j, packed = unit_of(c, r * per + t)
                at.append((i, j, kfull[blk(j), blk(i)].T))
            for i, j, m in at:
                kfull[blk(i), blk(j)] = m
            return cc

        def unpack(r, cc):
            both = []
            for v in range(4):
                i = r * 4 + v + nb // 2
                m = kfull[blk(i), blk(i)].astype(F32)
                mt = m.T
                both.append((jnp.where(eye, 1.0, jnp.where(low, m, mt)), jnp.where(eye, 1.0, jnp.where(low, mt, m))))
            for v, (m, mt) in enumerate(both):
                t = r * 4 + v
                kfull[blk(t + nb // 2), blk(t + nb // 2)] = m.astype(BF16)
                kfull[blk(t), blk(t)] = mt.astype(BF16)
            return cc
        with jax.named_scope("mirror1"):
            lax.fori_loop(0, div(n_chip - core * (nb // 2), per), functools.partial(mirror, core), 0)
        with jax.named_scope("swapwait"):
            take(len(swaps))
        with jax.named_scope("mirror2"):
            lax.fori_loop(0, div(n_chip - (1 - core) * (nb // 2), per), functools.partial(mirror, 1 - core), 0)
            lax.fori_loop(0, nb // 8, unpack, 0)

        def grads(r, cc):
            lowt = lax.dot_general(zt_b[:, panel(r)].astype(BF16), fact_ref[...], TN, preferred_element_type=F32)
            a_buf[panel(r)] = (-((get_rows(r) - mu_ref[...]) * lam_ref[...] + lowt)).astype(BF16)
            return cc
        with jax.named_scope("grads"):
            lax.fori_loop(0, n_panels, grads, 0)

        def update(r, cc):
            kr = kfull[panel(r)]
            mass = jnp.sum(kr.astype(F32), axis=1, keepdims=True)
            drive = jnp.dot(kr, a_buf[...], preferred_element_type=F32)
            pull = jnp.dot(kr, t_own[slot], preferred_element_type=F32)
            upd = (drive + (2.0 / kern_width) * (mass * t_own[slot, panel(r)].astype(F32) - pull)) / n_total
            theta = get_rows(r) + step_size * upd
            for v in range(4):
                th[r, v] = theta[v * B:(v + 1) * B]

            @pl.when(step < NUM_STEPS - 1)
            def _():
                prepare(r, theta, 1 - slot)
            return cc
        with jax.named_scope("update"):
            lax.fori_loop(0, n_panels, update, 0)
        with jax.named_scope("sendwait"):
            for m in pending:
                m.wait_send()
            for k, ta, tb in swaps:
                swap(k, ta, tb).wait_send()
        return carry

    lax.fori_loop(0, NUM_STEPS, one_step, 0)

    def out_first(h):
        d = 2 - h

        def sends(tag):
            way = tag[1] == "+"
            b = 0 if way else 1
            if tag[0] == "f":
                return [(rel2.at[h, b, v % 2], m1.at[h, side(d, 3 if way else 1), v]) for v in halves(tag)]
            to = side(d, {"r": 2, "d": 1 if way else 3}[tag[0]])
            return [(mine(th, h, v, to), m1.at[h, me[d], v] if tag[0] == "d" else rel2.at[h, b, v % 2])
                    for v in halves(tag)]
        return relayed(("out1", h), d, sends)

    def out_second(h):
        d = 1 + h

        def place_of(src_at, v):
            return out_ref.at[pl.ds(h * hb, hb), cols(src_at, v) if h == 0 else cols(v, src_at)]

        def sends(tag):
            way = tag[1] == "+"
            b = 0 if way else 1
            if tag[0] == "f":
                return [(rel3.at[h, b, t], place_of(side(d, 3 if way else 1), 2 * b + t)) for t in range(2)]
            to = side(d, {"r": 2, "d": 1 if way else 3}[tag[0]])
            if tag[0] == "r":
                return [(m1.at[h, v, to], rel3.at[h, b, v % 2]) for v in halves(tag)]
            return [(m1.at[h, v, to], place_of(me[d], v)) for v in range(4)]
        return relayed(("out2", h), d, sends)

    with jax.named_scope("out1"):
        first = [out_first(h) for h in range(2)]
        for v in range(4):
            m1[0, me[2], v] = th[me[2], v, pl.ds(0, hb)]
            m1[1, me[1], v] = th[v, me[1], pl.ds(hb, hb)]
        for relay, finish, started in first:
            relay()
    with jax.named_scope("out2"):
        second = []
        for h, (relay, finish, started) in enumerate(first):
            finish()
            second.append(out_second(h))
        own_out = []
        for v in range(4):
            own_out.append(local(("back", v), m1.at[0, v, me[1]], out_ref.at[pl.ds(0, hb), cols(me[1], v)]))
            own_out.append(local(("back", 4 + v), m1.at[1, v, me[2]], out_ref.at[pl.ds(hb, hb), cols(v, me[2])]))
        for m in own_out:
            m.start()
        for relay, finish, started in second:
            relay()
        for relay, finish, started in second:
            finish()
        for relay, finish, started in first + second:
            for m in started:
                m.wait_send()
        for m in own_out:
            m.wait()


def run_steps(theta, lam, mu, fac, sizes, kern_width, step_size):
    n_total, fcol = theta.shape[0] * sizes[1] * sizes[2], theta.shape[1] // (sizes[1] * sizes[2])
    rank = fac.shape[1]
    nb = n_total // B
    n_chip = sizes[0] * sizes[1] * sizes[2]
    assert nb * nb == 4 * n_chip and rank == 4 * nb
    hb = B // 2
    cfg = dict(sizes=sizes, nb=nb, kern_width=kern_width, step_size=step_size)
    n1, n2 = n_chip, n_chip
    vmem = pl.BlockSpec(memory_space=pltpu.VMEM)
    most1 = max(n_chip // sizes[k] for k in range(3))
    most2 = max(sizes)
    blocks = (4, 4, B, fcol)
    scratch = [
        pltpu.VMEM(blocks, F32),
        pltpu.VMEM((2, 4, hb, 4 * fcol), F32),
        pltpu.VMEM((2, 4, 4, hb, fcol), F32),
        pltpu.VMEM((2, 2, hb // 2, 4 * fcol), F32),
        pltpu.VMEM((2, 2, 2, hb, fcol), F32),
        pltpu.VMEM((2, 2, 2, hb, fcol), F32),
        pltpu.VMEM((1, fcol), F32),
        pltpu.VMEM((1, fcol), F32),
        pltpu.VMEM((rank, fcol), BF16),
        pltpu.VMEM((2, n_total, fcol), BF16),
        pltpu.VMEM((n_total, fcol), BF16),
        pltpu.VMEM((n_total, fcol), BF16),
        pltpu.VMEM((rank, n_total), F32),
        pltpu.VMEM((rank // 2, n_total), F32),
        pltpu.VMEM((rank, n_total), F32),
        pltpu.VMEM((nb, 8, B), F32),
        pltpu.VMEM((nb, B, B), F32),
        pltpu.VMEM((3, n_chip, PIECE, B), F32),
        pltpu.VMEM((3, 4, most1, PIECE, B), F32),
        pltpu.VMEM((3, 2, 2, PIECE, B), F32),
        pltpu.VMEM((3, 4, most2, PIECE, B), F32),
        pltpu.VMEM((3, 4, PIECE, B), F32),
        pltpu.VMEM((3, most1, PIECE, B), F32),
        pltpu.VMEM((3, most2, PIECE, B), F32),
        pltpu.VMEM((3, PIECE, B), F32),
        pltpu.VMEM((3, n_chip, PIECE, B), BF16),
        pltpu.VMEM((3, n_chip, PIECE, B), BF16),
        pltpu.VMEM((n_total, n_total), BF16),
        pltpu.SemaphoreType.DMA((NUM_SEMS,)),
        pltpu.SemaphoreType.DMA((NUM_SEMS,)),
    ]
    hbm = pl.BlockSpec(memory_space=pltpu.HBM)
    return pl.pallas_call(
        functools.partial(steps_kernel, cfg),
        out_shape=jax.ShapeDtypeStruct(theta.shape, F32),
        in_specs=[hbm, vmem, vmem, hbm],
        out_specs=hbm,
        scratch_shapes=scratch,
        compiler_params=pltpu.CompilerParams(collective_id=0, has_side_effects=True, vmem_limit_bytes=60 * 1024 * 1024),
        name="svgd_steps",
    )(theta, lam[None], mu[None], fac.T)


def solution(mesh, sizes=(4, 4, 4)):
    part_size = mesh.shape["part"]
    feat_size = mesh.shape["feat"]

    def local_steps(local_theta, prec_loc, mean_loc, factor_loc):
        rows_loc, feat_loc = local_theta.shape
        n_total = rows_loc * part_size
        feat_total = feat_loc * feat_size
        kern_width = 2.0 * feat_total / math.log(n_total)
        step_size = 0.15 * n_total * feat_total / math.log(n_total)
        return run_steps(local_theta, prec_loc, mean_loc, factor_loc, sizes, kern_width, step_size)

    row_spec = P(("ens", "part"), "feat")
    vec_spec = P(("ens", "feat"))
    fac_spec = P(("ens", "feat"), None)
    return jax.shard_map(local_steps, mesh=mesh, in_specs=(row_spec, vec_spec, vec_spec, fac_spec), out_specs=row_spec, check_vma=False)
```

```python
import functools
import math
import jax
import jax.numpy as jnp
from jax import lax
from jax.experimental import pallas as pl
from jax.experimental.pallas import tpu as pltpu
from jax.sharding import PartitionSpec as P

NUM_STEPS = 3
B = 128
PIECE = 48
F32 = jnp.float32
BF16 = jnp.bfloat16
NT = (((1,), (1,)), ((), ()))
TN = (((0,), (0,)), ((), ()))
NUM_SEMS = 416
PANEL = 512


def rem(a, n):
    return lax.rem(a, jnp.int32(n))


def div(a, n):
    return lax.div(a, jnp.int32(n))


def unrolled(count, by, body):
    def several(r, cc):
        for t in range(by):
            body(r * by + t)
        return cc
    lax.fori_loop(0, count // by, several, 0)


def mine(ref, h, v, src_at):
    hb = B // 2
    return ref.at[src_at, v, pl.ds(0, hb)] if h == 0 else ref.at[v, src_at, pl.ds(hb, hb)]


def steps_kernel(cfg, theta_ref, lam_all, mu_all, fact_all, out_ref, th, l1, m1, rel1, rel2, rel3, lam_ref, mu_ref, fact_ref,
                 t_own, t_par, a_buf, zt, zt_par, zt_b, s_all, d_all, g, ring1, relb, dirb, dir3, acc2, acc3, unit, ag,
                 ag_par, kfull, send_sems, recv_sems):
    nb, kern_width, step_size = cfg["nb"], cfg["kern_width"], cfg["step_size"]
    n_total = nb * B
    n_chip = 64
    part, feat = lax.axis_index("part"), lax.axis_index("feat")
    core = rem(feat, 2)
    me = (div(feat, 2), rem(part, 4), div(part, 4))
    near = [[me[d]] + [rem(me[d] + by, 4) for by in (1, 2, 3)] for d in range(3)]

    def dev(coord, c):
        return {"part": coord[2] * 4 + coord[1], "feat": coord[0] * 2 + c}

    def device_at(dim, by):
        c = list(me)
        c[dim] = near[dim][by]
        return dev(c, core)

    around = [[device_at(d, by) for by in range(4)] for d in range(3)]

    def shifted(dim, by):
        return around[dim][by]

    partner = dev(me, 1 - core)
    perms = [(k, (k + 1) % 3, (k + 2) % 3) for k in range(3)]

    ids = {}

    def slot_of(key):
        idx = ids.setdefault(key, len(ids))
        assert idx < NUM_SEMS - 8
        return idx

    def copy(key, src, dst, to):
        idx = slot_of(key)
        return pltpu.make_async_remote_copy(
            src_ref=src, dst_ref=dst, send_sem=send_sems.at[idx], recv_sem=recv_sems.at[idx],
            device_id=to, device_id_type=pl.DeviceIdType.MESH)

    def local(key, src, dst):
        return pltpu.make_async_copy(src, dst, send_sems.at[slot_of(key)])

    barrier = pltpu.get_barrier_semaphore()
    peers = [partner] + [shifted(d, by) for d in range(3) for by in (1, 2, 3)]
    for peer in peers:
        pl.semaphore_signal(barrier, inc=1, device_id=peer, device_id_type=pl.DeviceIdType.MESH)
    pl.semaphore_wait(barrier, len(peers))

    row = lax.broadcasted_iota(jnp.int32, (B, B), 0)
    col = lax.broadcasted_iota(jnp.int32, (B, B), 1)
    low, eye = row >= col, row == col

    def blk(i):
        return pl.ds(pl.multiple_of(i * B, B), B)

    def unit_of(c, q):
        u = c * n_chip + q
        i = rem(u, nb)
        return u, i, rem(i + div(u, nb) + 1, nb), u >= 2 * n_chip - nb // 2

    def chip_index(k, x, y, z):
        p = perms[k]
        c = (x, y, z)
        return (c[p[0]] * 4 + c[p[1]]) * 4 + c[p[2]]

    def split(n, wide):
        if n > 1:
            return (0, n // 2, 0, PIECE), (n // 2, n // 2, 0, PIECE)
        r = 32 if wide else 24
        return (0, 1, 0, r), (0, 1, r, PIECE - r)

    def part_of(ref, lead, base, half):
        return ref.at[lead, pl.ds(base + half[0], half[1]), pl.ds(half[2], half[3])]

    zh = zt.shape[0] // 2
    kc = nb // 4
    n_panels = n_total // PANEL

    def panel(r):
        return pl.ds(pl.multiple_of(r * PANEL, PANEL), PANEL)

    def swap_t(r, slot):
        return pltpu.make_async_remote_copy(
            src_ref=t_own.at[slot, panel(r)], dst_ref=t_par.at[panel(r)], send_sem=send_sems.at[NUM_SEMS - 1 - r],
            recv_sem=recv_sems.at[NUM_SEMS - 1 - r], device_id=partner, device_id_type=pl.DeviceIdType.MESH)

    def swap_z(r):
        return pltpu.make_async_remote_copy(
            src_ref=zt.at[pl.ds(pl.multiple_of((1 - core) * zh, 8), zh), panel(r)], dst_ref=zt_par.at[pl.ds(0, zh), panel(r)],
            send_sem=send_sems.at[NUM_SEMS - 1 - n_panels - r], recv_sem=recv_sems.at[NUM_SEMS - 1 - n_panels - r],
            device_id=partner, device_id_type=pl.DeviceIdType.MESH)

    def prepare(r, theta, slot):
        t_own[slot, panel(r)] = theta.astype(BF16)
        swap_t(r, slot).start()
        xb = (theta - mu_ref[...]).astype(BF16)
        zt[:, panel(r)] = lax.dot_general(fact_ref[...], xb, NT, preferred_element_type=F32)
        swap_z(r).start()

    def get_rows(r):
        return jnp.concatenate([th[r, v] for v in range(4)], 0)

    def first_prep(r, cc):
        prepare(r, get_rows(r), 0)
        return cc
    fcol, hb = fact_ref.shape[1], B // 2
    my = pl.ds(pl.multiple_of((me[1] * 4 + me[2]) * fcol, fcol), fcol)

    def cols(y, z, n=1):
        return pl.ds(pl.multiple_of((y * 4 + z) * fcol, fcol), n * fcol)

    def side(d, by):
        return near[d][by]

    def relayed(key, d, sends, begin=True):
        def copies(tag):
            return [copy((key, tag, t), src, dst, shifted(d, 1 if tag[1] == "+" else 3))
                    for t, (src, dst) in enumerate(sends(tag))]
        started = []

        def go(tags):
            for tag in tags:
                for m in copies(tag):
                    m.start()
                    started.append(m)

        def relay():
            for got, out in (("r+", "f+"), ("r-", "f-")):
                for m in copies(got):
                    m.wait_recv()
                go((out,))

        def finish():
            for tag in ("d+", "d-", "f+", "f-"):
                for m in copies(tag):
                    m.wait_recv()
        if begin:
            go(("r+", "r-", "d+", "d-"))
        else:
            for tag in ("r+", "r-", "d+", "d-"):
                started += copies(tag)
        return (relay, finish, started) if begin else (relay, finish, started, copies)

    def halves(tag):
        if tag[0] == "d":
            return (0, 1, 2, 3)
        return (0, 1) if tag[1] == "+" else (2, 3)

    def in_first(h):
        d = 1 + h

        def sends(tag):
            r0, nr = {"r+": (0, hb // 2), "r-": (hb // 2, hb // 2)}.get(tag, (0, hb))
            way = tag[1] == "+"
            if tag[0] == "f":
                b = 0 if way else 1
                return [(rel1.at[h, b], l1.at[h, side(d, 3 if way else 1), pl.ds(b * (hb // 2), hb // 2)])]
            to = side(d, {"r": 2, "d": 1 if way else 3}[tag[0]])
            rows = pl.ds(h * hb + r0, nr)

            def dst(y, n):
                at = pl.ds(y * fcol, n * fcol)
                if tag[0] == "d":
                    return l1.at[h, me[d], pl.ds(0, nr), at]
                return rel1.at[h, 0 if way else 1, pl.ds(0, nr), at]
            if h == 0:
                return [(theta_ref.at[rows, cols(to, 0, 4)], dst(0, 4))]
            return [(theta_ref.at[rows, cols(y, to)], dst(y, 1)) for y in range(4)]
        return relayed(("in1", h), d, sends)

    def in_second(h):
        d = 2 - h

        def sends(tag):
            way = tag[1] == "+"
            b = 0 if way else 1
            if tag[0] == "f":
                return [(rel2.at[h, b, v % 2], mine(th, h, v, side(d, 3 if way else 1))) for v in halves(tag)]
            to = side(d, {"r": 2, "d": 1 if way else 3}[tag[0]])
            at = pl.ds(pl.multiple_of(to * fcol, fcol), fcol)
            return [(l1.at[h, v, pl.ds(0, hb), at], mine(th, h, v, me[d]) if tag[0] == "d" else rel2.at[h, b, v % 2])
                    for v in halves(tag)]
        return relayed(("in2", h), d, sends)

    own_in = [local(("own", 0), theta_ref.at[pl.ds(0, hb), cols(me[1], 0, 4)], l1.at[0, me[1]])]
    own_in += [local(("own", 1 + y), theta_ref.at[pl.ds(hb, hb), cols(y, me[2])],
                     l1.at[1, me[2], pl.ds(0, hb), pl.ds(y * fcol, fcol)]) for y in range(4)]
    own_in.append(local(("own", 5), fact_all.at[pl.ds(0, fact_ref.shape[0]), my], fact_ref))

    with jax.named_scope("in1"):
        first = [in_first(h) for h in range(2)]
        for m in own_in:
            m.start()
        lam_ref[...] = lam_all[pl.ds(0, 1), my]
        mu_ref[...] = mu_all[pl.ds(0, 1), my]
        for relay, finish, started in first:
            relay()
    with jax.named_scope("in2"):
        for m in own_in:
            m.wait()
        second = []
        for h, (relay, finish, started) in enumerate(first):
            finish()
            second.append(in_second(h))
        for v in range(4):
            th[me[2], v, pl.ds(0, hb)] = l1[0, v, pl.ds(0, hb), pl.ds(pl.multiple_of(me[2] * fcol, fcol), fcol)]
            th[v, me[1], pl.ds(hb, hb)] = l1[1, v, pl.ds(0, hb), pl.ds(pl.multiple_of(me[1] * fcol, fcol), fcol)]
        for relay, finish, started in second:
            relay()
        for relay, finish, started in second:
            finish()
        for relay, finish, started in first + second:
            for m in started:
                m.wait_send()
    with jax.named_scope("prep"):
        lax.fori_loop(0, n_panels, first_prep, 0)

    def out_pieces(h, tag):
        if h == 0:
            return halves(tag)
        return (0, 1, 2, 3) if tag[0] == "d" else (2, 3) if tag[1] == "+" else (0, 1)

    def out_first(h):
        d = 2 - h

        def sends(tag):
            way = tag[1] == "+"
            b = 0 if way else 1
            vs = [(v if h == 0 else near[2][v], v % 2) for v in out_pieces(h, tag)]
            if tag[0] == "f":
                return [(rel2.at[h, b, at], m1.at[h, side(d, 3 if way else 1), v]) for v, at in vs]
            to = side(d, {"r": 2, "d": 1 if way else 3}[tag[0]])
            return [(mine(th, h, v, to), m1.at[h, me[d], v] if tag[0] == "d" else rel2.at[h, b, at]) for v, at in vs]
        return relayed(("out1", h), d, sends, begin=False)

    def out_start(o):
        for tag in ((), ("d+",), ("r+", "r-"), ("d-",))[o]:
            for m in out_first(0)[3](tag):
                m.start()
        for tag in ("r+" if o >= 2 else "r-", "d+", "d-"):
            out_first(1)[3](tag)[out_pieces(1, tag).index(o)].start()

    def one_step(step, carry):
        slot = rem(step, 2)
        with jax.named_scope("twait"):
            for r in range(n_panels):
                swap_t(r, slot).wait()
                swap_z(r).wait()

        def products(rows, cols):
            return (lax.dot_general(jnp.concatenate([t_own[slot, r] for r in rows], 0), t_own[slot, cols], NT,
                                    preferred_element_type=F32)
                    + lax.dot_general(jnp.concatenate([t_par[r] for r in rows], 0), t_par[cols], NT,
                                      preferred_element_type=F32))

        def put(m, x, y, z):
            g[0, chip_index(0, x, y, z)] = m[:48]
            g[1, chip_index(1, x, y, z)] = m[48:96]
            g[2, chip_index(2, x, y, z), pl.ds(0, 32)] = m[96:]

        def form(h, cc):
            i = h * 2
            cols = pl.ds(pl.multiple_of(i * B, 2 * B), 2 * B)
            dg = products([cols], cols)
            for t in range(2):
                dt = dg[t * B:(t + 1) * B, t * B:(t + 1) * B]
                d_all[i + t] = dt
                s_all[i + t] = jnp.broadcast_to(jnp.sum(jnp.where(eye, dt, 0.0), axis=0, keepdims=True), (8, B))
            m = products([blk(rem(i + core * kc + 1 + t, nb)) for t in range(kc + 1)], cols)
            y, z = div(h, 2), 2 * rem(h, 2)
            for t in range(kc + 1):
                if t < kc:
                    put(m[t * B:(t + 1) * B, :B], t, y, z)
                if t > 0:
                    put(m[t * B:(t + 1) * B, B:], t - 1, y, z + 1)
            return cc
        with jax.named_scope("form"):
            lax.fori_loop(0, nb // 2, form, 0, unroll=2)

        row8 = lax.broadcasted_iota(jnp.int32, (8, B), 0)

        def tails(i, cc):
            y, z = div(i, 4), rem(i, 4)
            for x in range(4):
                off = core * kc + x
                at = chip_index(2, x, y, z)
                g[2, at, pl.ds(32, 8)] = jnp.where(row8 == 0, s_all[rem(i + off + 1, nb)], s_all[i])
                g[2, at, pl.ds(40, 8)] = (zt[pl.ds(pl.multiple_of(off * 8, 8), 8), blk(i)]
                                          + zt_par[pl.ds(x * 8, 8), blk(i)])
            return cc
        with jax.named_scope("tails"):
            lax.fori_loop(0, nb, tails, 0)

            @pl.when(core == 1)
            def _():
                def pair(t, cc):
                    i = t + nb // 2
                    put(jnp.where(low, d_all[i], d_all[t]), 3, div(i, 4), rem(i, 4))
                    return cc
                lax.fori_loop(0, nb // 2, pair, 0)

        pending = []

        order = (2, 1, 3, 0)
        wave_base = [[[(near[perms[k][0]][t] * 4 + near[perms[k][1]][o]) * 4 for t in range(4)] for o in order]
                     for k in range(3)]

        def wave(k, s):
            return perms[k], 4, order[s], wave_base[k][s]

        def n_waves(k):
            return 4

        def ring_copy(k, s, tag):
            p, n, by, base = wave(k, s)
            ha, hb = split(n, False)
            at, half, kind, to = {
                "m1p": (2, ha, 0, 1), "m1m": (2, hb, 1, 3), "m2p": (1, hb, 2, 1), "m2m": (3, ha, 3, 3),
                "m3p": (1, ha, 2, 1), "m3m": (3, hb, 3, 3)}[tag]
            return copy(("rs", k, s, tag), part_of(g, k, base[at], half), part_of(ring1.at[k], kind, s * n, half),
                        shifted(p[0], to))

        def ring_start(s, tags):
            for tag in tags:
                for k in range(3):
                    if s < n_waves(k):
                        m = ring_copy(k, s, tag)
                        m.start()
                        pending.append(m)

        def ring_merge(s):
            for k in range(3):
                p, n, by, base = wave(k, s)
                ha, hb = split(n, False)
                for got, out, at, half, kind in (("m1p", "m3p", 1, ha, 0), ("m1m", "m3m", 3, hb, 1)):
                    ring_copy(k, s, got).wait_recv()
                    part_of(g, k, base[at], half)[...] += part_of(ring1.at[k], kind, s * n, half)[...]
                    m = ring_copy(k, s, out)
                    m.start()
                    pending.append(m)

        def owner_copy(k, by, s):
            return copy(("rb", k, by), acc2.at[k, pl.ds(s * 4, 4)], dirb.at[k, by], shifted(perms[k][1], by))

        def via_copy(k, b):
            return copy(("rv", k, b), acc2.at[k, pl.ds(2 * b, 2)], relb.at[k, b], shifted(perms[k][1], (1, 3)[b]))

        def ring_finish(s):
            for k in range(3):
                p, n, by, base = wave(k, s)
                for tag in ("m2p", "m2m", "m3p", "m3m"):
                    ring_copy(k, s, tag).wait_recv()
                if by in (1, 3):
                    via_copy(k, by // 2).wait_recv()
                for v in range(n):
                    tot = g[k, base[0] + v] + ring1[k, 2, s * n + v] + ring1[k, 3, s * n + v]
                    if by in (1, 3) and v // 2 == by // 2:
                        tot = tot + relb[k, by // 2, v % 2]
                    acc2[k, s * n + v] = tot
                ms = [via_copy(k, 0), via_copy(k, 1)] if by == 2 else [owner_copy(k, by, s)] if by else []
                for m in ms:
                    m.start()
                    pending.append(m)

        most = 4
        with jax.named_scope("rs0"):
            ring_start(0, ("m1p", "m1m", "m2p", "m2m"))
            ring_start(1, ("m1p", "m1m"))
            for s in range(most):
                ring_merge(s)
                ring_start(s + 1, ("m2p", "m2m"))
                ring_start(s + 2, ("m1p", "m1m"))
                if s:
                    ring_finish(s - 1)
            ring_finish(most - 1)
        last = []
        with jax.named_scope("rs1"):
            for k in range(3):
                p = perms[k]
                n, s = 4, 3
                bys = (1, 3)
                for by in bys:
                    owner_copy(k, by, 0).wait_recv()
                for v in range(n):
                    tot = acc2[k, s * n + v]
                    for by in bys:
                        tot = tot + dirb[k, by, v]
                    acc3[k, v] = tot
                ms = []
                for by in (1, 2, 3):
                    m = copy(("rc", k, by), acc3.at[k, near[p[2]][by]], dir3.at[k, by],
                             shifted(p[2], by))
                    m.start()
                    ms.append(m)
                last.append(ms)
                pending += ms
        with jax.named_scope("rs2"):
            for k in range(3):
                tot = acc3[k, me[perms[k][2]]]
                for m in last[k]:
                    m.wait_recv()
                for by in range(1, len(last[k]) + 1):
                    tot = tot + dir3[k, by]
                unit[k] = tot

        with jax.named_scope("kunit"):
            packed = unit_of(core, (me[0] * 4 + me[1]) * 4 + me[2])[3]
            g_u = jnp.concatenate([unit[0], unit[1], unit[2, pl.ds(0, 32)]], 0)
            sj = jnp.broadcast_to(unit[2, pl.ds(32, 1)], (B, B))
            si = jnp.broadcast_to(unit[2, pl.ds(33, 1)], (B, B))
            si_c = jnp.broadcast_to(jnp.sum(jnp.where(eye, si, 0.0), axis=1, keepdims=True), (B, B))
            sj_c = jnp.broadcast_to(jnp.sum(jnp.where(eye, sj, 0.0), axis=1, keepdims=True), (B, B))
            lower = jnp.logical_and(packed, low)
            upper = jnp.logical_and(packed, jnp.logical_not(low))
            s_sum = jnp.where(lower, si_c, sj_c) + jnp.where(upper, sj, si)
            dist = jnp.maximum(s_sum - 2.0 * g_u, 0.0)
            k_u = jnp.exp(-dist / kern_width)
            z_u = unit[2, pl.ds(40, 8)]
            pieces = (k_u[:48], k_u[48:96], jnp.concatenate([k_u[96:], z_u, jnp.zeros_like(z_u)], 0))
            own = [chip_index(k, *me) for k in range(3)]
            for k in range(3):
                ag[k, own[k]] = pieces[k].astype(BF16)

        def place(ref, c, k, a, b, at):
            for v in range(4):
                coord = [0, 0, 0]
                for d, t in zip(perms[k], (a, b, v)):
                    coord[d] = t
                off = c * kc + coord[0]
                i = coord[1] * 4 + coord[2]
                top = (rem(i + off + 1, nb) + div(off * nb + i, 2 * n_chip - nb // 2) * (nb // 2)) * B + 48 * k
                n = (48, 48, 32)[k]
                kfull[pl.ds(pl.multiple_of(top, 16), n), blk(i)] = ref[k, at + v, pl.ds(0, n)]
                if k == 2:
                    tail = ref[k, at + v, pl.ds(32, 16)].astype(F32)
                    zt_b[pl.ds(pl.multiple_of(off * 8, 8), 8), blk(i)] = tail[:8]

        chunks = {}

        def chunk(k, ta, tb):
            if (k, ta, tb) not in chunks:
                p = perms[k]
                a, b = near[p[0]][ta], near[p[1]][tb]
                chunks[k, ta, tb] = (a, b, (a * 4 + b) * 4, 4)
            return chunks[k, ta, tb]

        def swap(k, ta, tb):
            a, b, at, n = chunk(k, ta, tb)
            return copy(("sw", k, ta, tb), ag.at[k, pl.ds(at, n)], ag_par.at[k, pl.ds(at, n)], partner)

        swaps = []
        placed = []

        def take(upto):
            while len(placed) < upto:
                k, ta, tb = swaps[len(placed)]
                swap(k, ta, tb).wait_recv()
                a, b, at, n = chunk(k, ta, tb)
                place(ag_par, 1 - core, k, a, b, at)
                placed.append((k, ta, tb))

        def have(k, ta, tb):
            swap(k, ta, tb).start()
            swaps.append((k, ta, tb))
            a, b, at, n = chunk(k, ta, tb)
            place(ag, core, k, a, b, at)

        def unit_copy(stage, k, by, tc, start):
            p = perms[k]
            a, b, at, n = chunk(k, 0, 0)
            at = at + near[p[2]][tc]
            m = copy(("u", stage, k, by, tc), ag.at[k, at], ag.at[k, at], shifted(p[stage], by))
            if start:
                m.start()
                pending.append(m)
            return m

        def a_copy(k, tb, tag, start=False):
            p = perms[k]
            ta, h, to = {"n1p": (0, 0, 1), "n1m": (0, 1, 3), "n2p": (0, 1, 1), "n2m": (0, 0, 3), "n3p": (3, 0, 1),
                         "n3m": (1, 1, 3)}[tag]
            a, b, at, n = chunk(k, ta, tb)
            half = split(n, True)[h]
            m = copy(("a", k, tb, tag), part_of(ag, k, at, half), part_of(ag, k, at, half), shifted(p[0], to))
            if start:
                m.start()
                pending.append(m)
            return m

        def a_launch(k, tb):
            for tag in ("n1p", "n1m", "n2p", "n2m"):
                a_copy(k, tb, tag, True)
            have(k, 0, tb)

        def a_relay(tb):
            for k in range(3):
                if True:
                    for got, out in (("n1p", "n3p"), ("n1m", "n3m")):
                        a_copy(k, tb, got).wait_recv()
                        a_copy(k, tb, out, True)

        def a_near(tb):
            for k in range(3):
                if True:
                    for got, ta in (("n2p", 3), ("n2m", 1)):
                        a_copy(k, tb, got).wait_recv()
                        have(k, ta, tb)

        def a_far(tb):
            for k in range(3):
                if True:
                    for got in ("n3p", "n3m"):
                        a_copy(k, tb, got).wait_recv()
                    have(k, 2, tb)

        with jax.named_scope("ag2"):
            for k in range(3):
                for by in (1, 2, 3):
                    unit_copy(2, k, by, 0, True)
            for k in range(3):
                for by in (1, 3):
                    unit_copy(1, k, by, 0, True)
            for by in (1, 3, 2):
                for k in range(3):
                    unit_copy(2, k, by, 0, False).wait_recv()
                    for bb in (1, 3):
                        unit_copy(1, k, bb, 4 - by, True)
            for k in range(3):
                a_launch(k, 0)

        def b_relay(k, b, tc, start):
            at = chunk(k, 0, (3, 1)[b])[2] + near[perms[k][2]][tc]
            m = copy(("ur", k, b, tc), ag.at[k, at], ag.at[k, at], shifted(perms[k][1], (1, 3)[b]))
            if start:
                m.start()
                pending.append(m)
            return m

        relay_tc = ((0, 2), (1, 3))

        def b_arrivals(bb):
            for k in range(3):
                if bb == 2:
                    for b in range(2):
                        for tc in relay_tc[b]:
                            b_relay(k, b, tc, False).wait_recv()
                else:
                    for tc in range(4):
                        unit_copy(1, k, bb, tc, False).wait_recv()
                        if tc in relay_tc[bb // 2]:
                            b_relay(k, bb // 2, tc, True)

        def a_waves(tbs):
            for tb in tbs:
                for k in range(3):
                    a_launch(k, tb)

        with jax.named_scope("ag1"):
            for name, stage, at, got in (("b1", b_arrivals, 1, 0), ("b3", b_arrivals, 3, 0), ("r0", a_relay, 0, 0),
                                         ("w", a_waves, (3, 1), 0), ("n0", a_near, 0, 3), ("b2", b_arrivals, 2, 6),
                                         ("w2", a_waves, (2,), 6), ("r3", a_relay, 3, 9), ("r1", a_relay, 1, 12),
                                         ("n3", a_near, 3, 15), ("r2", a_relay, 2, 18)):
                with jax.named_scope("ag1_" + name):
                    stage(at)
                    take(min(got, len(swaps) - 3))
        with jax.named_scope("ag0"):
            for stage, tb in ((a_far, 0), (a_near, 1), (a_far, 3), (a_near, 2), (a_far, 1), (a_far, 2)):
                before = len(swaps)
                with jax.named_scope("ag0_%s%d" % (stage.__name__, tb)):
                    stage(tb)
                take(before - 12)

        per = 4 if nb > 4 else 2

        def mirror(c, r, cc):
            at = []
            for t in range(per):
                u, i, j, packed = unit_of(c, r * per + t)
                at.append((i, j, kfull[blk(j), blk(i)].T))
            for i, j, m in at:
                kfull[blk(i), blk(j)] = m
            return cc

        def unpack(r, cc):
            both = []
            for v in range(4):
                i = r * 4 + v + nb // 2
                m = kfull[blk(i), blk(i)].astype(F32)
                mt = m.T
                both.append((jnp.where(eye, 1.0, jnp.where(low, m, mt)), jnp.where(eye, 1.0, jnp.where(low, mt, m))))
            for v, (m, mt) in enumerate(both):
                t = r * 4 + v
                kfull[blk(t + nb // 2), blk(t + nb // 2)] = m.astype(BF16)
                kfull[blk(t), blk(t)] = mt.astype(BF16)
            return cc
        with jax.named_scope("mirror1"):
            lax.fori_loop(0, div(n_chip - core * (nb // 2), per), functools.partial(mirror, core), 0)
        with jax.named_scope("swapwait"):
            take(len(swaps))
        with jax.named_scope("mirror2"):
            lax.fori_loop(0, div(n_chip - (1 - core) * (nb // 2), per), functools.partial(mirror, 1 - core), 0)
            lax.fori_loop(0, nb // 8, unpack, 0)

        def grads(r, cc):
            lowt = lax.dot_general(zt_b[:, panel(r)].astype(BF16), fact_ref[...], TN, preferred_element_type=F32)
            a_buf[panel(r)] = (-((get_rows(r) - mu_ref[...]) * lam_ref[...] + lowt)).astype(BF16)
            return cc
        with jax.named_scope("grads"):
            lax.fori_loop(0, n_panels, grads, 0)

        def update(t, cc):
            r = rem(me[2] + 2 + t, 4)
            kr = kfull[panel(r)]
            mass = jnp.sum(kr.astype(F32), axis=1, keepdims=True)
            drive = jnp.dot(kr, a_buf[...], preferred_element_type=F32)
            pull = jnp.dot(kr, t_own[slot], preferred_element_type=F32)
            upd = (drive + (2.0 / kern_width) * (mass * t_own[slot, panel(r)].astype(F32) - pull)) / n_total
            theta = get_rows(r) + step_size * upd
            for v in range(4):
                th[r, v] = theta[v * B:(v + 1) * B]

            @pl.when(step < NUM_STEPS - 1)
            def _():
                prepare(r, theta, 1 - slot)

            for o in range(4):
                @pl.when(jnp.logical_and(step == NUM_STEPS - 1, t == (o + 2) % 4))
                def _():
                    out_start(o)
            return cc
        with jax.named_scope("update"):
            lax.fori_loop(0, n_panels, update, 0)
        with jax.named_scope("sendwait"):
            for m in pending:
                m.wait_send()
            for k, ta, tb in swaps:
                swap(k, ta, tb).wait_send()
        return carry

    lax.fori_loop(0, NUM_STEPS, one_step, 0)

    def out_second(h):
        d = 1 + h

        def place_of(src_at, v):
            return out_ref.at[pl.ds(h * hb, hb), cols(src_at, v) if h == 0 else cols(v, src_at)]

        def sends(tag):
            way = tag[1] == "+"
            b = 0 if way else 1
            if tag[0] == "f":
                return [(rel3.at[h, b, t], place_of(side(d, 3 if way else 1), 2 * b + t)) for t in range(2)]
            to = side(d, {"r": 2, "d": 1 if way else 3}[tag[0]])
            if tag[0] == "r":
                return [(m1.at[h, v, to], rel3.at[h, b, v % 2]) for v in halves(tag)]
            return [(m1.at[h, v, to], place_of(me[d], v)) for v in range(4)]
        return relayed(("out2", h), d, sends)

    with jax.named_scope("out1"):
        first = [out_first(h)[:3] for h in range(2)]
        for v in range(4):
            m1[0, me[2], v] = th[me[2], v, pl.ds(0, hb)]
            m1[1, me[1], v] = th[v, me[1], pl.ds(hb, hb)]
        for relay, finish, started in first:
            relay()
    with jax.named_scope("out2"):
        second = []
        for h, (relay, finish, started) in enumerate(first):
            finish()
            second.append(out_second(h))
        own_out = []
        for v in range(4):
            own_out.append(local(("back", v), m1.at[0, v, me[1]], out_ref.at[pl.ds(0, hb), cols(me[1], v)]))
            own_out.append(local(("back", 4 + v), m1.at[1, v, me[2]], out_ref.at[pl.ds(hb, hb), cols(v, me[2])]))
        for m in own_out:
            m.start()
        for relay, finish, started in second:
            relay()
        for relay, finish, started in second:
            finish()
        for relay, finish, started in first + second:
            for m in started:
                m.wait_send()
        for m in own_out:
            m.wait()


def run_steps(theta, lam, mu, fac, sizes, kern_width, step_size):
    n_total, fcol = theta.shape[0] * sizes[1] * sizes[2], theta.shape[1] // (sizes[1] * sizes[2])
    rank = fac.shape[1]
    nb = n_total // B
    n_chip = sizes[0] * sizes[1] * sizes[2]
    assert nb * nb == 4 * n_chip and rank == 4 * nb
    hb = B // 2
    cfg = dict(sizes=sizes, nb=nb, kern_width=kern_width, step_size=step_size)
    n1, n2 = n_chip, n_chip
    vmem = pl.BlockSpec(memory_space=pltpu.VMEM)
    most1 = max(n_chip // sizes[k] for k in range(3))
    most2 = max(sizes)
    blocks = (4, 4, B, fcol)
    scratch = [
        pltpu.VMEM(blocks, F32),
        pltpu.VMEM((2, 4, hb, 4 * fcol), F32),
        pltpu.VMEM((2, 4, 4, hb, fcol), F32),
        pltpu.VMEM((2, 2, hb // 2, 4 * fcol), F32),
        pltpu.VMEM((2, 2, 2, hb, fcol), F32),
        pltpu.VMEM((2, 2, 2, hb, fcol), F32),
        pltpu.VMEM((1, fcol), F32),
        pltpu.VMEM((1, fcol), F32),
        pltpu.VMEM((rank, fcol), BF16),
        pltpu.VMEM((2, n_total, fcol), BF16),
        pltpu.VMEM((n_total, fcol), BF16),
        pltpu.VMEM((n_total, fcol), BF16),
        pltpu.VMEM((rank, n_total), F32),
        pltpu.VMEM((rank // 2, n_total), F32),
        pltpu.VMEM((rank, n_total), F32),
        pltpu.VMEM((nb, 8, B), F32),
        pltpu.VMEM((nb, B, B), F32),
        pltpu.VMEM((3, n_chip, PIECE, B), F32),
        pltpu.VMEM((3, 4, most1, PIECE, B), F32),
        pltpu.VMEM((3, 2, 2, PIECE, B), F32),
        pltpu.VMEM((3, 4, most2, PIECE, B), F32),
        pltpu.VMEM((3, 4, PIECE, B), F32),
        pltpu.VMEM((3, most1, PIECE, B), F32),
        pltpu.VMEM((3, most2, PIECE, B), F32),
        pltpu.VMEM((3, PIECE, B), F32),
        pltpu.VMEM((3, n_chip, PIECE, B), BF16),
        pltpu.VMEM((3, n_chip, PIECE, B), BF16),
        pltpu.VMEM((n_total, n_total), BF16),
        pltpu.SemaphoreType.DMA((NUM_SEMS,)),
        pltpu.SemaphoreType.DMA((NUM_SEMS,)),
    ]
    hbm = pl.BlockSpec(memory_space=pltpu.HBM)
    return pl.pallas_call(
        functools.partial(steps_kernel, cfg),
        out_shape=jax.ShapeDtypeStruct(theta.shape, F32),
        in_specs=[hbm, vmem, vmem, hbm],
        out_specs=hbm,
        scratch_shapes=scratch,
        compiler_params=pltpu.CompilerParams(collective_id=0, has_side_effects=True, vmem_limit_bytes=60 * 1024 * 1024),
        name="svgd_steps",
    )(theta, lam[None], mu[None], fac.T)


def solution(mesh, sizes=(4, 4, 4)):
    part_size = mesh.shape["part"]
    feat_size = mesh.shape["feat"]

    def local_steps(local_theta, prec_loc, mean_loc, factor_loc):
        rows_loc, feat_loc = local_theta.shape
        n_total = rows_loc * part_size
        feat_total = feat_loc * feat_size
        kern_width = 2.0 * feat_total / math.log(n_total)
        step_size = 0.15 * n_total * feat_total / math.log(n_total)
        return run_steps(local_theta, prec_loc, mean_loc, factor_loc, sizes, kern_width, step_size)

    row_spec = P(("ens", "part"), "feat")
    vec_spec = P(("ens", "feat"))
    fac_spec = P(("ens", "feat"), None)
    return jax.shard_map(local_steps, mesh=mesh, in_specs=(row_spec, vec_spec, vec_spec, fac_spec), out_specs=row_spec, check_vma=False)
```

```python
import functools
import math
import jax
import jax.numpy as jnp
from jax import lax
from jax.experimental import pallas as pl
from jax.experimental.pallas import tpu as pltpu
from jax.sharding import PartitionSpec as P

NUM_STEPS = 3
B = 128
PIECE = 48
F32 = jnp.float32
BF16 = jnp.bfloat16
NT = (((1,), (1,)), ((), ()))
TN = (((0,), (0,)), ((), ()))
NUM_SEMS = 416
PANEL = 512


def rem(a, n):
    return lax.rem(a, jnp.int32(n))


def div(a, n):
    return lax.div(a, jnp.int32(n))


def unrolled(count, by, body):
    def several(r, cc):
        for t in range(by):
            body(r * by + t)
        return cc
    lax.fori_loop(0, count // by, several, 0)


def mine(ref, h, v, src_at):
    hb = B // 2
    return ref.at[src_at, v, pl.ds(0, hb)] if h == 0 else ref.at[v, src_at, pl.ds(hb, hb)]


def steps_kernel(cfg, theta_ref, lam_all, mu_all, fact_all, out_ref, th, l1, m1, rel1, rel2, rel3, lam_ref, mu_ref, fact_ref,
                 t_own, t_par, a_buf, zt, zt_par, zt_b, s_all, d_all, g, ring1, relb, dirb, dir3, acc2, acc3, unit, ag,
                 ag_par, kfull, send_sems, recv_sems):
    nb, kern_width, step_size = cfg["nb"], cfg["kern_width"], cfg["step_size"]
    n_total = nb * B
    n_chip = 64
    part, feat = lax.axis_index("part"), lax.axis_index("feat")
    core = rem(feat, 2)
    me = (div(feat, 2), rem(part, 4), div(part, 4))
    near = [[me[d]] + [rem(me[d] + by, 4) for by in (1, 2, 3)] for d in range(3)]

    def dev(coord, c):
        return {"part": coord[2] * 4 + coord[1], "feat": coord[0] * 2 + c}

    def device_at(dim, by):
        c = list(me)
        c[dim] = near[dim][by]
        return dev(c, core)

    around = [[device_at(d, by) for by in range(4)] for d in range(3)]

    def shifted(dim, by):
        return around[dim][by]

    partner = dev(me, 1 - core)
    perms = [(k, (k + 1) % 3, (k + 2) % 3) for k in range(3)]

    ids = {}

    def slot_of(key):
        idx = ids.setdefault(key, len(ids))
        assert idx < NUM_SEMS - 8
        return idx

    def copy(key, src, dst, to):
        idx = slot_of(key)
        return pltpu.make_async_remote_copy(
            src_ref=src, dst_ref=dst, send_sem=send_sems.at[idx], recv_sem=recv_sems.at[idx],
            device_id=to, device_id_type=pl.DeviceIdType.MESH)

    def local(key, src, dst):
        return pltpu.make_async_copy(src, dst, send_sems.at[slot_of(key)])

    barrier = pltpu.get_barrier_semaphore()
    peers = [partner] + [shifted(d, by) for d in range(3) for by in (1, 2, 3)]
    for peer in peers:
        pl.semaphore_signal(barrier, inc=1, device_id=peer, device_id_type=pl.DeviceIdType.MESH)
    pl.semaphore_wait(barrier, len(peers))

    row = lax.broadcasted_iota(jnp.int32, (B, B), 0)
    col = lax.broadcasted_iota(jnp.int32, (B, B), 1)
    low, eye = row >= col, row == col

    def blk(i):
        return pl.ds(pl.multiple_of(i * B, B), B)

    def unit_of(c, q):
        u = c * n_chip + q
        i = rem(u, nb)
        return u, i, rem(i + div(u, nb) + 1, nb), u >= 2 * n_chip - nb // 2

    def chip_index(k, x, y, z):
        p = perms[k]
        c = (x, y, z)
        return (c[p[0]] * 4 + c[p[1]]) * 4 + c[p[2]]

    def split(n, wide):
        if n > 1:
            return (0, n // 2, 0, PIECE), (n // 2, n // 2, 0, PIECE)
        r = 32 if wide else 24
        return (0, 1, 0, r), (0, 1, r, PIECE - r)

    def part_of(ref, lead, base, half):
        return ref.at[lead, pl.ds(base + half[0], half[1]), pl.ds(half[2], half[3])]

    zh = zt.shape[0] // 2
    kc = nb // 4
    n_panels = n_total // PANEL

    def panel(r):
        return pl.ds(pl.multiple_of(r * PANEL, PANEL), PANEL)

    def swap_t(r, slot):
        return pltpu.make_async_remote_copy(
            src_ref=t_own.at[slot, panel(r)], dst_ref=t_par.at[panel(r)], send_sem=send_sems.at[NUM_SEMS - 1 - r],
            recv_sem=recv_sems.at[NUM_SEMS - 1 - r], device_id=partner, device_id_type=pl.DeviceIdType.MESH)

    def swap_z(r):
        return pltpu.make_async_remote_copy(
            src_ref=zt.at[pl.ds(pl.multiple_of((1 - core) * zh, 8), zh), panel(r)], dst_ref=zt_par.at[pl.ds(0, zh), panel(r)],
            send_sem=send_sems.at[NUM_SEMS - 1 - n_panels - r], recv_sem=recv_sems.at[NUM_SEMS - 1 - n_panels - r],
            device_id=partner, device_id_type=pl.DeviceIdType.MESH)

    def prepare(r, theta, slot):
        t_own[slot, panel(r)] = theta.astype(BF16)
        swap_t(r, slot).start()
        xb = (theta - mu_ref[...]).astype(BF16)
        zt[:, panel(r)] = lax.dot_general(fact_ref[...], xb, NT, preferred_element_type=F32)
        swap_z(r).start()

    def get_rows(r):
        return jnp.concatenate([th[r, v] for v in range(4)], 0)

    def first_prep(r, cc):
        prepare(r, get_rows(r), 0)
        return cc
    fcol, hb = fact_ref.shape[1], B // 2
    my = pl.ds(pl.multiple_of((me[1] * 4 + me[2]) * fcol, fcol), fcol)

    def cols(y, z, n=1):
        return pl.ds(pl.multiple_of((y * 4 + z) * fcol, fcol), n * fcol)

    def side(d, by):
        return near[d][by]

    def relayed(key, d, sends, begin=True):
        def copies(tag):
            return [copy((key, tag, t), src, dst, shifted(d, 1 if tag[1] == "+" else 3))
                    for t, (src, dst) in enumerate(sends(tag))]
        started = []

        def go(tags):
            for tag in tags:
                for m in copies(tag):
                    m.start()
                    started.append(m)

        def relay():
            for got, out in (("r+", "f+"), ("r-", "f-")):
                for m in copies(got):
                    m.wait_recv()
                go((out,))

        def finish():
            for tag in ("d+", "d-", "f+", "f-"):
                for m in copies(tag):
                    m.wait_recv()
        if begin:
            go(("r+", "r-", "d+", "d-"))
        else:
            for tag in ("r+", "r-", "d+", "d-"):
                started += copies(tag)
        return (relay, finish, started) if begin else (relay, finish, started, copies)

    def halves(tag):
        if tag[0] == "d":
            return (0, 1, 2, 3)
        return (0, 1) if tag[1] == "+" else (2, 3)

    def in_first(h):
        d = 1 + h

        def sends(tag):
            r0, nr = {"r+": (0, hb // 2), "r-": (hb // 2, hb // 2)}.get(tag, (0, hb))
            way = tag[1] == "+"
            if tag[0] == "f":
                b = 0 if way else 1
                return [(rel1.at[h, b], l1.at[h, side(d, 3 if way else 1), pl.ds(b * (hb // 2), hb // 2)])]
            to = side(d, {"r": 2, "d": 1 if way else 3}[tag[0]])
            rows = pl.ds(h * hb + r0, nr)

            def dst(y, n):
                at = pl.ds(y * fcol, n * fcol)
                if tag[0] == "d":
                    return l1.at[h, me[d], pl.ds(0, nr), at]
                return rel1.at[h, 0 if way else 1, pl.ds(0, nr), at]
            if h == 0:
                return [(theta_ref.at[rows, cols(to, 0, 4)], dst(0, 4))]
            return [(theta_ref.at[rows, cols(y, to)], dst(y, 1)) for y in range(4)]
        return relayed(("in1", h), d, sends)

    def in_second(h):
        d = 2 - h

        def sends(tag):
            way = tag[1] == "+"
            b = 0 if way else 1
            if tag[0] == "f":
                return [(rel2.at[h, b, v % 2], mine(th, h, v, side(d, 3 if way else 1))) for v in halves(tag)]
            to = side(d, {"r": 2, "d": 1 if way else 3}[tag[0]])
            at = pl.ds(pl.multiple_of(to * fcol, fcol), fcol)
            return [(l1.at[h, v, pl.ds(0, hb), at], mine(th, h, v, me[d]) if tag[0] == "d" else rel2.at[h, b, v % 2])
                    for v in halves(tag)]
        return relayed(("in2", h), d, sends)

    own_in = [local(("own", 0), theta_ref.at[pl.ds(0, hb), cols(me[1], 0, 4)], l1.at[0, me[1]])]
    own_in += [local(("own", 1 + y), theta_ref.at[pl.ds(hb, hb), cols(y, me[2])],
                     l1.at[1, me[2], pl.ds(0, hb), pl.ds(y * fcol, fcol)]) for y in range(4)]
    own_in.append(local(("own", 5), fact_all.at[pl.ds(0, fact_ref.shape[0]), my], fact_ref))

    with jax.named_scope("in1"):
        first = [in_first(h) for h in range(2)]
        for m in own_in:
            m.start()
        lam_ref[...] = lam_all[pl.ds(0, 1), my]
        mu_ref[...] = mu_all[pl.ds(0, 1), my]
        for relay, finish, started in first:
            relay()
    with jax.named_scope("in2"):
        for m in own_in:
            m.wait()
        second = []
        for h, (relay, finish, started) in enumerate(first):
            finish()
            second.append(in_second(h))
        for v in range(4):
            th[me[2], v, pl.ds(0, hb)] = l1[0, v, pl.ds(0, hb), pl.ds(pl.multiple_of(me[2] * fcol, fcol), fcol)]
            th[v, me[1], pl.ds(hb, hb)] = l1[1, v, pl.ds(0, hb), pl.ds(pl.multiple_of(me[1] * fcol, fcol), fcol)]
        for relay, finish, started in second:
            relay()
        for relay, finish, started in second:
            finish()
        for relay, finish, started in first + second:
            for m in started:
                m.wait_send()
    with jax.named_scope("prep"):
        lax.fori_loop(0, n_panels, first_prep, 0)

    def out_pieces(h, tag):
        if h == 0:
            return halves(tag)
        return (0, 1, 2, 3) if tag[0] == "d" else (2, 3) if tag[1] == "+" else (0, 1)

    def out_first(h):
        d = 2 - h

        def sends(tag):
            way = tag[1] == "+"
            b = 0 if way else 1
            vs = [(v if h == 0 else near[2][v], v % 2) for v in out_pieces(h, tag)]
            if tag[0] == "f":
                return [(rel2.at[h, b, at], m1.at[h, side(d, 3 if way else 1), v]) for v, at in vs]
            to = side(d, {"r": 2, "d": 1 if way else 3}[tag[0]])
            return [(mine(th, h, v, to), m1.at[h, me[d], v] if tag[0] == "d" else rel2.at[h, b, at]) for v, at in vs]
        return relayed(("out1", h), d, sends, begin=False)

    def out_start(o):
        for tag in ((), ("d+",), ("r+", "r-"), ("d-",))[o]:
            for m in out_first(0)[3](tag):
                m.start()
        for tag in ("r+" if o >= 2 else "r-", "d+", "d-"):
            out_first(1)[3](tag)[out_pieces(1, tag).index(o)].start()

    def one_step(step, carry):
        slot = rem(step, 2)
        with jax.named_scope("twait"):
            for r in range(n_panels):
                swap_t(r, slot).wait()
                swap_z(r).wait()

        def products(rows, cols):
            return (lax.dot_general(jnp.concatenate([t_own[slot, r] for r in rows], 0), t_own[slot, cols], NT,
                                    preferred_element_type=F32)
                    + lax.dot_general(jnp.concatenate([t_par[r] for r in rows], 0), t_par[cols], NT,
                                      preferred_element_type=F32))

        def put(m, x, y, z):
            g[0, chip_index(0, x, y, z)] = m[:48]
            g[1, chip_index(1, x, y, z)] = m[48:96]
            g[2, chip_index(2, x, y, z), pl.ds(0, 32)] = m[96:]

        def form(h, cc):
            i = h * 2
            cols = pl.ds(pl.multiple_of(i * B, 2 * B), 2 * B)
            dg = products([cols], cols)
            for t in range(2):
                dt = dg[t * B:(t + 1) * B, t * B:(t + 1) * B]
                d_all[i + t] = dt
                s_all[i + t] = jnp.broadcast_to(jnp.sum(jnp.where(eye, dt, 0.0), axis=0, keepdims=True), (8, B))
            m = products([blk(rem(i + core * kc + 1 + t, nb)) for t in range(kc + 1)], cols)
            y, z = div(h, 2), 2 * rem(h, 2)
            for t in range(kc + 1):
                if t < kc:
                    put(m[t * B:(t + 1) * B, :B], t, y, z)
                if t > 0:
                    put(m[t * B:(t + 1) * B, B:], t - 1, y, z + 1)
            return cc
        with jax.named_scope("form"):
            lax.fori_loop(0, nb // 2, form, 0, unroll=2)

        with jax.named_scope("pair"):
            @pl.when(core == 1)
            def _():
                def pair(t, cc):
                    i = t + nb // 2
                    put(jnp.where(low, d_all[i], d_all[t]), 3, div(i, 4), rem(i, 4))
                    return cc
                lax.fori_loop(0, nb // 2, pair, 0)

        pending = []

        order = (2, 1, 3, 0)
        wave_base = [[[(near[perms[k][0]][t] * 4 + near[perms[k][1]][o]) * 4 for t in range(4)] for o in order]
                     for k in range(3)]

        def wave(k, s):
            return perms[k], 4, order[s], wave_base[k][s]

        def n_waves(k):
            return 4

        def ring_copy(k, s, tag):
            p, n, by, base = wave(k, s)
            ha, hb = split(n, False)
            at, half, kind, to = {
                "m1p": (2, ha, 0, 1), "m1m": (2, hb, 1, 3), "m2p": (1, hb, 2, 1), "m2m": (3, ha, 3, 3),
                "m3p": (1, ha, 2, 1), "m3m": (3, hb, 3, 3)}[tag]
            return copy(("rs", k, s, tag), part_of(g, k, base[at], half), part_of(ring1.at[k], kind, s * n, half),
                        shifted(p[0], to))

        def ring_start(s, tags, colours=(0, 1, 2)):
            for tag in tags:
                for k in colours:
                    if s < n_waves(k):
                        m = ring_copy(k, s, tag)
                        m.start()
                        pending.append(m)

        def ring_merge(s):
            for k in range(3):
                p, n, by, base = wave(k, s)
                ha, hb = split(n, False)
                for got, out, at, half, kind in (("m1p", "m3p", 1, ha, 0), ("m1m", "m3m", 3, hb, 1)):
                    ring_copy(k, s, got).wait_recv()
                    part_of(g, k, base[at], half)[...] += part_of(ring1.at[k], kind, s * n, half)[...]
                    m = ring_copy(k, s, out)
                    m.start()
                    pending.append(m)

        def owner_copy(k, by, s):
            return copy(("rb", k, by), acc2.at[k, pl.ds(s * 4, 4)], dirb.at[k, by], shifted(perms[k][1], by))

        def via_copy(k, b):
            return copy(("rv", k, b), acc2.at[k, pl.ds(2 * b, 2)], relb.at[k, b], shifted(perms[k][1], (1, 3)[b]))

        def ring_finish(s):
            for k in range(3):
                p, n, by, base = wave(k, s)
                for tag in ("m2p", "m2m", "m3p", "m3m"):
                    ring_copy(k, s, tag).wait_recv()
                if by in (1, 3):
                    via_copy(k, by // 2).wait_recv()
                for v in range(n):
                    tot = g[k, base[0] + v] + ring1[k, 2, s * n + v] + ring1[k, 3, s * n + v]
                    if by in (1, 3) and v // 2 == by // 2:
                        tot = tot + relb[k, by // 2, v % 2]
                    acc2[k, s * n + v] = tot
                ms = [via_copy(k, 0), via_copy(k, 1)] if by == 2 else [owner_copy(k, by, s)] if by else []
                for m in ms:
                    m.start()
                    pending.append(m)

        ring_start(0, ("m1p", "m1m"), (0, 1))

        row8 = lax.broadcasted_iota(jnp.int32, (8, B), 0)

        def tails(i, cc):
            y, z = div(i, 4), rem(i, 4)
            for x in range(4):
                off = core * kc + x
                at = chip_index(2, x, y, z)
                g[2, at, pl.ds(32, 8)] = jnp.where(row8 == 0, s_all[rem(i + off + 1, nb)], s_all[i])
                g[2, at, pl.ds(40, 8)] = (zt[pl.ds(pl.multiple_of(off * 8, 8), 8), blk(i)]
                                          + zt_par[pl.ds(x * 8, 8), blk(i)])
            return cc
        with jax.named_scope("tails"):
            lax.fori_loop(0, nb, tails, 0)

        most = 4
        with jax.named_scope("rs0"):
            ring_start(0, ("m1p", "m1m"), (2,))
            ring_start(0, ("m2p", "m2m"))
            ring_start(1, ("m1p", "m1m"))
            for s in range(most):
                ring_merge(s)
                ring_start(s + 1, ("m2p", "m2m"))
                ring_start(s + 2, ("m1p", "m1m"))
                if s:
                    ring_finish(s - 1)
            ring_finish(most - 1)
        last = []
        with jax.named_scope("rs1"):
            for k in range(3):
                p = perms[k]
                n, s = 4, 3
                bys = (1, 3)
                for by in bys:
                    owner_copy(k, by, 0).wait_recv()
                for v in range(n):
                    tot = acc2[k, s * n + v]
                    for by in bys:
                        tot = tot + dirb[k, by, v]
                    acc3[k, v] = tot
                ms = []
                for by in (1, 2, 3):
                    m = copy(("rc", k, by), acc3.at[k, near[p[2]][by]], dir3.at[k, by],
                             shifted(p[2], by))
                    m.start()
                    ms.append(m)
                last.append(ms)
                pending += ms
        with jax.named_scope("rs2"):
            for k in range(3):
                tot = acc3[k, me[perms[k][2]]]
                for m in last[k]:
                    m.wait_recv()
                for by in range(1, len(last[k]) + 1):
                    tot = tot + dir3[k, by]
                unit[k] = tot

        summed = pending
        pending = []
        with jax.named_scope("kunit"):
            packed = unit_of(core, (me[0] * 4 + me[1]) * 4 + me[2])[3]
            g_u = jnp.concatenate([unit[0], unit[1], unit[2, pl.ds(0, 32)]], 0)
            sj = jnp.broadcast_to(unit[2, pl.ds(32, 1)], (B, B))
            si = jnp.broadcast_to(unit[2, pl.ds(33, 1)], (B, B))
            si_c = jnp.broadcast_to(jnp.sum(jnp.where(eye, si, 0.0), axis=1, keepdims=True), (B, B))
            sj_c = jnp.broadcast_to(jnp.sum(jnp.where(eye, sj, 0.0), axis=1, keepdims=True), (B, B))
            lower = jnp.logical_and(packed, low)
            upper = jnp.logical_and(packed, jnp.logical_not(low))
            s_sum = jnp.where(lower, si_c, sj_c) + jnp.where(upper, sj, si)
            dist = jnp.maximum(s_sum - 2.0 * g_u, 0.0)
            k_u = jnp.exp(-dist / kern_width)
            z_u = unit[2, pl.ds(40, 8)]
            pieces = (k_u[:48], k_u[48:96], jnp.concatenate([k_u[96:], z_u, jnp.zeros_like(z_u)], 0))
            own = [chip_index(k, *me) for k in range(3)]
            for k in range(3):
                ag[k, own[k]] = pieces[k].astype(BF16)

        def place(ref, c, k, a, b, at):
            for v in range(4):
                coord = [0, 0, 0]
                for d, t in zip(perms[k], (a, b, v)):
                    coord[d] = t
                off = c * kc + coord[0]
                i = coord[1] * 4 + coord[2]
                top = (rem(i + off + 1, nb) + div(off * nb + i, 2 * n_chip - nb // 2) * (nb // 2)) * B + 48 * k
                n = (48, 48, 32)[k]
                kfull[pl.ds(pl.multiple_of(top, 16), n), blk(i)] = ref[k, at + v, pl.ds(0, n)]
                if k == 2:
                    tail = ref[k, at + v, pl.ds(32, 16)].astype(F32)
                    zt_b[pl.ds(pl.multiple_of(off * 8, 8), 8), blk(i)] = tail[:8]

        chunks = {}

        def chunk(k, ta, tb):
            if (k, ta, tb) not in chunks:
                p = perms[k]
                a, b = near[p[0]][ta], near[p[1]][tb]
                chunks[k, ta, tb] = (a, b, (a * 4 + b) * 4, 4)
            return chunks[k, ta, tb]

        def swap(k, ta, tb):
            a, b, at, n = chunk(k, ta, tb)
            return copy(("sw", k, ta, tb), ag.at[k, pl.ds(at, n)], ag_par.at[k, pl.ds(at, n)], partner)

        swaps = []
        placed = []

        def take(upto):
            while len(placed) < upto:
                k, ta, tb = swaps[len(placed)]
                swap(k, ta, tb).wait_recv()
                a, b, at, n = chunk(k, ta, tb)
                place(ag_par, 1 - core, k, a, b, at)
                placed.append((k, ta, tb))

        def have(k, ta, tb):
            swap(k, ta, tb).start()
            swaps.append((k, ta, tb))
            a, b, at, n = chunk(k, ta, tb)
            place(ag, core, k, a, b, at)

        def unit_copy(stage, k, by, tc, start):
            p = perms[k]
            a, b, at, n = chunk(k, 0, 0)
            at = at + near[p[2]][tc]
            m = copy(("u", stage, k, by, tc), ag.at[k, at], ag.at[k, at], shifted(p[stage], by))
            if start:
                m.start()
                pending.append(m)
            return m

        def a_copy(k, tb, tag, start=False):
            p = perms[k]
            ta, h, to = {"n1p": (0, 0, 1), "n1m": (0, 1, 3), "n2p": (0, 1, 1), "n2m": (0, 0, 3), "n3p": (3, 0, 1),
                         "n3m": (1, 1, 3)}[tag]
            a, b, at, n = chunk(k, ta, tb)
            half = split(n, True)[h]
            m = copy(("a", k, tb, tag), part_of(ag, k, at, half), part_of(ag, k, at, half), shifted(p[0], to))
            if start:
                m.start()
                pending.append(m)
            return m

        def a_launch(k, tb):
            for tag in ("n1p", "n1m", "n2p", "n2m"):
                a_copy(k, tb, tag, True)
            have(k, 0, tb)

        def a_relay(tb):
            for k in range(3):
                if True:
                    for got, out in (("n1p", "n3p"), ("n1m", "n3m")):
                        a_copy(k, tb, got).wait_recv()
                        a_copy(k, tb, out, True)

        def a_near(tb):
            for k in range(3):
                if True:
                    for got, ta in (("n2p", 3), ("n2m", 1)):
                        a_copy(k, tb, got).wait_recv()
                        have(k, ta, tb)

        def a_far(tb):
            for k in range(3):
                if True:
                    for got in ("n3p", "n3m"):
                        a_copy(k, tb, got).wait_recv()
                    have(k, 2, tb)

        def a_waves(tbs):
            for tb in tbs:
                for k in range(3):
                    a_launch(k, tb)

        with jax.named_scope("ag2"):
            for k in range(3):
                for by in (1, 2, 3):
                    unit_copy(2, k, by, 0, True)
            for k in range(3):
                for by in (2, 1, 3):
                    unit_copy(1, k, by, 0, True)
            for m in summed:
                m.wait_send()
            for by in (1, 3, 2):
                for k in range(3):
                    unit_copy(2, k, by, 0, False).wait_recv()
                    for bb in (2, 1, 3):
                        unit_copy(1, k, bb, 4 - by, True)
            a_waves((0,))

        def b_arrivals(bb):
            for k in range(3):
                for tc in range(4):
                    unit_copy(1, k, bb, tc, False).wait_recv()

        with jax.named_scope("ag1"):
            for name, stage, at, got in (("b1", b_arrivals, 1, 0), ("b3", b_arrivals, 3, 0), ("r0", a_relay, 0, 0),
                                         ("w", a_waves, (3, 1), 0), ("b2", b_arrivals, 2, 0), ("w2", a_waves, (2,), 0),
                                         ("n0", a_near, 0, 6), ("r3", a_relay, 3, 9), ("r1", a_relay, 1, 12),
                                         ("n3", a_near, 3, 15), ("r2", a_relay, 2, 18)):
                with jax.named_scope("ag1_" + name):
                    stage(at)
                    take(min(got, len(swaps) - 3))
        with jax.named_scope("ag0"):
            for stage, tb in ((a_far, 0), (a_near, 1), (a_far, 3), (a_near, 2), (a_far, 1), (a_far, 2)):
                before = len(swaps)
                with jax.named_scope("ag0_%s%d" % (stage.__name__, tb)):
                    stage(tb)
                take(before - 12)

        per = 4 if nb > 4 else 2

        def mirror(c, r, cc):
            at = []
            for t in range(per):
                u, i, j, packed = unit_of(c, r * per + t)
                at.append((i, j, kfull[blk(j), blk(i)].T))
            for i, j, m in at:
                kfull[blk(i), blk(j)] = m
            return cc

        def unpack(r, cc):
            both = []
            for v in range(4):
                i = r * 4 + v + nb // 2
                m = kfull[blk(i), blk(i)].astype(F32)
                mt = m.T
                both.append((jnp.where(eye, 1.0, jnp.where(low, m, mt)), jnp.where(eye, 1.0, jnp.where(low, mt, m))))
            for v, (m, mt) in enumerate(both):
                t = r * 4 + v
                kfull[blk(t + nb // 2), blk(t + nb // 2)] = m.astype(BF16)
                kfull[blk(t), blk(t)] = mt.astype(BF16)
            return cc
        with jax.named_scope("mirror1"):
            lax.fori_loop(0, div(n_chip - core * (nb // 2), per), functools.partial(mirror, core), 0)
        with jax.named_scope("swapwait"):
            take(len(swaps))
        with jax.named_scope("mirror2"):
            lax.fori_loop(0, div(n_chip - (1 - core) * (nb // 2), per), functools.partial(mirror, 1 - core), 0)
            lax.fori_loop(0, nb // 8, unpack, 0)

        def grads(r, cc):
            lowt = lax.dot_general(zt_b[:, panel(r)].astype(BF16), fact_ref[...], TN, preferred_element_type=F32)
            a_buf[panel(r)] = (-((get_rows(r) - mu_ref[...]) * lam_ref[...] + lowt)).astype(BF16)
            return cc
        with jax.named_scope("grads"):
            lax.fori_loop(0, n_panels, grads, 0)

        def update(h, cc):
            done = []
            for t in range(2):
                r = rem(me[2] + 2 + 2 * h + t, 4)
                kr = kfull[panel(r)]
                mass = jnp.sum(kr.astype(F32), axis=1, keepdims=True)
                drive = jnp.dot(kr, a_buf[...], preferred_element_type=F32)
                pull = jnp.dot(kr, t_own[slot], preferred_element_type=F32)
                upd = (drive + (2.0 / kern_width) * (mass * t_own[slot, panel(r)].astype(F32) - pull)) / n_total
                theta = get_rows(r) + step_size * upd
                for v in range(4):
                    th[r, v] = theta[v * B:(v + 1) * B]
                done.append(r)

            @pl.when(step < NUM_STEPS - 1)
            def _():
                for r in done:
                    prepare(r, get_rows(r), 1 - slot)

            for o in range(4):
                @pl.when(jnp.logical_and(step == NUM_STEPS - 1, h == (o + 2) % 4 // 2))
                def _():
                    out_start(o)
            return cc
        with jax.named_scope("update"):
            lax.fori_loop(0, n_panels // 2, update, 0)
        with jax.named_scope("sendwait"):
            for m in pending:
                m.wait_send()
            for k, ta, tb in swaps:
                swap(k, ta, tb).wait_send()
        return carry

    lax.fori_loop(0, NUM_STEPS, one_step, 0)

    def out_second(h):
        d = 1 + h

        def place_of(src_at, v):
            return out_ref.at[pl.ds(h * hb, hb), cols(src_at, v) if h == 0 else cols(v, src_at)]

        def sends(tag):
            way = tag[1] == "+"
            b = 0 if way else 1
            if tag[0] == "f":
                return [(rel3.at[h, b, t], place_of(side(d, 3 if way else 1), 2 * b + t)) for t in range(2)]
            to = side(d, {"r": 2, "d": 1 if way else 3}[tag[0]])
            if tag[0] == "r":
                return [(m1.at[h, v, to], rel3.at[h, b, v % 2]) for v in halves(tag)]
            return [(m1.at[h, v, to], place_of(me[d], v)) for v in range(4)]
        return relayed(("out2", h), d, sends)

    with jax.named_scope("out1"):
        first = [out_first(h)[:3] for h in range(2)]
        for v in range(4):
            m1[0, me[2], v] = th[me[2], v, pl.ds(0, hb)]
            m1[1, me[1], v] = th[v, me[1], pl.ds(hb, hb)]
        for relay, finish, started in first:
            relay()
    with jax.named_scope("out2"):
        second = []
        for h, (relay, finish, started) in enumerate(first):
            finish()
            second.append(out_second(h))
        own_out = []
        for v in range(4):
            own_out.append(local(("back", v), m1.at[0, v, me[1]], out_ref.at[pl.ds(0, hb), cols(me[1], v)]))
            own_out.append(local(("back", 4 + v), m1.at[1, v, me[2]], out_ref.at[pl.ds(hb, hb), cols(v, me[2])]))
        for m in own_out:
            m.start()
        for relay, finish, started in second:
            relay()
        for relay, finish, started in second:
            finish()
        for relay, finish, started in first + second:
            for m in started:
                m.wait_send()
        for m in own_out:
            m.wait()


def run_steps(theta, lam, mu, fac, sizes, kern_width, step_size):
    n_total, fcol = theta.shape[0] * sizes[1] * sizes[2], theta.shape[1] // (sizes[1] * sizes[2])
    rank = fac.shape[1]
    nb = n_total // B
    n_chip = sizes[0] * sizes[1] * sizes[2]
    assert nb * nb == 4 * n_chip and rank == 4 * nb
    hb = B // 2
    cfg = dict(sizes=sizes, nb=nb, kern_width=kern_width, step_size=step_size)
    n1, n2 = n_chip, n_chip
    vmem = pl.BlockSpec(memory_space=pltpu.VMEM)
    most1 = max(n_chip // sizes[k] for k in range(3))
    most2 = max(sizes)
    blocks = (4, 4, B, fcol)
    scratch = [
        pltpu.VMEM(blocks, F32),
        pltpu.VMEM((2, 4, hb, 4 * fcol), F32),
        pltpu.VMEM((2, 4, 4, hb, fcol), F32),
        pltpu.VMEM((2, 2, hb // 2, 4 * fcol), F32),
        pltpu.VMEM((2, 2, 2, hb, fcol), F32),
        pltpu.VMEM((2, 2, 2, hb, fcol), F32),
        pltpu.VMEM((1, fcol), F32),
        pltpu.VMEM((1, fcol), F32),
        pltpu.VMEM((rank, fcol), BF16),
        pltpu.VMEM((2, n_total, fcol), BF16),
        pltpu.VMEM((n_total, fcol), BF16),
        pltpu.VMEM((n_total, fcol), BF16),
        pltpu.VMEM((rank, n_total), F32),
        pltpu.VMEM((rank // 2, n_total), F32),
        pltpu.VMEM((rank, n_total), F32),
        pltpu.VMEM((nb, 8, B), F32),
        pltpu.VMEM((nb, B, B), F32),
        pltpu.VMEM((3, n_chip, PIECE, B), F32),
        pltpu.VMEM((3, 4, most1, PIECE, B), F32),
        pltpu.VMEM((3, 2, 2, PIECE, B), F32),
        pltpu.VMEM((3, 4, most2, PIECE, B), F32),
        pltpu.VMEM((3, 4, PIECE, B), F32),
        pltpu.VMEM((3, most1, PIECE, B), F32),
        pltpu.VMEM((3, most2, PIECE, B), F32),
        pltpu.VMEM((3, PIECE, B), F32),
        pltpu.VMEM((3, n_chip, PIECE, B), BF16),
        pltpu.VMEM((3, n_chip, PIECE, B), BF16),
        pltpu.VMEM((n_total, n_total), BF16),
        pltpu.SemaphoreType.DMA((NUM_SEMS,)),
        pltpu.SemaphoreType.DMA((NUM_SEMS,)),
    ]
    hbm = pl.BlockSpec(memory_space=pltpu.HBM)
    return pl.pallas_call(
        functools.partial(steps_kernel, cfg),
        out_shape=jax.ShapeDtypeStruct(theta.shape, F32),
        in_specs=[hbm, vmem, vmem, hbm],
        out_specs=hbm,
        scratch_shapes=scratch,
        compiler_params=pltpu.CompilerParams(collective_id=0, has_side_effects=True, vmem_limit_bytes=60 * 1024 * 1024),
        name="svgd_steps",
    )(theta, lam[None], mu[None], fac.T)


def solution(mesh, sizes=(4, 4, 4)):
    part_size = mesh.shape["part"]
    feat_size = mesh.shape["feat"]

    def local_steps(local_theta, prec_loc, mean_loc, factor_loc):
        rows_loc, feat_loc = local_theta.shape
        n_total = rows_loc * part_size
        feat_total = feat_loc * feat_size
        kern_width = 2.0 * feat_total / math.log(n_total)
        step_size = 0.15 * n_total * feat_total / math.log(n_total)
        return run_steps(local_theta, prec_loc, mean_loc, factor_loc, sizes, kern_width, step_size)

    row_spec = P(("ens", "part"), "feat")
    vec_spec = P(("ens", "feat"))
    fac_spec = P(("ens", "feat"), None)
    return jax.shard_map(local_steps, mesh=mesh, in_specs=(row_spec, vec_spec, vec_spec, fac_spec), out_specs=row_spec, check_vma=False)
```

```python
import functools
import math
import jax
import jax.numpy as jnp
from jax import lax
from jax.experimental import pallas as pl
from jax.experimental.pallas import tpu as pltpu
from jax.sharding import PartitionSpec as P

NUM_STEPS = 3
B = 128
PIECE = 48
F32 = jnp.float32
BF16 = jnp.bfloat16
NT = (((1,), (1,)), ((), ()))
TN = (((0,), (0,)), ((), ()))
NUM_SEMS = 416
PANEL = 512


def rem(a, n):
    return lax.rem(a, jnp.int32(n))


def div(a, n):
    return lax.div(a, jnp.int32(n))


def unrolled(count, by, body):
    def several(r, cc):
        for t in range(by):
            body(r * by + t)
        return cc
    lax.fori_loop(0, count // by, several, 0)


def mine(ref, h, v, src_at):
    hb = B // 2
    return ref.at[src_at, v, pl.ds(0, hb)] if h == 0 else ref.at[v, src_at, pl.ds(hb, hb)]


def steps_kernel(cfg, theta_ref, lam_all, mu_all, fact_all, out_ref, th, l1, m1, rel1, rel2, rel3, lam_ref, mu_ref, fact_ref,
                 t_own, t_par, a_buf, zt, zt_par, zt_b, s_all, d_all, g, ring1, relb, dirb, dir3, acc2, acc3, unit, ag,
                 ag_par, kfull, send_sems, recv_sems):
    nb, kern_width, step_size = cfg["nb"], cfg["kern_width"], cfg["step_size"]
    n_total = nb * B
    n_chip = 64
    part, feat = lax.axis_index("part"), lax.axis_index("feat")
    core = rem(feat, 2)
    me = (div(feat, 2), rem(part, 4), div(part, 4))
    near = [[me[d]] + [rem(me[d] + by, 4) for by in (1, 2, 3)] for d in range(3)]

    def dev(coord, c):
        return {"part": coord[2] * 4 + coord[1], "feat": coord[0] * 2 + c}

    def device_at(dim, by):
        c = list(me)
        c[dim] = near[dim][by]
        return dev(c, core)

    around = [[device_at(d, by) for by in range(4)] for d in range(3)]

    def shifted(dim, by):
        return around[dim][by]

    partner = dev(me, 1 - core)
    perms = [(k, (k + 1) % 3, (k + 2) % 3) for k in range(3)]

    ids = {}

    def slot_of(key):
        idx = ids.setdefault(key, len(ids))
        assert idx < NUM_SEMS - 8
        return idx

    def copy(key, src, dst, to):
        idx = slot_of(key)
        return pltpu.make_async_remote_copy(
            src_ref=src, dst_ref=dst, send_sem=send_sems.at[idx], recv_sem=recv_sems.at[idx],
            device_id=to, device_id_type=pl.DeviceIdType.MESH)

    def local(key, src, dst):
        return pltpu.make_async_copy(src, dst, send_sems.at[slot_of(key)])

    barrier = pltpu.get_barrier_semaphore()
    peers = [partner] + [shifted(d, by) for d in range(3) for by in (1, 2, 3)]
    for peer in peers:
        pl.semaphore_signal(barrier, inc=1, device_id=peer, device_id_type=pl.DeviceIdType.MESH)
    pl.semaphore_wait(barrier, len(peers))

    row = lax.broadcasted_iota(jnp.int32, (B, B), 0)
    col = lax.broadcasted_iota(jnp.int32, (B, B), 1)
    low, eye = row >= col, row == col

    def blk(i):
        return pl.ds(pl.multiple_of(i * B, B), B)

    def unit_of(c, q):
        u = c * n_chip + q
        i = rem(u, nb)
        return u, i, rem(i + div(u, nb) + 1, nb), u >= 2 * n_chip - nb // 2

    def chip_index(k, x, y, z):
        p = perms[k]
        c = (x, y, z)
        return (c[p[0]] * 4 + c[p[1]]) * 4 + c[p[2]]

    def split(n, wide):
        if n > 1:
            return (0, n // 2, 0, PIECE), (n // 2, n // 2, 0, PIECE)
        r = 32 if wide else 24
        return (0, 1, 0, r), (0, 1, r, PIECE - r)

    def part_of(ref, lead, base, half):
        return ref.at[lead, pl.ds(base + half[0], half[1]), pl.ds(half[2], half[3])]

    zh = zt.shape[0] // 2
    kc = nb // 4
    n_panels = n_total // PANEL

    def panel(r):
        return pl.ds(pl.multiple_of(r * PANEL, PANEL), PANEL)

    def swap_t(r, slot):
        return pltpu.make_async_remote_copy(
            src_ref=t_own.at[slot, panel(r)], dst_ref=t_par.at[panel(r)], send_sem=send_sems.at[NUM_SEMS - 1 - r],
            recv_sem=recv_sems.at[NUM_SEMS - 1 - r], device_id=partner, device_id_type=pl.DeviceIdType.MESH)

    def swap_z(r):
        return pltpu.make_async_remote_copy(
            src_ref=zt.at[pl.ds(pl.multiple_of((1 - core) * zh, 8), zh), panel(r)], dst_ref=zt_par.at[pl.ds(0, zh), panel(r)],
            send_sem=send_sems.at[NUM_SEMS - 1 - n_panels - r], recv_sem=recv_sems.at[NUM_SEMS - 1 - n_panels - r],
            device_id=partner, device_id_type=pl.DeviceIdType.MESH)

    def prepare(r, theta, slot):
        t_own[slot, panel(r)] = theta.astype(BF16)
        swap_t(r, slot).start()
        xb = (theta - mu_ref[...]).astype(BF16)
        zt[:, panel(r)] = lax.dot_general(fact_ref[...], xb, NT, preferred_element_type=F32)
        swap_z(r).start()

    def get_rows(r):
        return jnp.concatenate([th[r, v] for v in range(4)], 0)

    def first_prep(r, cc):
        prepare(r, get_rows(r), 0)
        return cc
    fcol, hb = fact_ref.shape[1], B // 2
    my = pl.ds(pl.multiple_of((me[1] * 4 + me[2]) * fcol, fcol), fcol)

    def cols(y, z, n=1):
        return pl.ds(pl.multiple_of((y * 4 + z) * fcol, fcol), n * fcol)

    def side(d, by):
        return near[d][by]

    def relayed(key, d, sends, begin=True):
        def copies(tag):
            return [copy((key, tag, t), src, dst, shifted(d, 1 if tag[1] == "+" else 3))
                    for t, (src, dst) in enumerate(sends(tag))]
        started = []

        def go(tags):
            for tag in tags:
                for m in copies(tag):
                    m.start()
                    started.append(m)

        def relay():
            for got, out in (("r+", "f+"), ("r-", "f-")):
                for m in copies(got):
                    m.wait_recv()
                go((out,))

        def finish():
            for tag in ("d+", "d-", "f+", "f-"):
                for m in copies(tag):
                    m.wait_recv()
        if begin:
            go(("r+", "r-", "d+", "d-"))
        else:
            for tag in ("r+", "r-", "d+", "d-"):
                started += copies(tag)
        return (relay, finish, started) if begin else (relay, finish, started, copies)

    def halves(tag):
        if tag[0] == "d":
            return (0, 1, 2, 3)
        return (0, 1) if tag[1] == "+" else (2, 3)

    def in_first(h):
        d = 1 + h

        def sends(tag):
            r0, nr = {"r+": (0, hb // 2), "r-": (hb // 2, hb // 2)}.get(tag, (0, hb))
            way = tag[1] == "+"
            if tag[0] == "f":
                b = 0 if way else 1
                return [(rel1.at[h, b], l1.at[h, side(d, 3 if way else 1), pl.ds(b * (hb // 2), hb // 2)])]
            to = side(d, {"r": 2, "d": 1 if way else 3}[tag[0]])
            rows = pl.ds(h * hb + r0, nr)

            def dst(y, n):
                at = pl.ds(y * fcol, n * fcol)
                if tag[0] == "d":
                    return l1.at[h, me[d], pl.ds(0, nr), at]
                return rel1.at[h, 0 if way else 1, pl.ds(0, nr), at]
            if h == 0:
                return [(theta_ref.at[rows, cols(to, 0, 4)], dst(0, 4))]
            return [(theta_ref.at[rows, cols(y, to)], dst(y, 1)) for y in range(4)]
        return relayed(("in1", h), d, sends)

    def in_second(h):
        d = 2 - h

        def sends(tag):
            way = tag[1] == "+"
            b = 0 if way else 1
            if tag[0] == "f":
                return [(rel2.at[h, b, v % 2], mine(th, h, v, side(d, 3 if way else 1))) for v in halves(tag)]
            to = side(d, {"r": 2, "d": 1 if way else 3}[tag[0]])
            at = pl.ds(pl.multiple_of(to * fcol, fcol), fcol)
            return [(l1.at[h, v, pl.ds(0, hb), at], mine(th, h, v, me[d]) if tag[0] == "d" else rel2.at[h, b, v % 2])
                    for v in halves(tag)]
        return relayed(("in2", h), d, sends)

    own_in = [local(("own", 0), theta_ref.at[pl.ds(0, hb), cols(me[1], 0, 4)], l1.at[0, me[1]])]
    own_in += [local(("own", 1 + y), theta_ref.at[pl.ds(hb, hb), cols(y, me[2])],
                     l1.at[1, me[2], pl.ds(0, hb), pl.ds(y * fcol, fcol)]) for y in range(4)]
    own_in.append(local(("own", 5), fact_all.at[pl.ds(0, fact_ref.shape[0]), my], fact_ref))

    with jax.named_scope("in1"):
        first = [in_first(h) for h in range(2)]
        for m in own_in:
            m.start()
        lam_ref[...] = lam_all[pl.ds(0, 1), my]
        mu_ref[...] = mu_all[pl.ds(0, 1), my]
        for relay, finish, started in first:
            relay()
    with jax.named_scope("in2"):
        for m in own_in:
            m.wait()
        second = []
        for h, (relay, finish, started) in enumerate(first):
            finish()
            second.append(in_second(h))
        for v in range(4):
            th[me[2], v, pl.ds(0, hb)] = l1[0, v, pl.ds(0, hb), pl.ds(pl.multiple_of(me[2] * fcol, fcol), fcol)]
            th[v, me[1], pl.ds(hb, hb)] = l1[1, v, pl.ds(0, hb), pl.ds(pl.multiple_of(me[1] * fcol, fcol), fcol)]
        for relay, finish, started in second:
            relay()
        for relay, finish, started in second:
            finish()
        for relay, finish, started in first + second:
            for m in started:
                m.wait_send()
    with jax.named_scope("prep"):
        lax.fori_loop(0, n_panels, first_prep, 0)

    def out_pieces(h, tag):
        if h == 0:
            return halves(tag)
        return (0, 1, 2, 3) if tag[0] == "d" else (2, 3) if tag[1] == "+" else (0, 1)

    def out_first(h):
        d = 2 - h

        def sends(tag):
            way = tag[1] == "+"
            b = 0 if way else 1
            vs = [(v if h == 0 else near[2][v], v % 2) for v in out_pieces(h, tag)]
            if tag[0] == "f":
                return [(rel2.at[h, b, at], m1.at[h, side(d, 3 if way else 1), v]) for v, at in vs]
            to = side(d, {"r": 2, "d": 1 if way else 3}[tag[0]])
            return [(mine(th, h, v, to), m1.at[h, me[d], v] if tag[0] == "d" else rel2.at[h, b, at]) for v, at in vs]
        return relayed(("out1", h), d, sends, begin=False)

    def out_start(o):
        for tag in ((), ("d+",), ("r+", "r-"), ("d-",))[o]:
            for m in out_first(0)[3](tag):
                m.start()
        for tag in ("r+" if o >= 2 else "r-", "d+", "d-"):
            out_first(1)[3](tag)[out_pieces(1, tag).index(o)].start()

    def one_step(step, carry):
        slot = rem(step, 2)
        with jax.named_scope("twait"):
            for r in range(n_panels):
                swap_t(r, slot).wait()
                swap_z(r).wait()

        def products(rows, cols):
            return (lax.dot_general(jnp.concatenate([t_own[slot, r] for r in rows], 0), t_own[slot, cols], NT,
                                    preferred_element_type=F32)
                    + lax.dot_general(jnp.concatenate([t_par[r] for r in rows], 0), t_par[cols], NT,
                                      preferred_element_type=F32))

        def put(m, x, y, z):
            g[0, chip_index(0, x, y, z)] = m[:48]
            g[1, chip_index(1, x, y, z)] = m[48:96]
            g[2, chip_index(2, x, y, z), pl.ds(0, 32)] = m[96:]

        def form(h, cc):
            i = h * 2
            cols = pl.ds(pl.multiple_of(i * B, 2 * B), 2 * B)
            dg = products([cols], cols)
            for t in range(2):
                dt = dg[t * B:(t + 1) * B, t * B:(t + 1) * B]
                d_all[i + t] = dt
                s_all[i + t] = jnp.broadcast_to(jnp.sum(jnp.where(eye, dt, 0.0), axis=0, keepdims=True), (8, B))
            m = products([blk(rem(i + core * kc + 1 + t, nb)) for t in range(kc + 1)], cols)
            y, z = div(h, 2), 2 * rem(h, 2)
            for t in range(kc + 1):
                if t < kc:
                    put(m[t * B:(t + 1) * B, :B], t, y, z)
                if t > 0:
                    put(m[t * B:(t + 1) * B, B:], t - 1, y, z + 1)
            return cc
        with jax.named_scope("form"):
            lax.fori_loop(0, nb // 2, form, 0, unroll=4)

        with jax.named_scope("pair"):
            @pl.when(core == 1)
            def _():
                def pair(t, cc):
                    i = t + nb // 2
                    put(jnp.where(low, d_all[i], d_all[t]), 3, div(i, 4), rem(i, 4))
                    return cc
                lax.fori_loop(0, nb // 2, pair, 0)

        pending = []

        order = (2, 1, 3, 0)
        wave_base = [[[(near[perms[k][0]][t] * 4 + near[perms[k][1]][o]) * 4 for t in range(4)] for o in order]
                     for k in range(3)]

        def wave(k, s):
            return perms[k], 4, order[s], wave_base[k][s]

        def n_waves(k):
            return 4

        def ring_copy(k, s, tag):
            p, n, by, base = wave(k, s)
            ha, hb = split(n, False)
            at, half, kind, to = {
                "m1p": (2, ha, 0, 1), "m1m": (2, hb, 1, 3), "m2p": (1, hb, 2, 1), "m2m": (3, ha, 3, 3),
                "m3p": (1, ha, 2, 1), "m3m": (3, hb, 3, 3)}[tag]
            return copy(("rs", k, s, tag), part_of(g, k, base[at], half), part_of(ring1.at[k], kind, s * n, half),
                        shifted(p[0], to))

        def ring_start(s, tags, colours=(0, 1, 2)):
            for tag in tags:
                for k in colours:
                    if s < n_waves(k):
                        m = ring_copy(k, s, tag)
                        m.start()
                        pending.append(m)

        def ring_merge(s):
            for k in range(3):
                p, n, by, base = wave(k, s)
                ha, hb = split(n, False)
                for got, out, at, half, kind in (("m1p", "m3p", 1, ha, 0), ("m1m", "m3m", 3, hb, 1)):
                    ring_copy(k, s, got).wait_recv()
                    part_of(g, k, base[at], half)[...] += part_of(ring1.at[k], kind, s * n, half)[...]
                    m = ring_copy(k, s, out)
                    m.start()
                    pending.append(m)

        def owner_copy(k, by, s):
            return copy(("rb", k, by), acc2.at[k, pl.ds(s * 4, 4)], dirb.at[k, by], shifted(perms[k][1], by))

        def via_copy(k, b):
            return copy(("rv", k, b), acc2.at[k, pl.ds(2 * b, 2)], relb.at[k, b], shifted(perms[k][1], (1, 3)[b]))

        def ring_finish(s):
            for k in range(3):
                p, n, by, base = wave(k, s)
                for tag in ("m2p", "m2m", "m3p", "m3m"):
                    ring_copy(k, s, tag).wait_recv()
                if by in (1, 3):
                    via_copy(k, by // 2).wait_recv()
                for v in range(n):
                    tot = g[k, base[0] + v] + ring1[k, 2, s * n + v] + ring1[k, 3, s * n + v]
                    if by in (1, 3) and v // 2 == by // 2:
                        tot = tot + relb[k, by // 2, v % 2]
                    acc2[k, s * n + v] = tot
                ms = [via_copy(k, 0), via_copy(k, 1)] if by == 2 else [owner_copy(k, by, s)] if by else []
                for m in ms:
                    m.start()
                    pending.append(m)

        ring_start(0, ("m1p", "m1m"), (0, 1))

        row8 = lax.broadcasted_iota(jnp.int32, (8, B), 0)

        def tails(i, cc):
            y, z = div(i, 4), rem(i, 4)
            for x in range(4):
                off = core * kc + x
                at = chip_index(2, x, y, z)
                g[2, at, pl.ds(32, 8)] = jnp.where(row8 == 0, s_all[rem(i + off + 1, nb)], s_all[i])
                g[2, at, pl.ds(40, 8)] = (zt[pl.ds(pl.multiple_of(off * 8, 8), 8), blk(i)]
                                          + zt_par[pl.ds(x * 8, 8), blk(i)])
            return cc
        with jax.named_scope("tails"):
            lax.fori_loop(0, nb, tails, 0)

        most = 4
        with jax.named_scope("rs0"):
            ring_start(0, ("m1p", "m1m"), (2,))
            ring_start(0, ("m2p", "m2m"))
            ring_start(1, ("m1p", "m1m"))
            for s in range(most):
                ring_merge(s)
                ring_start(s + 1, ("m2p", "m2m"))
                ring_start(s + 2, ("m1p", "m1m"))
                if s:
                    ring_finish(s - 1)
            ring_finish(most - 1)
        last = []
        with jax.named_scope("rs1"):
            for k in range(3):
                p = perms[k]
                n, s = 4, 3
                bys = (1, 3)
                for by in bys:
                    owner_copy(k, by, 0).wait_recv()
                for v in range(n):
                    tot = acc2[k, s * n + v]
                    for by in bys:
                        tot = tot + dirb[k, by, v]
                    acc3[k, v] = tot
                ms = []
                for by in (1, 2, 3):
                    m = copy(("rc", k, by), acc3.at[k, near[p[2]][by]], dir3.at[k, by],
                             shifted(p[2], by))
                    m.start()
                    ms.append(m)
                last.append(ms)
                pending += ms
        with jax.named_scope("rs2"):
            for k in range(3):
                tot = acc3[k, me[perms[k][2]]]
                for m in last[k]:
                    m.wait_recv()
                for by in range(1, len(last[k]) + 1):
                    tot = tot + dir3[k, by]
                unit[k] = tot

        summed = pending
        pending = []
        with jax.named_scope("kunit"):
            packed = unit_of(core, (me[0] * 4 + me[1]) * 4 + me[2])[3]
            g_u = jnp.concatenate([unit[0], unit[1], unit[2, pl.ds(0, 32)]], 0)
            sj = jnp.broadcast_to(unit[2, pl.ds(32, 1)], (B, B))
            si = jnp.broadcast_to(unit[2, pl.ds(33, 1)], (B, B))
            si_c = jnp.broadcast_to(jnp.sum(jnp.where(eye, si, 0.0), axis=1, keepdims=True), (B, B))
            sj_c = jnp.broadcast_to(jnp.sum(jnp.where(eye, sj, 0.0), axis=1, keepdims=True), (B, B))
            lower = jnp.logical_and(packed, low)
            upper = jnp.logical_and(packed, jnp.logical_not(low))
            s_sum = jnp.where(lower, si_c, sj_c) + jnp.where(upper, sj, si)
            dist = jnp.maximum(s_sum - 2.0 * g_u, 0.0)
            k_u = jnp.exp(-dist / kern_width)
            z_u = unit[2, pl.ds(40, 8)]
            pieces = (k_u[:48], k_u[48:96], jnp.concatenate([k_u[96:], z_u, jnp.zeros_like(z_u)], 0))
            own = [chip_index(k, *me) for k in range(3)]
            for k in range(3):
                ag[k, own[k]] = pieces[k].astype(BF16)

        def place(ref, c, k, a, b, at):
            for v in range(4):
                coord = [0, 0, 0]
                for d, t in zip(perms[k], (a, b, v)):
                    coord[d] = t
                off = c * kc + coord[0]
                i = coord[1] * 4 + coord[2]
                top = (rem(i + off + 1, nb) + div(off * nb + i, 2 * n_chip - nb // 2) * (nb // 2)) * B + 48 * k
                n = (48, 48, 32)[k]
                kfull[pl.ds(pl.multiple_of(top, 16), n), blk(i)] = ref[k, at + v, pl.ds(0, n)]
                if k == 2:
                    tail = ref[k, at + v, pl.ds(32, 16)].astype(F32)
                    zt_b[pl.ds(pl.multiple_of(off * 8, 8), 8), blk(i)] = tail[:8]

        chunks = {}

        def chunk(k, ta, tb):
            if (k, ta, tb) not in chunks:
                p = perms[k]
                a, b = near[p[0]][ta], near[p[1]][tb]
                chunks[k, ta, tb] = (a, b, (a * 4 + b) * 4, 4)
            return chunks[k, ta, tb]

        def swap(k, ta, tb):
            a, b, at, n = chunk(k, ta, tb)
            return copy(("sw", k, ta, tb), ag.at[k, pl.ds(at, n)], ag_par.at[k, pl.ds(at, n)], partner)

        swaps = []
        placed = []

        def take(upto):
            while len(placed) < upto:
                k, ta, tb = swaps[len(placed)]
                swap(k, ta, tb).wait_recv()
                a, b, at, n = chunk(k, ta, tb)
                place(ag_par, 1 - core, k, a, b, at)
                placed.append((k, ta, tb))

        def have(k, ta, tb):
            swap(k, ta, tb).start()
            swaps.append((k, ta, tb))
            a, b, at, n = chunk(k, ta, tb)
            place(ag, core, k, a, b, at)

        def unit_copy(stage, k, by, tc, start):
            p = perms[k]
            a, b, at, n = chunk(k, 0, 0)
            at = at + near[p[2]][tc]
            m = copy(("u", stage, k, by, tc), ag.at[k, at], ag.at[k, at], shifted(p[stage], by))
            if start:
                m.start()
                pending.append(m)
            return m

        def a_copy(k, tb, tag, start=False):
            p = perms[k]
            ta, h, to = {"n1p": (0, 0, 1), "n1m": (0, 1, 3), "n2p": (0, 1, 1), "n2m": (0, 0, 3), "n3p": (3, 0, 1),
                         "n3m": (1, 1, 3)}[tag]
            a, b, at, n = chunk(k, ta, tb)
            half = split(n, True)[h]
            m = copy(("a", k, tb, tag), part_of(ag, k, at, half), part_of(ag, k, at, half), shifted(p[0], to))
            if start:
                m.start()
                pending.append(m)
            return m

        def a_launch(k, tb):
            for tag in ("n1p", "n1m", "n2p", "n2m"):
                a_copy(k, tb, tag, True)
            have(k, 0, tb)

        def a_relay(tb):
            for k in range(3):
                if True:
                    for got, out in (("n1p", "n3p"), ("n1m", "n3m")):
                        a_copy(k, tb, got).wait_recv()
                        a_copy(k, tb, out, True)

        def a_near(tb):
            for k in range(3):
                if True:
                    for got, ta in (("n2p", 3), ("n2m", 1)):
                        a_copy(k, tb, got).wait_recv()
                        have(k, ta, tb)

        def a_far(tb):
            for k in range(3):
                if True:
                    for got in ("n3p", "n3m"):
                        a_copy(k, tb, got).wait_recv()
                    have(k, 2, tb)

        def a_waves(tbs):
            for tb in tbs:
                for k in range(3):
                    a_launch(k, tb)

        with jax.named_scope("ag2"):
            for k in range(3):
                for by in (1, 2, 3):
                    unit_copy(2, k, by, 0, True)
            for k in range(3):
                for by in (2, 1, 3):
                    unit_copy(1, k, by, 0, True)
            for m in summed:
                m.wait_send()
            for by in (1, 3, 2):
                for k in range(3):
                    unit_copy(2, k, by, 0, False).wait_recv()
                    for bb in (2, 1, 3):
                        unit_copy(1, k, bb, 4 - by, True)
            a_waves((0,))

        def b_arrivals(bb):
            for k in range(3):
                for tc in range(4):
                    unit_copy(1, k, bb, tc, False).wait_recv()

        with jax.named_scope("ag1"):
            for name, stage, at, got in (("b1", b_arrivals, 1, 0), ("b3", b_arrivals, 3, 0), ("r0", a_relay, 0, 0),
                                         ("w", a_waves, (3, 1), 0), ("b2", b_arrivals, 2, 0), ("w2", a_waves, (2,), 0),
                                         ("n0", a_near, 0, 6), ("r3", a_relay, 3, 9), ("r1", a_relay, 1, 12),
                                         ("n3", a_near, 3, 15), ("r2", a_relay, 2, 18)):
                with jax.named_scope("ag1_" + name):
                    stage(at)
                    take(min(got, len(swaps) - 3))
        with jax.named_scope("ag0"):
            for stage, tb in ((a_far, 0), (a_near, 1), (a_far, 3), (a_near, 2), (a_far, 1), (a_far, 2)):
                before = len(swaps)
                with jax.named_scope("ag0_%s%d" % (stage.__name__, tb)):
                    stage(tb)
                take(before - 12)

        per = 8

        def mirror(c, r, cc):
            at = []
            for t in range(per):
                u, i, j, packed = unit_of(c, r * per + t)
                at.append((i, j, kfull[blk(j), blk(i)].T))
            for i, j, m in at:
                kfull[blk(i), blk(j)] = m
            return cc

        def unpack(r, cc):
            both = []
            for v in range(4):
                i = r * 4 + v + nb // 2
                m = kfull[blk(i), blk(i)].astype(F32)
                mt = m.T
                both.append((jnp.where(eye, 1.0, jnp.where(low, m, mt)), jnp.where(eye, 1.0, jnp.where(low, mt, m))))
            for v, (m, mt) in enumerate(both):
                t = r * 4 + v
                kfull[blk(t + nb // 2), blk(t + nb // 2)] = m.astype(BF16)
                kfull[blk(t), blk(t)] = mt.astype(BF16)
            return cc
        with jax.named_scope("mirror1"):
            lax.fori_loop(0, div(n_chip - core * (nb // 2), per), functools.partial(mirror, core), 0)
        with jax.named_scope("swapwait"):
            take(len(swaps))
        with jax.named_scope("mirror2"):
            lax.fori_loop(0, div(n_chip - (1 - core) * (nb // 2), per), functools.partial(mirror, 1 - core), 0)
            lax.fori_loop(0, nb // 8, unpack, 0)

        def grads(r, cc):
            lowt = lax.dot_general(zt_b[:, panel(r)].astype(BF16), fact_ref[...], TN, preferred_element_type=F32)
            a_buf[panel(r)] = (-((get_rows(r) - mu_ref[...]) * lam_ref[...] + lowt)).astype(BF16)
            return cc
        with jax.named_scope("grads"):
            lax.fori_loop(0, n_panels, grads, 0, unroll=2)

        def update(h, cc):
            done = []
            for t in range(2):
                r = rem(me[2] + 2 + 2 * h + t, 4)
                kr = kfull[panel(r)]
                mass = jnp.sum(kr.astype(F32), axis=1, keepdims=True)
                drive = jnp.dot(kr, a_buf[...], preferred_element_type=F32)
                pull = jnp.dot(kr, t_own[slot], preferred_element_type=F32)
                upd = (drive + (2.0 / kern_width) * (mass * t_own[slot, panel(r)].astype(F32) - pull)) / n_total
                theta = get_rows(r) + step_size * upd
                for v in range(4):
                    th[r, v] = theta[v * B:(v + 1) * B]
                done.append(r)

            @pl.when(step < NUM_STEPS - 1)
            def _():
                for r in done:
                    prepare(r, get_rows(r), 1 - slot)

            for o in range(4):
                @pl.when(jnp.logical_and(step == NUM_STEPS - 1, h == (o + 2) % 4 // 2))
                def _():
                    out_start(o)
            return cc
        with jax.named_scope("update"):
            lax.fori_loop(0, n_panels // 2, update, 0)
        with jax.named_scope("sendwait"):
            for m in pending:
                m.wait_send()
            for k, ta, tb in swaps:
                swap(k, ta, tb).wait_send()
        return carry

    lax.fori_loop(0, NUM_STEPS, one_step, 0)

    def out_second(h):
        d = 1 + h

        def place_of(src_at, v):
            return out_ref.at[pl.ds(h * hb, hb), cols(src_at, v) if h == 0 else cols(v, src_at)]

        def sends(tag):
            way = tag[1] == "+"
            b = 0 if way else 1
            if tag[0] == "f":
                return [(rel3.at[h, b, t], place_of(side(d, 3 if way else 1), 2 * b + t)) for t in range(2)]
            to = side(d, {"r": 2, "d": 1 if way else 3}[tag[0]])
            if tag[0] == "r":
                return [(m1.at[h, v, to], rel3.at[h, b, v % 2]) for v in halves(tag)]
            return [(m1.at[h, v, to], place_of(me[d], v)) for v in range(4)]
        return relayed(("out2", h), d, sends)

    with jax.named_scope("out1"):
        first = [out_first(h)[:3] for h in range(2)]
        for v in range(4):
            m1[0, me[2], v] = th[me[2], v, pl.ds(0, hb)]
            m1[1, me[1], v] = th[v, me[1], pl.ds(hb, hb)]
        for relay, finish, started in first:
            relay()
    with jax.named_scope("out2"):
        second = []
        for h, (relay, finish, started) in enumerate(first):
            finish()
            second.append(out_second(h))
        own_out = []
        for v in range(4):
            own_out.append(local(("back", v), m1.at[0, v, me[1]], out_ref.at[pl.ds(0, hb), cols(me[1], v)]))
            own_out.append(local(("back", 4 + v), m1.at[1, v, me[2]], out_ref.at[pl.ds(hb, hb), cols(v, me[2])]))
        for m in own_out:
            m.start()
        for relay, finish, started in second:
            relay()
        for relay, finish, started in second:
            finish()
        for relay, finish, started in first + second:
            for m in started:
                m.wait_send()
        for m in own_out:
            m.wait()


def run_steps(theta, lam, mu, fac, sizes, kern_width, step_size):
    n_total, fcol = theta.shape[0] * sizes[1] * sizes[2], theta.shape[1] // (sizes[1] * sizes[2])
    rank = fac.shape[1]
    nb = n_total // B
    n_chip = sizes[0] * sizes[1] * sizes[2]
    assert nb * nb == 4 * n_chip and rank == 4 * nb
    hb = B // 2
    cfg = dict(sizes=sizes, nb=nb, kern_width=kern_width, step_size=step_size)
    n1, n2 = n_chip, n_chip
    vmem = pl.BlockSpec(memory_space=pltpu.VMEM)
    most1 = max(n_chip // sizes[k] for k in range(3))
    most2 = max(sizes)
    blocks = (4, 4, B, fcol)
    scratch = [
        pltpu.VMEM(blocks, F32),
        pltpu.VMEM((2, 4, hb, 4 * fcol), F32),
        pltpu.VMEM((2, 4, 4, hb, fcol), F32),
        pltpu.VMEM((2, 2, hb // 2, 4 * fcol), F32),
        pltpu.VMEM((2, 2, 2, hb, fcol), F32),
        pltpu.VMEM((2, 2, 2, hb, fcol), F32),
        pltpu.VMEM((1, fcol), F32),
        pltpu.VMEM((1, fcol), F32),
        pltpu.VMEM((rank, fcol), BF16),
        pltpu.VMEM((2, n_total, fcol), BF16),
        pltpu.VMEM((n_total, fcol), BF16),
        pltpu.VMEM((n_total, fcol), BF16),
        pltpu.VMEM((rank, n_total), F32),
        pltpu.VMEM((rank // 2, n_total), F32),
        pltpu.VMEM((rank, n_total), F32),
        pltpu.VMEM((nb, 8, B), F32),
        pltpu.VMEM((nb, B, B), F32),
        pltpu.VMEM((3, n_chip, PIECE, B), F32),
        pltpu.VMEM((3, 4, most1, PIECE, B), F32),
        pltpu.VMEM((3, 2, 2, PIECE, B), F32),
        pltpu.VMEM((3, 4, most2, PIECE, B), F32),
        pltpu.VMEM((3, 4, PIECE, B), F32),
        pltpu.VMEM((3, most1, PIECE, B), F32),
        pltpu.VMEM((3, most2, PIECE, B), F32),
        pltpu.VMEM((3, PIECE, B), F32),
        pltpu.VMEM((3, n_chip, PIECE, B), BF16),
        pltpu.VMEM((3, n_chip, PIECE, B), BF16),
        pltpu.VMEM((n_total, n_total), BF16),
        pltpu.SemaphoreType.DMA((NUM_SEMS,)),
        pltpu.SemaphoreType.DMA((NUM_SEMS,)),
    ]
    hbm = pl.BlockSpec(memory_space=pltpu.HBM)
    return pl.pallas_call(
        functools.partial(steps_kernel, cfg),
        out_shape=jax.ShapeDtypeStruct(theta.shape, F32),
        in_specs=[hbm, vmem, vmem, hbm],
        out_specs=hbm,
        scratch_shapes=scratch,
        compiler_params=pltpu.CompilerParams(collective_id=0, has_side_effects=True, vmem_limit_bytes=60 * 1024 * 1024),
        name="svgd_steps",
    )(theta, lam[None], mu[None], fac.T)


def solution(mesh, sizes=(4, 4, 4)):
    part_size = mesh.shape["part"]
    feat_size = mesh.shape["feat"]

    def local_steps(local_theta, prec_loc, mean_loc, factor_loc):
        rows_loc, feat_loc = local_theta.shape
        n_total = rows_loc * part_size
        feat_total = feat_loc * feat_size
        kern_width = 2.0 * feat_total / math.log(n_total)
        step_size = 0.15 * n_total * feat_total / math.log(n_total)
        return run_steps(local_theta, prec_loc, mean_loc, factor_loc, sizes, kern_width, step_size)

    row_spec = P(("ens", "part"), "feat")
    vec_spec = P(("ens", "feat"))
    fac_spec = P(("ens", "feat"), None)
    return jax.shard_map(local_steps, mesh=mesh, in_specs=(row_spec, vec_spec, vec_spec, fac_spec), out_specs=row_spec, check_vma=False)
```

```python
import functools
import math
import jax
import jax.numpy as jnp
from jax import lax
from jax.experimental import pallas as pl
from jax.experimental.pallas import tpu as pltpu
from jax.sharding import PartitionSpec as P

NUM_STEPS = 3
B = 128
PIECE = 48
F32 = jnp.float32
BF16 = jnp.bfloat16
NT = (((1,), (1,)), ((), ()))
TN = (((0,), (0,)), ((), ()))
NUM_SEMS = 416
PANEL = 512


def rem(a, n):
    return lax.rem(a, jnp.int32(n))


def div(a, n):
    return lax.div(a, jnp.int32(n))


def unrolled(count, by, body):
    def several(r, cc):
        for t in range(by):
            body(r * by + t)
        return cc
    lax.fori_loop(0, count // by, several, 0)


def mine(ref, h, v, src_at):
    hb = B // 2
    return ref.at[src_at, v, pl.ds(0, hb)] if h == 0 else ref.at[v, src_at, pl.ds(hb, hb)]


def steps_kernel(cfg, theta_ref, lam_all, mu_all, fact_all, out_ref, th, l1, m1, rel1, rel2, rel3, lam_ref, mu_ref, fact_ref,
                 t_own, t_par, a_buf, zt, zt_par, zt_b, s_all, d_all, g, ring1, relb, dirb, dir3, acc2, acc3, unit, ag,
                 ag_par, kfull, send_sems, recv_sems):
    nb, kern_width, step_size = cfg["nb"], cfg["kern_width"], cfg["step_size"]
    n_total = nb * B
    n_chip = 64
    part, feat = lax.axis_index("part"), lax.axis_index("feat")
    core = rem(feat, 2)
    me = (div(feat, 2), rem(part, 4), div(part, 4))
    near = [[me[d]] + [rem(me[d] + by, 4) for by in (1, 2, 3)] for d in range(3)]

    def dev(coord, c):
        return {"part": coord[2] * 4 + coord[1], "feat": coord[0] * 2 + c}

    def device_at(dim, by):
        c = list(me)
        c[dim] = near[dim][by]
        return dev(c, core)

    around = [[device_at(d, by) for by in range(4)] for d in range(3)]

    def shifted(dim, by):
        return around[dim][by]

    partner = dev(me, 1 - core)
    perms = [(k, (k + 1) % 3, (k + 2) % 3) for k in range(3)]

    ids = {}

    def slot_of(key):
        idx = ids.setdefault(key, len(ids))
        assert idx < NUM_SEMS - 8
        return idx

    def copy(key, src, dst, to):
        idx = slot_of(key)
        return pltpu.make_async_remote_copy(
            src_ref=src, dst_ref=dst, send_sem=send_sems.at[idx], recv_sem=recv_sems.at[idx],
            device_id=to, device_id_type=pl.DeviceIdType.MESH)

    def local(key, src, dst):
        return pltpu.make_async_copy(src, dst, send_sems.at[slot_of(key)])

    barrier = pltpu.get_barrier_semaphore()
    peers = [partner] + [shifted(d, by) for d in range(3) for by in (1, 2, 3)]
    for peer in peers:
        pl.semaphore_signal(barrier, inc=1, device_id=peer, device_id_type=pl.DeviceIdType.MESH)
    pl.semaphore_wait(barrier, len(peers))

    row = lax.broadcasted_iota(jnp.int32, (B, B), 0)
    col = lax.broadcasted_iota(jnp.int32, (B, B), 1)
    low, eye = row >= col, row == col

    def blk(i):
        return pl.ds(pl.multiple_of(i * B, B), B)

    def unit_of(c, q):
        u = c * n_chip + q
        i = rem(u, nb)
        return u, i, rem(i + div(u, nb) + 1, nb), u >= 2 * n_chip - nb // 2

    def chip_index(k, x, y, z):
        p = perms[k]
        c = (x, y, z)
        return (c[p[0]] * 4 + c[p[1]]) * 4 + c[p[2]]

    def split(n, wide):
        if n > 1:
            return (0, n // 2, 0, PIECE), (n // 2, n // 2, 0, PIECE)
        r = 32 if wide else 24
        return (0, 1, 0, r), (0, 1, r, PIECE - r)

    def part_of(ref, lead, base, half):
        return ref.at[lead, pl.ds(base + half[0], half[1]), pl.ds(half[2], half[3])]

    zh = zt.shape[0] // 2
    kc = nb // 4
    n_panels = n_total // PANEL

    def panel(r):
        return pl.ds(pl.multiple_of(r * PANEL, PANEL), PANEL)

    def swap_t(r, slot):
        return pltpu.make_async_remote_copy(
            src_ref=t_own.at[slot, panel(r)], dst_ref=t_par.at[panel(r)], send_sem=send_sems.at[NUM_SEMS - 1 - r],
            recv_sem=recv_sems.at[NUM_SEMS - 1 - r], device_id=partner, device_id_type=pl.DeviceIdType.MESH)

    def swap_z(r):
        return pltpu.make_async_remote_copy(
            src_ref=zt.at[pl.ds(pl.multiple_of((1 - core) * zh, 8), zh), panel(r)], dst_ref=zt_par.at[pl.ds(0, zh), panel(r)],
            send_sem=send_sems.at[NUM_SEMS - 1 - n_panels - r], recv_sem=recv_sems.at[NUM_SEMS - 1 - n_panels - r],
            device_id=partner, device_id_type=pl.DeviceIdType.MESH)

    def prepare(r, theta, slot):
        t_own[slot, panel(r)] = theta.astype(BF16)
        swap_t(r, slot).start()
        xb = (theta - mu_ref[...]).astype(BF16)
        zt[:, panel(r)] = lax.dot_general(fact_ref[...], xb, NT, preferred_element_type=F32)
        swap_z(r).start()

    def get_rows(r):
        return jnp.concatenate([th[r, v] for v in range(4)], 0)

    def first_prep(r, cc):
        prepare(r, get_rows(r), 0)
        return cc
    fcol, hb = fact_ref.shape[1], B // 2
    my = pl.ds(pl.multiple_of((me[1] * 4 + me[2]) * fcol, fcol), fcol)

    def cols(y, z, n=1):
        return pl.ds(pl.multiple_of((y * 4 + z) * fcol, fcol), n * fcol)

    def side(d, by):
        return near[d][by]

    def relayed(key, d, sends, begin=True):
        def copies(tag):
            return [copy((key, tag, t), src, dst, shifted(d, 1 if tag[1] == "+" else 3))
                    for t, (src, dst) in enumerate(sends(tag))]
        started = []

        def go(tags):
            for tag in tags:
                for m in copies(tag):
                    m.start()
                    started.append(m)

        def relay():
            for got, out in (("r+", "f+"), ("r-", "f-")):
                for m in copies(got):
                    m.wait_recv()
                go((out,))

        def finish():
            for tag in ("d+", "d-", "f+", "f-"):
                for m in copies(tag):
                    m.wait_recv()
        if begin:
            go(("r+", "r-", "d+", "d-"))
        else:
            for tag in ("r+", "r-", "d+", "d-"):
                started += copies(tag)
        return relay, finish, started, copies

    def halves(tag):
        if tag[0] == "d":
            return (0, 1, 2, 3)
        return (0, 1) if tag[1] == "+" else (2, 3)

    def in_first(h):
        d = 1 + h

        def sends(tag):
            r0, nr = {"r+": (0, hb // 2), "r-": (hb // 2, hb // 2)}.get(tag, (0, hb))
            way = tag[1] == "+"
            if tag[0] == "f":
                b = 0 if way else 1
                return [(rel1.at[h, b], l1.at[h, side(d, 3 if way else 1), pl.ds(b * (hb // 2), hb // 2)])]
            to = side(d, {"r": 2, "d": 1 if way else 3}[tag[0]])
            rows = pl.ds(h * hb + r0, nr)

            def dst(y, n):
                at = pl.ds(y * fcol, n * fcol)
                if tag[0] == "d":
                    return l1.at[h, me[d], pl.ds(0, nr), at]
                return rel1.at[h, 0 if way else 1, pl.ds(0, nr), at]
            if h == 0:
                return [(theta_ref.at[rows, cols(to, 0, 4)], dst(0, 4))]
            return [(theta_ref.at[rows, cols(y, to)], dst(y, 1)) for y in range(4)]
        return relayed(("in1", h), d, sends)

    def pieces(tag):
        return (0, 3, 1, 2) if tag[0] == "d" else (0, 3) if tag[1] == "+" else (1, 2)

    def start_piece(leg, o):
        for tag in ("r+" if o in (0, 3) else "r-", "d+", "d-"):
            leg[3](tag)[pieces(tag).index(o)].start()

    def two_legs(first, second):
        for h in range(2):
            first[h][0]()
        for tag, o in (("d+", 3), ("d-", 1)):
            for h in range(2):
                for m in first[h][3](tag):
                    m.wait_recv()
                start_piece(second[h], o)
        for h in range(2):
            for tag in ("f+", "f-"):
                for m in first[h][3](tag):
                    m.wait_recv()
            start_piece(second[h], 2)

    def close(first, second):
        for h in range(2):
            second[h][0]()
        for h in range(2):
            second[h][1]()
        for leg in first + second:
            for m in leg[2]:
                m.wait_send()

    def in_second(h):
        d = 2 - h

        def sends(tag):
            way = tag[1] == "+"
            b = 0 if way else 1
            out = []
            to = side(d, {"r": 2, "d": 1 if way else 3, "f": 0}[tag[0]])
            for at, o in enumerate(pieces(tag)):
                v = near[1 + h][o]
                if tag[0] == "f":
                    out.append((rel2.at[h, b, at], mine(th, h, v, side(d, 3 if way else 1))))
                    continue
                if o == 0:
                    src = theta_ref.at[pl.ds(h * hb, hb), cols(me[1], to) if h == 0 else cols(to, me[2])]
                else:
                    src = l1.at[h, v, pl.ds(0, hb), pl.ds(pl.multiple_of(to * fcol, fcol), fcol)]
                out.append((src, mine(th, h, v, me[d]) if tag[0] == "d" else rel2.at[h, b, at]))
            return out
        return relayed(("in2", h), d, sends, begin=False)

    own_in = [local(("own", 0), theta_ref.at[pl.ds(0, hb), cols(me[1], 0, 4)], l1.at[0, me[1]])]
    own_in += [local(("own", 1 + y), theta_ref.at[pl.ds(hb, hb), cols(y, me[2])],
                     l1.at[1, me[2], pl.ds(0, hb), pl.ds(y * fcol, fcol)]) for y in range(4)]
    own_in.append(local(("own", 5), fact_all.at[pl.ds(0, fact_ref.shape[0]), my], fact_ref))

    with jax.named_scope("in1"):
        first = [in_first(h) for h in range(2)]
        second = [in_second(h) for h in range(2)]
        for m in own_in:
            m.start()
        for h in range(2):
            start_piece(second[h], 0)
        lam_ref[...] = lam_all[pl.ds(0, 1), my]
        mu_ref[...] = mu_all[pl.ds(0, 1), my]
    with jax.named_scope("in2"):
        two_legs(first, second)
        for m in own_in:
            m.wait()
        for v in range(4):
            th[me[2], v, pl.ds(0, hb)] = l1[0, v, pl.ds(0, hb), pl.ds(pl.multiple_of(me[2] * fcol, fcol), fcol)]
            th[v, me[1], pl.ds(hb, hb)] = l1[1, v, pl.ds(0, hb), pl.ds(pl.multiple_of(me[1] * fcol, fcol), fcol)]
        close(first, second)

    with jax.named_scope("prep"):
        lax.fori_loop(0, n_panels, first_prep, 0)

    def out_pieces(h, tag):
        if h == 0:
            return halves(tag)
        return (0, 1, 2, 3) if tag[0] == "d" else (2, 3) if tag[1] == "+" else (0, 1)

    def out_first(h):
        d = 2 - h

        def sends(tag):
            way = tag[1] == "+"
            b = 0 if way else 1
            vs = [(v if h == 0 else near[2][v], v % 2) for v in out_pieces(h, tag)]
            if tag[0] == "f":
                return [(rel2.at[h, b, at], m1.at[h, side(d, 3 if way else 1), v]) for v, at in vs]
            to = side(d, {"r": 2, "d": 1 if way else 3}[tag[0]])
            return [(mine(th, h, v, to), m1.at[h, me[d], v] if tag[0] == "d" else rel2.at[h, b, at]) for v, at in vs]
        return relayed(("out1", h), d, sends, begin=False)

    def out_start(o):
        for tag in ((), ("d+",), ("r+", "r-"), ("d-",))[o]:
            for m in out_first(0)[3](tag):
                m.start()
        for tag in ("r+" if o >= 2 else "r-", "d+", "d-"):
            out_first(1)[3](tag)[out_pieces(1, tag).index(o)].start()

    def one_step(step, carry):
        slot = rem(step, 2)
        with jax.named_scope("twait"):
            for r in range(n_panels):
                swap_t(r, slot).wait()
                swap_z(r).wait()

        def products(rows, cols):
            return (lax.dot_general(jnp.concatenate([t_own[slot, r] for r in rows], 0), t_own[slot, cols], NT,
                                    preferred_element_type=F32)
                    + lax.dot_general(jnp.concatenate([t_par[r] for r in rows], 0), t_par[cols], NT,
                                      preferred_element_type=F32))

        def put(m, x, y, z):
            g[0, chip_index(0, x, y, z)] = m[:48]
            g[1, chip_index(1, x, y, z)] = m[48:96]
            g[2, chip_index(2, x, y, z), pl.ds(0, 32)] = m[96:]

        def form(h, cc):
            i = h * 2
            cols = pl.ds(pl.multiple_of(i * B, 2 * B), 2 * B)
            dg = products([cols], cols)
            for t in range(2):
                dt = dg[t * B:(t + 1) * B, t * B:(t + 1) * B]
                d_all[i + t] = dt
                s_all[i + t] = jnp.broadcast_to(jnp.sum(jnp.where(eye, dt, 0.0), axis=0, keepdims=True), (8, B))
            m = products([blk(rem(i + core * kc + 1 + t, nb)) for t in range(kc + 1)], cols)
            y, z = div(h, 2), 2 * rem(h, 2)
            for t in range(kc + 1):
                if t < kc:
                    put(m[t * B:(t + 1) * B, :B], t, y, z)
                if t > 0:
                    put(m[t * B:(t + 1) * B, B:], t - 1, y, z + 1)
            return cc
        with jax.named_scope("form"):
            lax.fori_loop(0, nb // 2, form, 0, unroll=4)

        with jax.named_scope("pair"):
            @pl.when(core == 1)
            def _():
                def pair(t, cc):
                    i = t + nb // 2
                    put(jnp.where(low, d_all[i], d_all[t]), 3, div(i, 4), rem(i, 4))
                    return cc
                lax.fori_loop(0, nb // 2, pair, 0)

        pending = []

        order = (2, 1, 3, 0)
        wave_base = [[[(near[perms[k][0]][t] * 4 + near[perms[k][1]][o]) * 4 for t in range(4)] for o in order]
                     for k in range(3)]

        def wave(k, s):
            return perms[k], 4, order[s], wave_base[k][s]

        def n_waves(k):
            return 4

        def ring_copy(k, s, tag):
            p, n, by, base = wave(k, s)
            ha, hb = split(n, False)
            at, half, kind, to = {
                "m1p": (2, ha, 0, 1), "m1m": (2, hb, 1, 3), "m2p": (1, hb, 2, 1), "m2m": (3, ha, 3, 3),
                "m3p": (1, ha, 2, 1), "m3m": (3, hb, 3, 3)}[tag]
            return copy(("rs", k, s, tag), part_of(g, k, base[at], half), part_of(ring1.at[k], kind, s * n, half),
                        shifted(p[0], to))

        def ring_start(s, tags, colours=(0, 1, 2)):
            for tag in tags:
                for k in colours:
                    if s < n_waves(k):
                        m = ring_copy(k, s, tag)
                        m.start()
                        pending.append(m)

        def ring_merge(s):
            for k in range(3):
                p, n, by, base = wave(k, s)
                ha, hb = split(n, False)
                for got, out, at, half, kind in (("m1p", "m3p", 1, ha, 0), ("m1m", "m3m", 3, hb, 1)):
                    ring_copy(k, s, got).wait_recv()
                    part_of(g, k, base[at], half)[...] += part_of(ring1.at[k], kind, s * n, half)[...]
                    m = ring_copy(k, s, out)
                    m.start()
                    pending.append(m)

        def owner_copy(k, by, s):
            return copy(("rb", k, by), acc2.at[k, pl.ds(s * 4, 4)], dirb.at[k, by], shifted(perms[k][1], by))

        def via_copy(k, b):
            return copy(("rv", k, b), acc2.at[k, pl.ds(2 * b, 2)], relb.at[k, b], shifted(perms[k][1], (1, 3)[b]))

        def ring_finish(s):
            for k in range(3):
                p, n, by, base = wave(k, s)
                for tag in ("m2p", "m2m", "m3p", "m3m"):
                    ring_copy(k, s, tag).wait_recv()
                if by in (1, 3):
                    via_copy(k, by // 2).wait_recv()
                for v in range(n):
                    tot = g[k, base[0] + v] + ring1[k, 2, s * n + v] + ring1[k, 3, s * n + v]
                    if by in (1, 3) and v // 2 == by // 2:
                        tot = tot + relb[k, by // 2, v % 2]
                    acc2[k, s * n + v] = tot
                ms = [via_copy(k, 0), via_copy(k, 1)] if by == 2 else [owner_copy(k, by, s)] if by else []
                for m in ms:
                    m.start()
                    pending.append(m)

        ring_start(0, ("m1p", "m1m"), (0, 1))

        row8 = lax.broadcasted_iota(jnp.int32, (8, B), 0)

        def tails(i, cc):
            y, z = div(i, 4), rem(i, 4)
            for x in range(4):
                off = core * kc + x
                at = chip_index(2, x, y, z)
                g[2, at, pl.ds(32, 8)] = jnp.where(row8 == 0, s_all[rem(i + off + 1, nb)], s_all[i])
                g[2, at, pl.ds(40, 8)] = (zt[pl.ds(pl.multiple_of(off * 8, 8), 8), blk(i)]
                                          + zt_par[pl.ds(x * 8, 8), blk(i)])
            return cc
        with jax.named_scope("tails"):
            lax.fori_loop(0, nb, tails, 0)

        most = 4
        with jax.named_scope("rs0"):
            ring_start(0, ("m1p", "m1m"), (2,))
            ring_start(0, ("m2p", "m2m"))
            ring_start(1, ("m1p", "m1m"))
            for s in range(most):
                ring_merge(s)
                ring_start(s + 1, ("m2p", "m2m"))
                ring_start(s + 2, ("m1p", "m1m"))
                if s:
                    ring_finish(s - 1)
            ring_finish(most - 1)
        last = []
        with jax.named_scope("rs1"):
            for k in range(3):
                p = perms[k]
                n, s = 4, 3
                bys = (1, 3)
                for by in bys:
                    owner_copy(k, by, 0).wait_recv()
                for v in range(n):
                    tot = acc2[k, s * n + v]
                    for by in bys:
                        tot = tot + dirb[k, by, v]
                    acc3[k, v] = tot
                ms = []
                for by in (1, 2, 3):
                    m = copy(("rc", k, by), acc3.at[k, near[p[2]][by]], dir3.at[k, by],
                             shifted(p[2], by))
                    m.start()
                    ms.append(m)
                last.append(ms)
                pending += ms
        with jax.named_scope("rs2"):
            for k in range(3):
                tot = acc3[k, me[perms[k][2]]]
                for m in last[k]:
                    m.wait_recv()
                for by in range(1, len(last[k]) + 1):
                    tot = tot + dir3[k, by]
                unit[k] = tot

        summed = pending
        pending = []
        with jax.named_scope("kunit"):
            packed = unit_of(core, (me[0] * 4 + me[1]) * 4 + me[2])[3]
            g_u = jnp.concatenate([unit[0], unit[1], unit[2, pl.ds(0, 32)]], 0)
            sj = jnp.broadcast_to(unit[2, pl.ds(32, 1)], (B, B))
            si = jnp.broadcast_to(unit[2, pl.ds(33, 1)], (B, B))
            si_c = jnp.broadcast_to(jnp.sum(jnp.where(eye, si, 0.0), axis=1, keepdims=True), (B, B))
            sj_c = jnp.broadcast_to(jnp.sum(jnp.where(eye, sj, 0.0), axis=1, keepdims=True), (B, B))
            lower = jnp.logical_and(packed, low)
            upper = jnp.logical_and(packed, jnp.logical_not(low))
            s_sum = jnp.where(lower, si_c, sj_c) + jnp.where(upper, sj, si)
            dist = jnp.maximum(s_sum - 2.0 * g_u, 0.0)
            k_u = jnp.exp(-dist / kern_width)
            z_u = unit[2, pl.ds(40, 8)]
            pieces = (k_u[:48], k_u[48:96], jnp.concatenate([k_u[96:], z_u, jnp.zeros_like(z_u)], 0))
            own = [chip_index(k, *me) for k in range(3)]
            for k in range(3):
                ag[k, own[k]] = pieces[k].astype(BF16)

        def place(ref, c, k, a, b, at):
            for v in range(4):
                coord = [0, 0, 0]
                for d, t in zip(perms[k], (a, b, v)):
                    coord[d] = t
                off = c * kc + coord[0]
                i = coord[1] * 4 + coord[2]
                top = (rem(i + off + 1, nb) + div(off * nb + i, 2 * n_chip - nb // 2) * (nb // 2)) * B + 48 * k
                n = (48, 48, 32)[k]
                kfull[pl.ds(pl.multiple_of(top, 16), n), blk(i)] = ref[k, at + v, pl.ds(0, n)]
                if k == 2:
                    tail = ref[k, at + v, pl.ds(32, 16)].astype(F32)
                    zt_b[pl.ds(pl.multiple_of(off * 8, 8), 8), blk(i)] = tail[:8]

        chunks = {}

        def chunk(k, ta, tb):
            if (k, ta, tb) not in chunks:
                p = perms[k]
                a, b = near[p[0]][ta], near[p[1]][tb]
                chunks[k, ta, tb] = (a, b, (a * 4 + b) * 4, 4)
            return chunks[k, ta, tb]

        def swap(k, ta, tb):
            a, b, at, n = chunk(k, ta, tb)
            return copy(("sw", k, ta, tb), ag.at[k, pl.ds(at, n)], ag_par.at[k, pl.ds(at, n)], partner)

        swaps = []
        placed = []

        def take(upto):
            while len(placed) < upto:
                k, ta, tb = swaps[len(placed)]
                swap(k, ta, tb).wait_recv()
                a, b, at, n = chunk(k, ta, tb)
                place(ag_par, 1 - core, k, a, b, at)
                placed.append((k, ta, tb))

        def have(k, ta, tb):
            swap(k, ta, tb).start()
            swaps.append((k, ta, tb))
            a, b, at, n = chunk(k, ta, tb)
            place(ag, core, k, a, b, at)

        def unit_copy(stage, k, by, tc, start):
            p = perms[k]
            a, b, at, n = chunk(k, 0, 0)
            at = at + near[p[2]][tc]
            m = copy(("u", stage, k, by, tc), ag.at[k, at], ag.at[k, at], shifted(p[stage], by))
            if start:
                m.start()
                pending.append(m)
            return m

        def a_copy(k, tb, tag, start=False):
            p = perms[k]
            ta, h, to = {"n1p": (0, 0, 1), "n1m": (0, 1, 3), "n2p": (0, 1, 1), "n2m": (0, 0, 3), "n3p": (3, 0, 1),
                         "n3m": (1, 1, 3)}[tag]
            a, b, at, n = chunk(k, ta, tb)
            half = split(n, True)[h]
            m = copy(("a", k, tb, tag), part_of(ag, k, at, half), part_of(ag, k, at, half), shifted(p[0], to))
            if start:
                m.start()
                pending.append(m)
            return m

        def a_launch(k, tb):
            for tag in ("n1p", "n1m", "n2p", "n2m"):
                a_copy(k, tb, tag, True)
            have(k, 0, tb)

        def a_relay(tb):
            for k in range(3):
                if True:
                    for got, out in (("n1p", "n3p"), ("n1m", "n3m")):
                        a_copy(k, tb, got).wait_recv()
                        a_copy(k, tb, out, True)

        def a_near(tb):
            for k in range(3):
                if True:
                    for got, ta in (("n2p", 3), ("n2m", 1)):
                        a_copy(k, tb, got).wait_recv()
                        have(k, ta, tb)

        def a_far(tb):
            for k in range(3):
                if True:
                    for got in ("n3p", "n3m"):
                        a_copy(k, tb, got).wait_recv()
                    have(k, 2, tb)

        def a_waves(tbs):
            for tb in tbs:
                for k in range(3):
                    a_launch(k, tb)

        with jax.named_scope("ag2"):
            for k in range(3):
                for by in (1, 2, 3):
                    unit_copy(2, k, by, 0, True)
            for k in range(3):
                for by in (2, 1, 3):
                    unit_copy(1, k, by, 0, True)
            for m in summed:
                m.wait_send()
            for by in (1, 3, 2):
                for k in range(3):
                    unit_copy(2, k, by, 0, False).wait_recv()
                    for bb in (2, 1, 3):
                        unit_copy(1, k, bb, 4 - by, True)
            a_waves((0,))

        def b_arrivals(bb):
            for k in range(3):
                for tc in range(4):
                    unit_copy(1, k, bb, tc, False).wait_recv()

        with jax.named_scope("ag1"):
            for name, stage, at, got in (("b1", b_arrivals, 1, 0), ("b3", b_arrivals, 3, 0), ("r0", a_relay, 0, 0),
                                         ("w", a_waves, (3, 1), 0), ("b2", b_arrivals, 2, 0), ("w2", a_waves, (2,), 0),
                                         ("n0", a_near, 0, 6), ("r3", a_relay, 3, 9), ("r1", a_relay, 1, 12),
                                         ("n3", a_near, 3, 15), ("r2", a_relay, 2, 18)):
                with jax.named_scope("ag1_" + name):
                    stage(at)
                    take(min(got, len(swaps) - 3))
        with jax.named_scope("ag0"):
            for stage, tb in ((a_far, 0), (a_near, 1), (a_far, 3), (a_near, 2), (a_far, 1), (a_far, 2)):
                before = len(swaps)
                with jax.named_scope("ag0_%s%d" % (stage.__name__, tb)):
                    stage(tb)
                take(before - 12)

        per = 8

        def mirror(c, r, cc):
            at = []
            for t in range(per):
                u, i, j, packed = unit_of(c, r * per + t)
                at.append((i, j, kfull[blk(j), blk(i)].T))
            for i, j, m in at:
                kfull[blk(i), blk(j)] = m
            return cc

        def unpack(r, cc):
            both = []
            for v in range(4):
                i = r * 4 + v + nb // 2
                m = kfull[blk(i), blk(i)].astype(F32)
                mt = m.T
                both.append((jnp.where(eye, 1.0, jnp.where(low, m, mt)), jnp.where(eye, 1.0, jnp.where(low, mt, m))))
            for v, (m, mt) in enumerate(both):
                t = r * 4 + v
                kfull[blk(t + nb // 2), blk(t + nb // 2)] = m.astype(BF16)
                kfull[blk(t), blk(t)] = mt.astype(BF16)
            return cc
        with jax.named_scope("mirror1"):
            lax.fori_loop(0, div(n_chip - core * (nb // 2), per), functools.partial(mirror, core), 0)
        with jax.named_scope("swapwait"):
            take(len(swaps))
        with jax.named_scope("mirror2"):
            lax.fori_loop(0, div(n_chip - (1 - core) * (nb // 2), per), functools.partial(mirror, 1 - core), 0)
            lax.fori_loop(0, nb // 8, unpack, 0)

        def grads(r, cc):
            lowt = lax.dot_general(zt_b[:, panel(r)].astype(BF16), fact_ref[...], TN, preferred_element_type=F32)
            a_buf[panel(r)] = (-((get_rows(r) - mu_ref[...]) * lam_ref[...] + lowt)).astype(BF16)
            return cc
        with jax.named_scope("grads"):
            lax.fori_loop(0, n_panels, grads, 0, unroll=2)

        def update(h, cc):
            done = []
            for t in range(2):
                r = rem(me[2] + 2 + 2 * h + t, 4)
                kr = kfull[panel(r)]
                mass = jnp.sum(kr.astype(F32), axis=1, keepdims=True)
                drive = jnp.dot(kr, a_buf[...], preferred_element_type=F32)
                pull = jnp.dot(kr, t_own[slot], preferred_element_type=F32)
                upd = (drive + (2.0 / kern_width) * (mass * t_own[slot, panel(r)].astype(F32) - pull)) / n_total
                theta = get_rows(r) + step_size * upd
                for v in range(4):
                    th[r, v] = theta[v * B:(v + 1) * B]
                done.append(r)

            @pl.when(step < NUM_STEPS - 1)
            def _():
                for r in done:
                    prepare(r, get_rows(r), 1 - slot)

            for o in range(4):
                @pl.when(jnp.logical_and(step == NUM_STEPS - 1, h == (o + 2) % 4 // 2))
                def _():
                    out_start(o)
            return cc
        with jax.named_scope("update"):
            lax.fori_loop(0, n_panels // 2, update, 0)
        with jax.named_scope("sendwait"):
            for m in pending:
                m.wait_send()
            for k, ta, tb in swaps:
                swap(k, ta, tb).wait_send()
        return carry

    lax.fori_loop(0, NUM_STEPS, one_step, 0)

    def out_second(h):
        d = 1 + h

        def place_of(src_at, v):
            return out_ref.at[pl.ds(h * hb, hb), cols(src_at, v) if h == 0 else cols(v, src_at)]

        def sends(tag):
            way = tag[1] == "+"
            b = 0 if way else 1
            out = []
            to = side(d, {"r": 2, "d": 1 if way else 3, "f": 0}[tag[0]])
            for at, o in enumerate(pieces(tag)):
                v = near[2 - h][o]
                if tag[0] == "f":
                    out.append((rel3.at[h, b, at], place_of(side(d, 3 if way else 1), v)))
                    continue
                src = mine(th, h, to, me[2 - h]) if o == 0 else m1.at[h, v, to]
                out.append((src, place_of(me[d], v) if tag[0] == "d" else rel3.at[h, b, at]))
            return out
        return relayed(("out2", h), d, sends, begin=False)

    with jax.named_scope("out1"):
        first = [out_first(h) for h in range(2)]
        second = [out_second(h) for h in range(2)]
        for h in range(2):
            start_piece(second[h], 0)
        for v in range(4):
            m1[0, me[2], v] = th[me[2], v, pl.ds(0, hb)]
            m1[1, me[1], v] = th[v, me[1], pl.ds(hb, hb)]
    with jax.named_scope("out2"):
        two_legs(first, second)
        own_out = []
        for v in range(4):
            own_out.append(local(("back", v), m1.at[0, v, me[1]], out_ref.at[pl.ds(0, hb), cols(me[1], v)]))
            own_out.append(local(("back", 4 + v), m1.at[1, v, me[2]], out_ref.at[pl.ds(hb, hb), cols(v, me[2])]))
        for m in own_out:
            m.start()
        close(first, second)
        for m in own_out:
            m.wait()


def run_steps(theta, lam, mu, fac, sizes, kern_width, step_size):
    n_total, fcol = theta.shape[0] * sizes[1] * sizes[2], theta.shape[1] // (sizes[1] * sizes[2])
    rank = fac.shape[1]
    nb = n_total // B
    n_chip = sizes[0] * sizes[1] * sizes[2]
    assert nb * nb == 4 * n_chip and rank == 4 * nb
    hb = B // 2
    cfg = dict(sizes=sizes, nb=nb, kern_width=kern_width, step_size=step_size)
    n1, n2 = n_chip, n_chip
    vmem = pl.BlockSpec(memory_space=pltpu.VMEM)
    most1 = max(n_chip // sizes[k] for k in range(3))
    most2 = max(sizes)
    blocks = (4, 4, B, fcol)
    scratch = [
        pltpu.VMEM(blocks, F32),
        pltpu.VMEM((2, 4, hb, 4 * fcol), F32),
        pltpu.VMEM((2, 4, 4, hb, fcol), F32),
        pltpu.VMEM((2, 2, hb // 2, 4 * fcol), F32),
        pltpu.VMEM((2, 2, 2, hb, fcol), F32),
        pltpu.VMEM((2, 2, 2, hb, fcol), F32),
        pltpu.VMEM((1, fcol), F32),
        pltpu.VMEM((1, fcol), F32),
        pltpu.VMEM((rank, fcol), BF16),
        pltpu.VMEM((2, n_total, fcol), BF16),
        pltpu.VMEM((n_total, fcol), BF16),
        pltpu.VMEM((n_total, fcol), BF16),
        pltpu.VMEM((rank, n_total), F32),
        pltpu.VMEM((rank // 2, n_total), F32),
        pltpu.VMEM((rank, n_total), F32),
        pltpu.VMEM((nb, 8, B), F32),
        pltpu.VMEM((nb, B, B), F32),
        pltpu.VMEM((3, n_chip, PIECE, B), F32),
        pltpu.VMEM((3, 4, most1, PIECE, B), F32),
        pltpu.VMEM((3, 2, 2, PIECE, B), F32),
        pltpu.VMEM((3, 4, most2, PIECE, B), F32),
        pltpu.VMEM((3, 4, PIECE, B), F32),
        pltpu.VMEM((3, most1, PIECE, B), F32),
        pltpu.VMEM((3, most2, PIECE, B), F32),
        pltpu.VMEM((3, PIECE, B), F32),
        pltpu.VMEM((3, n_chip, PIECE, B), BF16),
        pltpu.VMEM((3, n_chip, PIECE, B), BF16),
        pltpu.VMEM((n_total, n_total), BF16),
        pltpu.SemaphoreType.DMA((NUM_SEMS,)),
        pltpu.SemaphoreType.DMA((NUM_SEMS,)),
    ]
    hbm = pl.BlockSpec(memory_space=pltpu.HBM)
    return pl.pallas_call(
        functools.partial(steps_kernel, cfg),
        out_shape=jax.ShapeDtypeStruct(theta.shape, F32),
        in_specs=[hbm, vmem, vmem, hbm],
        out_specs=hbm,
        scratch_shapes=scratch,
        compiler_params=pltpu.CompilerParams(collective_id=0, has_side_effects=True, vmem_limit_bytes=60 * 1024 * 1024),
        name="svgd_steps",
    )(theta, lam[None], mu[None], fac.T)


def solution(mesh, sizes=(4, 4, 4)):
    part_size = mesh.shape["part"]
    feat_size = mesh.shape["feat"]

    def local_steps(local_theta, prec_loc, mean_loc, factor_loc):
        rows_loc, feat_loc = local_theta.shape
        n_total = rows_loc * part_size
        feat_total = feat_loc * feat_size
        kern_width = 2.0 * feat_total / math.log(n_total)
        step_size = 0.15 * n_total * feat_total / math.log(n_total)
        return run_steps(local_theta, prec_loc, mean_loc, factor_loc, sizes, kern_width, step_size)

    row_spec = P(("ens", "part"), "feat")
    vec_spec = P(("ens", "feat"))
    fac_spec = P(("ens", "feat"), None)
    return jax.shard_map(local_steps, mesh=mesh, in_specs=(row_spec, vec_spec, vec_spec, fac_spec), out_specs=row_spec, check_vma=False)
```

```python
import functools
import math
import jax
import jax.numpy as jnp
from jax import lax
from jax.experimental import pallas as pl
from jax.experimental.pallas import tpu as pltpu
from jax.sharding import PartitionSpec as P

NUM_STEPS = 3
B = 128
PIECE = 48
F32 = jnp.float32
BF16 = jnp.bfloat16
NT = (((1,), (1,)), ((), ()))
TN = (((0,), (0,)), ((), ()))
NUM_SEMS = 416
PANEL = 512


def rem(a, n):
    return lax.rem(a, jnp.int32(n))


def div(a, n):
    return lax.div(a, jnp.int32(n))


def unrolled(count, by, body):
    def several(r, cc):
        for t in range(by):
            body(r * by + t)
        return cc
    lax.fori_loop(0, count // by, several, 0)


def mine(ref, h, v, src_at):
    hb = B // 2
    return ref.at[src_at, v, pl.ds(0, hb)] if h == 0 else ref.at[v, src_at, pl.ds(hb, hb)]


def steps_kernel(cfg, theta_ref, lam_all, mu_all, fact_all, out_ref, th, l1, m1, rel1, rel2, rel3, lam_ref, mu_ref, fact_ref,
                 t_own, t_par, a_buf, zt, zt_par, zt_b, s_all, d_all, g, ring1, relb, dirb, dir3, acc2, acc3, unit, ag,
                 ag_par, kfull, send_sems, recv_sems):
    nb, kern_width, step_size = cfg["nb"], cfg["kern_width"], cfg["step_size"]
    n_total = nb * B
    n_chip = 64
    part, feat = lax.axis_index("part"), lax.axis_index("feat")
    core = rem(feat, 2)
    me = (div(feat, 2), rem(part, 4), div(part, 4))
    near = [[me[d]] + [rem(me[d] + by, 4) for by in (1, 2, 3)] for d in range(3)]

    def dev(coord, c):
        return {"part": coord[2] * 4 + coord[1], "feat": coord[0] * 2 + c}

    def device_at(dim, by):
        c = list(me)
        c[dim] = near[dim][by]
        return dev(c, core)

    around = [[device_at(d, by) for by in range(4)] for d in range(3)]

    def shifted(dim, by):
        return around[dim][by]

    partner = dev(me, 1 - core)
    perms = [(k, (k + 1) % 3, (k + 2) % 3) for k in range(3)]

    ids = {}

    def slot_of(key):
        idx = ids.setdefault(key, len(ids))
        assert idx < NUM_SEMS - 8
        return idx

    def copy(key, src, dst, to):
        idx = slot_of(key)
        return pltpu.make_async_remote_copy(
            src_ref=src, dst_ref=dst, send_sem=send_sems.at[idx], recv_sem=recv_sems.at[idx],
            device_id=to, device_id_type=pl.DeviceIdType.MESH)

    def local(key, src, dst):
        return pltpu.make_async_copy(src, dst, send_sems.at[slot_of(key)])

    barrier = pltpu.get_barrier_semaphore()
    peers = [partner] + [shifted(d, by) for d in range(3) for by in (1, 2, 3)]
    for peer in peers:
        pl.semaphore_signal(barrier, inc=1, device_id=peer, device_id_type=pl.DeviceIdType.MESH)
    pl.semaphore_wait(barrier, len(peers))

    row = lax.broadcasted_iota(jnp.int32, (B, B), 0)
    col = lax.broadcasted_iota(jnp.int32, (B, B), 1)
    low, eye = row >= col, row == col

    def blk(i):
        return pl.ds(pl.multiple_of(i * B, B), B)

    def unit_of(c, q):
        u = c * n_chip + q
        i = rem(u, nb)
        return u, i, rem(i + div(u, nb) + 1, nb), u >= 2 * n_chip - nb // 2

    def chip_index(k, x, y, z):
        p = perms[k]
        c = (x, y, z)
        return (c[p[0]] * 4 + c[p[1]]) * 4 + c[p[2]]

    def split(n, wide):
        if n > 1:
            return (0, n // 2, 0, PIECE), (n // 2, n // 2, 0, PIECE)
        r = 32 if wide else 24
        return (0, 1, 0, r), (0, 1, r, PIECE - r)

    def part_of(ref, lead, base, half):
        return ref.at[lead, pl.ds(base + half[0], half[1]), pl.ds(half[2], half[3])]

    zh = zt.shape[0] // 2
    kc = nb // 4
    n_panels = n_total // PANEL

    def panel(r):
        return pl.ds(pl.multiple_of(r * PANEL, PANEL), PANEL)

    def swap_t(r, slot):
        return pltpu.make_async_remote_copy(
            src_ref=t_own.at[slot, panel(r)], dst_ref=t_par.at[panel(r)], send_sem=send_sems.at[NUM_SEMS - 1 - r],
            recv_sem=recv_sems.at[NUM_SEMS - 1 - r], device_id=partner, device_id_type=pl.DeviceIdType.MESH)

    def swap_z(r):
        return pltpu.make_async_remote_copy(
            src_ref=zt.at[pl.ds(pl.multiple_of((1 - core) * zh, 8), zh), panel(r)], dst_ref=zt_par.at[pl.ds(0, zh), panel(r)],
            send_sem=send_sems.at[NUM_SEMS - 1 - n_panels - r], recv_sem=recv_sems.at[NUM_SEMS - 1 - n_panels - r],
            device_id=partner, device_id_type=pl.DeviceIdType.MESH)

    def prepare(r, theta, slot):
        t_own[slot, panel(r)] = theta.astype(BF16)
        swap_t(r, slot).start()
        xb = (theta - mu_ref[...]).astype(BF16)
        zt[:, panel(r)] = lax.dot_general(fact_ref[...], xb, NT, preferred_element_type=F32)
        swap_z(r).start()

    def get_rows(r):
        return jnp.concatenate([th[r, v] for v in range(4)], 0)

    def first_prep(r, cc):
        prepare(r, get_rows(r), 0)
        return cc
    fcol, hb = fact_ref.shape[1], B // 2
    my = pl.ds(pl.multiple_of((me[1] * 4 + me[2]) * fcol, fcol), fcol)

    def cols(y, z, n=1):
        return pl.ds(pl.multiple_of((y * 4 + z) * fcol, fcol), n * fcol)

    def side(d, by):
        return near[d][by]

    def relayed(key, d, sends, begin=True):
        def copies(tag):
            return [copy((key, tag, t), src, dst, shifted(d, 1 if tag[1] == "+" else 3))
                    for t, (src, dst) in enumerate(sends(tag))]
        started = []

        def go(tags):
            for tag in tags:
                for m in copies(tag):
                    m.start()
                    started.append(m)

        def relay():
            for got, out in (("r+", "f+"), ("r-", "f-")):
                for m in copies(got):
                    m.wait_recv()
                go((out,))

        def finish():
            for tag in ("d+", "d-", "f+", "f-"):
                for m in copies(tag):
                    m.wait_recv()
        if begin:
            go(("r+", "r-", "d+", "d-"))
        else:
            for tag in ("r+", "r-", "d+", "d-"):
                started += copies(tag)
        return relay, finish, started, copies

    def halves(tag):
        if tag[0] == "d":
            return (0, 1, 2, 3)
        return (0, 1) if tag[1] == "+" else (2, 3)

    def in_first(h):
        d = 1 + h

        def sends(tag):
            r0, nr = {"r+": (0, hb // 2), "r-": (hb // 2, hb // 2)}.get(tag, (0, hb))
            way = tag[1] == "+"
            if tag[0] == "f":
                b = 0 if way else 1
                return [(rel1.at[h, b], l1.at[h, side(d, 3 if way else 1), pl.ds(b * (hb // 2), hb // 2)])]
            to = side(d, {"r": 2, "d": 1 if way else 3}[tag[0]])
            rows = pl.ds(h * hb + r0, nr)

            def dst(y, n):
                at = pl.ds(y * fcol, n * fcol)
                if tag[0] == "d":
                    return l1.at[h, me[d], pl.ds(0, nr), at]
                return rel1.at[h, 0 if way else 1, pl.ds(0, nr), at]
            if h == 0:
                return [(theta_ref.at[rows, cols(to, 0, 4)], dst(0, 4))]
            return [(theta_ref.at[rows, cols(y, to)], dst(y, 1)) for y in range(4)]
        return relayed(("in1", h), d, sends)

    def pieces(tag):
        return (0, 3, 1, 2) if tag[0] == "d" else (0, 3) if tag[1] == "+" else (1, 2)

    def start_piece(leg, o):
        for tag in ("r+" if o in (0, 3) else "r-", "d+", "d-"):
            leg[3](tag)[pieces(tag).index(o)].start()

    def two_legs(first, second):
        for h in range(2):
            first[h][0]()
        for tag, o in (("d+", 3), ("d-", 1)):
            for h in range(2):
                for m in first[h][3](tag):
                    m.wait_recv()
                start_piece(second[h], o)
        for h in range(2):
            for tag in ("f+", "f-"):
                for m in first[h][3](tag):
                    m.wait_recv()
            start_piece(second[h], 2)

    def close(first, second):
        for h in range(2):
            second[h][0]()
        for h in range(2):
            second[h][1]()
        for leg in first + second:
            for m in leg[2]:
                m.wait_send()

    def in_second(h):
        d = 2 - h

        def sends(tag):
            way = tag[1] == "+"
            b = 0 if way else 1
            out = []
            to = side(d, {"r": 2, "d": 1 if way else 3, "f": 0}[tag[0]])
            for at, o in enumerate(pieces(tag)):
                v = near[1 + h][o]
                if tag[0] == "f":
                    out.append((rel2.at[h, b, at], mine(th, h, v, side(d, 3 if way else 1))))
                    continue
                if o == 0:
                    src = theta_ref.at[pl.ds(h * hb, hb), cols(me[1], to) if h == 0 else cols(to, me[2])]
                else:
                    src = l1.at[h, v, pl.ds(0, hb), pl.ds(pl.multiple_of(to * fcol, fcol), fcol)]
                out.append((src, mine(th, h, v, me[d]) if tag[0] == "d" else rel2.at[h, b, at]))
            return out
        return relayed(("in2", h), d, sends, begin=False)

    own_in = [local(("own", 0), theta_ref.at[pl.ds(0, hb), cols(me[1], 0, 4)], l1.at[0, me[1]])]
    own_in += [local(("own", 1 + y), theta_ref.at[pl.ds(hb, hb), cols(y, me[2])],
                     l1.at[1, me[2], pl.ds(0, hb), pl.ds(y * fcol, fcol)]) for y in range(4)]
    own_in.append(local(("own", 5), fact_all.at[pl.ds(0, fact_ref.shape[0]), my], fact_ref))

    with jax.named_scope("in1"):
        first = [in_first(h) for h in range(2)]
        second = [in_second(h) for h in range(2)]
        for m in own_in:
            m.start()
        for h in range(2):
            start_piece(second[h], 0)
        lam_ref[...] = lam_all[pl.ds(0, 1), my]
        mu_ref[...] = mu_all[pl.ds(0, 1), my]
    with jax.named_scope("in2"):
        two_legs(first, second)
        for m in own_in:
            m.wait()
        for v in range(4):
            th[me[2], v, pl.ds(0, hb)] = l1[0, v, pl.ds(0, hb), pl.ds(pl.multiple_of(me[2] * fcol, fcol), fcol)]
            th[v, me[1], pl.ds(hb, hb)] = l1[1, v, pl.ds(0, hb), pl.ds(pl.multiple_of(me[1] * fcol, fcol), fcol)]
        close(first, second)

    with jax.named_scope("prep"):
        lax.fori_loop(0, n_panels, first_prep, 0)

    def out_pieces(h, tag):
        if h == 0:
            return halves(tag)
        return (0, 1, 2, 3) if tag[0] == "d" else (2, 3) if tag[1] == "+" else (0, 1)

    def out_first(h):
        d = 2 - h

        def sends(tag):
            way = tag[1] == "+"
            b = 0 if way else 1
            vs = [(v if h == 0 else near[2][v], v % 2) for v in out_pieces(h, tag)]
            if tag[0] == "f":
                return [(rel2.at[h, b, at], m1.at[h, side(d, 3 if way else 1), v]) for v, at in vs]
            to = side(d, {"r": 2, "d": 1 if way else 3}[tag[0]])
            return [(mine(th, h, v, to), m1.at[h, me[d], v] if tag[0] == "d" else rel2.at[h, b, at]) for v, at in vs]
        return relayed(("out1", h), d, sends, begin=False)

    def out_start(o):
        for tag in ((), ("d+",), ("r+", "r-"), ("d-",))[o]:
            for m in out_first(0)[3](tag):
                m.start()
        for tag in ("r+" if o >= 2 else "r-", "d+", "d-"):
            out_first(1)[3](tag)[out_pieces(1, tag).index(o)].start()

    def one_step(step, carry):
        slot = rem(step, 2)
        with jax.named_scope("twait"):
            for r in range(n_panels):
                swap_t(r, slot).wait()
                swap_z(r).wait()

        def products(rows, cols):
            return (lax.dot_general(jnp.concatenate([t_own[slot, r] for r in rows], 0), t_own[slot, cols], NT,
                                    preferred_element_type=F32)
                    + lax.dot_general(jnp.concatenate([t_par[r] for r in rows], 0), t_par[cols], NT,
                                      preferred_element_type=F32))

        def put(m, x, y, z):
            g[0, chip_index(0, x, y, z)] = m[:48]
            g[1, chip_index(1, x, y, z)] = m[48:96]
            g[2, chip_index(2, x, y, z), pl.ds(0, 32)] = m[96:]

        def form(h, cc):
            i = h * 2
            cols = pl.ds(pl.multiple_of(i * B, 2 * B), 2 * B)
            dg = products([cols], cols)
            for t in range(2):
                dt = dg[t * B:(t + 1) * B, t * B:(t + 1) * B]
                d_all[i + t] = dt
                s_all[i + t] = jnp.broadcast_to(jnp.sum(jnp.where(eye, dt, 0.0), axis=0, keepdims=True), (8, B))
            m = products([blk(rem(i + core * kc + 1 + t, nb)) for t in range(kc + 1)], cols)
            y, z = div(h, 2), 2 * rem(h, 2)
            for t in range(kc + 1):
                if t < kc:
                    put(m[t * B:(t + 1) * B, :B], t, y, z)
                if t > 0:
                    put(m[t * B:(t + 1) * B, B:], t - 1, y, z + 1)
            return cc
        with jax.named_scope("form"):
            lax.fori_loop(0, nb // 2, form, 0, unroll=4)

        with jax.named_scope("pair"):
            @pl.when(core == 1)
            def _():
                def pair(t, cc):
                    i = t + nb // 2
                    put(jnp.where(low, d_all[i], d_all[t]), 3, div(i, 4), rem(i, 4))
                    return cc
                lax.fori_loop(0, nb // 2, pair, 0)

        pending = []

        order = (2, 1, 3, 0)
        wave_base = [[[(near[perms[k][0]][t] * 4 + near[perms[k][1]][o]) * 4 for t in range(4)] for o in order]
                     for k in range(3)]

        def wave(k, s):
            return perms[k], 4, order[s], wave_base[k][s]

        def n_waves(k):
            return 4

        def ring_copy(k, s, tag):
            p, n, by, base = wave(k, s)
            ha, hb = split(n, False)
            at, half, kind, to = {
                "m1p": (2, ha, 0, 1), "m1m": (2, hb, 1, 3), "m2p": (1, hb, 2, 1), "m2m": (3, ha, 3, 3),
                "m3p": (1, ha, 2, 1), "m3m": (3, hb, 3, 3)}[tag]
            return copy(("rs", k, s, tag), part_of(g, k, base[at], half), part_of(ring1.at[k], kind, s * n, half),
                        shifted(p[0], to))

        def ring_start(s, tags, colours=(0, 1, 2)):
            for tag in tags:
                for k in colours:
                    if s < n_waves(k):
                        m = ring_copy(k, s, tag)
                        m.start()
                        pending.append(m)

        def ring_merge(s):
            for k in range(3):
                p, n, by, base = wave(k, s)
                ha, hb = split(n, False)
                for got, out, at, half, kind in (("m1p", "m3p", 1, ha, 0), ("m1m", "m3m", 3, hb, 1)):
                    ring_copy(k, s, got).wait_recv()
                    part_of(g, k, base[at], half)[...] += part_of(ring1.at[k], kind, s * n, half)[...]
                    m = ring_copy(k, s, out)
                    m.start()
                    pending.append(m)

        def owner_copy(k, by, s):
            return copy(("rb", k, by), acc2.at[k, pl.ds(s * 4, 4)], dirb.at[k, by], shifted(perms[k][1], by))

        def via_copy(k, b):
            return copy(("rv", k, b), acc2.at[k, pl.ds(2 * b, 2)], relb.at[k, b], shifted(perms[k][1], (1, 3)[b]))

        def ring_finish(s):
            for k in range(3):
                p, n, by, base = wave(k, s)
                for tag in ("m2p", "m2m", "m3p", "m3m"):
                    ring_copy(k, s, tag).wait_recv()
                if by in (1, 3):
                    via_copy(k, by // 2).wait_recv()
                for v in range(n):
                    tot = g[k, base[0] + v] + ring1[k, 2, s * n + v] + ring1[k, 3, s * n + v]
                    if by in (1, 3) and v // 2 == by // 2:
                        tot = tot + relb[k, by // 2, v % 2]
                    acc2[k, s * n + v] = tot
                ms = [via_copy(k, 0), via_copy(k, 1)] if by == 2 else [owner_copy(k, by, s)] if by else []
                for m in ms:
                    m.start()
                    pending.append(m)

        ring_start(0, ("m1p", "m1m"), (0, 1))

        row8 = lax.broadcasted_iota(jnp.int32, (8, B), 0)

        def tails(i, cc):
            y, z = div(i, 4), rem(i, 4)
            for x in range(4):
                off = core * kc + x
                at = chip_index(2, x, y, z)
                g[2, at, pl.ds(32, 8)] = jnp.where(row8 == 0, s_all[rem(i + off + 1, nb)], s_all[i])
                g[2, at, pl.ds(40, 8)] = (zt[pl.ds(pl.multiple_of(off * 8, 8), 8), blk(i)]
                                          + zt_par[pl.ds(x * 8, 8), blk(i)])
            return cc
        with jax.named_scope("tails"):
            lax.fori_loop(0, nb, tails, 0)

        most = 4
        with jax.named_scope("rs0"):
            ring_start(0, ("m1p", "m1m"), (2,))
            ring_start(0, ("m2p", "m2m"))
            ring_start(1, ("m1p", "m1m"))
            for s in range(most):
                ring_merge(s)
                ring_start(s + 1, ("m2p", "m2m"))
                ring_start(s + 2, ("m1p", "m1m"))
                if s:
                    ring_finish(s - 1)
            ring_finish(most - 1)
        last = []
        with jax.named_scope("rs1"):
            for k in range(3):
                p = perms[k]
                n, s = 4, 3
                bys = (1, 3)
                for by in bys:
                    owner_copy(k, by, 0).wait_recv()
                for v in range(n):
                    tot = acc2[k, s * n + v]
                    for by in bys:
                        tot = tot + dirb[k, by, v]
                    acc3[k, v] = tot
                ms = []
                for by in (1, 2, 3):
                    m = copy(("rc", k, by), acc3.at[k, near[p[2]][by]], dir3.at[k, by],
                             shifted(p[2], by))
                    m.start()
                    ms.append(m)
                last.append(ms)
                pending += ms
        with jax.named_scope("rs2"):
            for k in range(3):
                tot = acc3[k, me[perms[k][2]]]
                for m in last[k]:
                    m.wait_recv()
                for by in range(1, len(last[k]) + 1):
                    tot = tot + dir3[k, by]
                unit[k] = tot

        summed = pending
        pending = []
        with jax.named_scope("kunit"):
            packed = unit_of(core, (me[0] * 4 + me[1]) * 4 + me[2])[3]
            g_u = jnp.concatenate([unit[0], unit[1], unit[2, pl.ds(0, 32)]], 0)
            sj = jnp.broadcast_to(unit[2, pl.ds(32, 1)], (B, B))
            si = jnp.broadcast_to(unit[2, pl.ds(33, 1)], (B, B))
            si_c = jnp.broadcast_to(jnp.sum(jnp.where(eye, si, 0.0), axis=1, keepdims=True), (B, B))
            sj_c = jnp.broadcast_to(jnp.sum(jnp.where(eye, sj, 0.0), axis=1, keepdims=True), (B, B))
            lower = jnp.logical_and(packed, low)
            upper = jnp.logical_and(packed, jnp.logical_not(low))
            s_sum = jnp.where(lower, si_c, sj_c) + jnp.where(upper, sj, si)
            dist = jnp.maximum(s_sum - 2.0 * g_u, 0.0)
            k_u = jnp.exp(-dist / kern_width)
            z_u = unit[2, pl.ds(40, 8)]
            pieces = (k_u[:48], k_u[48:96], jnp.concatenate([k_u[96:], z_u, jnp.zeros_like(z_u)], 0))
            own = [chip_index(k, *me) for k in range(3)]
            for k in range(3):
                ag[k, own[k]] = pieces[k].astype(BF16)

        def place(ref, c, k, a, b, at):
            for v in range(4):
                coord = [0, 0, 0]
                for d, t in zip(perms[k], (a, b, v)):
                    coord[d] = t
                off = c * kc + coord[0]
                i = coord[1] * 4 + coord[2]
                top = (rem(i + off + 1, nb) + div(off * nb + i, 2 * n_chip - nb // 2) * (nb // 2)) * B + 48 * k
                n = (48, 48, 32)[k]
                kfull[pl.ds(pl.multiple_of(top, 16), n), blk(i)] = ref[k, at + v, pl.ds(0, n)]
                if k == 2:
                    tail = ref[k, at + v, pl.ds(32, 16)].astype(F32)
                    zt_b[pl.ds(pl.multiple_of(off * 8, 8), 8), blk(i)] = tail[:8]

        chunks = {}

        def chunk(k, ta, tb):
            if (k, ta, tb) not in chunks:
                p = perms[k]
                a, b = near[p[0]][ta], near[p[1]][tb]
                chunks[k, ta, tb] = (a, b, (a * 4 + b) * 4, 4)
            return chunks[k, ta, tb]

        def swap(k, ta, tb):
            a, b, at, n = chunk(k, ta, tb)
            return copy(("sw", k, ta, tb), ag.at[k, pl.ds(at, n)], ag_par.at[k, pl.ds(at, n)], partner)

        swaps = []
        placed = []

        def take(upto):
            while len(placed) < upto:
                k, ta, tb = swaps[len(placed)]
                swap(k, ta, tb).wait_recv()
                a, b, at, n = chunk(k, ta, tb)
                place(ag_par, 1 - core, k, a, b, at)
                placed.append((k, ta, tb))

        def have(k, ta, tb):
            swap(k, ta, tb).start()
            swaps.append((k, ta, tb))
            a, b, at, n = chunk(k, ta, tb)
            place(ag, core, k, a, b, at)

        def unit_copy(stage, k, by, tc, start):
            p = perms[k]
            a, b, at, n = chunk(k, 0, 0)
            at = at + near[p[2]][tc]
            m = copy(("u", stage, k, by, tc), ag.at[k, at], ag.at[k, at], shifted(p[stage], by))
            if start:
                m.start()
                pending.append(m)
            return m

        def a_copy(k, tb, tag, start=False):
            p = perms[k]
            ta, h, to = {"n1p": (0, 0, 1), "n1m": (0, 1, 3), "n2p": (0, 1, 1), "n2m": (0, 0, 3), "n3p": (3, 0, 1),
                         "n3m": (1, 1, 3)}[tag]
            a, b, at, n = chunk(k, ta, tb)
            half = split(n, True)[h]
            m = copy(("a", k, tb, tag), part_of(ag, k, at, half), part_of(ag, k, at, half), shifted(p[0], to))
            if start:
                m.start()
                pending.append(m)
            return m

        def a_launch(k, tb):
            for tag in ("n1p", "n1m", "n2p", "n2m"):
                a_copy(k, tb, tag, True)
            have(k, 0, tb)

        def a_relay(tb):
            for k in range(3):
                if True:
                    for got, out in (("n1p", "n3p"), ("n1m", "n3m")):
                        a_copy(k, tb, got).wait_recv()
                        a_copy(k, tb, out, True)

        def a_near(tb):
            for k in range(3):
                if True:
                    for got, ta in (("n2p", 3), ("n2m", 1)):
                        a_copy(k, tb, got).wait_recv()
                        have(k, ta, tb)

        def a_far(tb):
            for k in range(3):
                if True:
                    for got in ("n3p", "n3m"):
                        a_copy(k, tb, got).wait_recv()
                    have(k, 2, tb)

        def a_waves(tbs):
            for tb in tbs:
                for k in range(3):
                    a_launch(k, tb)

        with jax.named_scope("ag2"):
            for k in range(3):
                for by in (1, 2, 3):
                    unit_copy(2, k, by, 0, True)
            for k in range(3):
                for by in (2, 1, 3):
                    unit_copy(1, k, by, 0, True)
            for m in summed:
                m.wait_send()
            for by in (1, 3, 2):
                for k in range(3):
                    unit_copy(2, k, by, 0, False).wait_recv()
                    for bb in (2, 1, 3):
                        unit_copy(1, k, bb, 4 - by, True)
            a_waves((0,))

        def b_arrivals(bb):
            for k in range(3):
                for tc in range(4):
                    unit_copy(1, k, bb, tc, False).wait_recv()

        with jax.named_scope("ag1"):
            for name, stage, at, got in (("b1", b_arrivals, 1, 0), ("b3", b_arrivals, 3, 0), ("r0", a_relay, 0, 0),
                                         ("w", a_waves, (3, 1), 0), ("b2", b_arrivals, 2, 0), ("w2", a_waves, (2,), 3),
                                         ("r3", a_relay, 3, 3), ("n0", a_near, 0, 6), ("r1", a_relay, 1, 9),
                                         ("r2", a_relay, 2, 12), ("n3", a_near, 3, 15)):
                with jax.named_scope("ag1_" + name):
                    stage(at)
                    take(min(got, len(swaps) - 3))
        with jax.named_scope("ag0"):
            for stage, tb in ((a_far, 0), (a_near, 1), (a_far, 3), (a_near, 2), (a_far, 1), (a_far, 2)):
                before = len(swaps)
                with jax.named_scope("ag0_%s%d" % (stage.__name__, tb)):
                    stage(tb)
                take(before - 12)

        per = 8

        def mirror(c, r, cc):
            at = []
            for t in range(per):
                u, i, j, packed = unit_of(c, r * per + t)
                at.append((i, j, kfull[blk(j), blk(i)].T))
            for i, j, m in at:
                kfull[blk(i), blk(j)] = m
            return cc

        def unpack(r, cc):
            both = []
            for v in range(4):
                i = r * 4 + v + nb // 2
                m = kfull[blk(i), blk(i)].astype(F32)
                mt = m.T
                both.append((jnp.where(eye, 1.0, jnp.where(low, m, mt)), jnp.where(eye, 1.0, jnp.where(low, mt, m))))
            for v, (m, mt) in enumerate(both):
                t = r * 4 + v
                kfull[blk(t + nb // 2), blk(t + nb // 2)] = m.astype(BF16)
                kfull[blk(t), blk(t)] = mt.astype(BF16)
            return cc
        with jax.named_scope("mirror1"):
            lax.fori_loop(0, div(n_chip - core * (nb // 2), per), functools.partial(mirror, core), 0)
        with jax.named_scope("swapwait"):
            take(len(swaps))
        with jax.named_scope("mirror2"):
            lax.fori_loop(0, div(n_chip - (1 - core) * (nb // 2), per), functools.partial(mirror, 1 - core), 0)
            lax.fori_loop(0, nb // 8, unpack, 0)

        def grads(r, cc):
            lowt = lax.dot_general(zt_b[:, panel(r)].astype(BF16), fact_ref[...], TN, preferred_element_type=F32)
            a_buf[panel(r)] = (-((get_rows(r) - mu_ref[...]) * lam_ref[...] + lowt)).astype(BF16)
            return cc
        with jax.named_scope("grads"):
            lax.fori_loop(0, n_panels, grads, 0, unroll=2)

        def update(h, cc):
            done = []
            for t in range(2):
                r = rem(me[2] + 2 + 2 * h + t, 4)
                kr = kfull[panel(r)]
                mass = jnp.sum(kr.astype(F32), axis=1, keepdims=True)
                drive = jnp.dot(kr, a_buf[...], preferred_element_type=F32)
                pull = jnp.dot(kr, t_own[slot], preferred_element_type=F32)
                upd = (drive + (2.0 / kern_width) * (mass * t_own[slot, panel(r)].astype(F32) - pull)) / n_total
                theta = get_rows(r) + step_size * upd
                for v in range(4):
                    th[r, v] = theta[v * B:(v + 1) * B]
                done.append(r)

            @pl.when(step < NUM_STEPS - 1)
            def _():
                for r in done:
                    prepare(r, get_rows(r), 1 - slot)

            for o in range(4):
                @pl.when(jnp.logical_and(step == NUM_STEPS - 1, h == (o + 2) % 4 // 2))
                def _():
                    out_start(o)
            return cc
        with jax.named_scope("update"):
            lax.fori_loop(0, n_panels // 2, update, 0)
        with jax.named_scope("sendwait"):
            for m in pending:
                m.wait_send()
            for k, ta, tb in swaps:
                swap(k, ta, tb).wait_send()
        return carry

    lax.fori_loop(0, NUM_STEPS, one_step, 0)

    def out_second(h):
        d = 1 + h

        def place_of(src_at, v):
            return out_ref.at[pl.ds(h * hb, hb), cols(src_at, v) if h == 0 else cols(v, src_at)]

        def sends(tag):
            way = tag[1] == "+"
            b = 0 if way else 1
            out = []
            to = side(d, {"r": 2, "d": 1 if way else 3, "f": 0}[tag[0]])
            for at, o in enumerate(pieces(tag)):
                v = near[2 - h][o]
                if tag[0] == "f":
                    out.append((rel3.at[h, b, at], place_of(side(d, 3 if way else 1), v)))
                    continue
                src = mine(th, h, to, me[2 - h]) if o == 0 else m1.at[h, v, to]
                out.append((src, place_of(me[d], v) if tag[0] == "d" else rel3.at[h, b, at]))
            return out
        return relayed(("out2", h), d, sends, begin=False)

    with jax.named_scope("out1"):
        first = [out_first(h) for h in range(2)]
        second = [out_second(h) for h in range(2)]
        for h in range(2):
            start_piece(second[h], 0)
        for v in range(4):
            m1[0, me[2], v] = th[me[2], v, pl.ds(0, hb)]
            m1[1, me[1], v] = th[v, me[1], pl.ds(hb, hb)]
    with jax.named_scope("out2"):
        two_legs(first, second)
        own_out = []
        for v in range(4):
            own_out.append(local(("back", v), m1.at[0, v, me[1]], out_ref.at[pl.ds(0, hb), cols(me[1], v)]))
            own_out.append(local(("back", 4 + v), m1.at[1, v, me[2]], out_ref.at[pl.ds(hb, hb), cols(v, me[2])]))
        for m in own_out:
            m.start()
        close(first, second)
        for m in own_out:
            m.wait()


def run_steps(theta, lam, mu, fac, sizes, kern_width, step_size):
    n_total, fcol = theta.shape[0] * sizes[1] * sizes[2], theta.shape[1] // (sizes[1] * sizes[2])
    rank = fac.shape[1]
    nb = n_total // B
    n_chip = sizes[0] * sizes[1] * sizes[2]
    assert nb * nb == 4 * n_chip and rank == 4 * nb
    hb = B // 2
    cfg = dict(sizes=sizes, nb=nb, kern_width=kern_width, step_size=step_size)
    n1, n2 = n_chip, n_chip
    vmem = pl.BlockSpec(memory_space=pltpu.VMEM)
    most1 = max(n_chip // sizes[k] for k in range(3))
    most2 = max(sizes)
    blocks = (4, 4, B, fcol)
    scratch = [
        pltpu.VMEM(blocks, F32),
        pltpu.VMEM((2, 4, hb, 4 * fcol), F32),
        pltpu.VMEM((2, 4, 4, hb, fcol), F32),
        pltpu.VMEM((2, 2, hb // 2, 4 * fcol), F32),
        pltpu.VMEM((2, 2, 2, hb, fcol), F32),
        pltpu.VMEM((2, 2, 2, hb, fcol), F32),
        pltpu.VMEM((1, fcol), F32),
        pltpu.VMEM((1, fcol), F32),
        pltpu.VMEM((rank, fcol), BF16),
        pltpu.VMEM((2, n_total, fcol), BF16),
        pltpu.VMEM((n_total, fcol), BF16),
        pltpu.VMEM((n_total, fcol), BF16),
        pltpu.VMEM((rank, n_total), F32),
        pltpu.VMEM((rank // 2, n_total), F32),
        pltpu.VMEM((rank, n_total), F32),
        pltpu.VMEM((nb, 8, B), F32),
        pltpu.VMEM((nb, B, B), F32),
        pltpu.VMEM((3, n_chip, PIECE, B), F32),
        pltpu.VMEM((3, 4, most1, PIECE, B), F32),
        pltpu.VMEM((3, 2, 2, PIECE, B), F32),
        pltpu.VMEM((3, 4, most2, PIECE, B), F32),
        pltpu.VMEM((3, 4, PIECE, B), F32),
        pltpu.VMEM((3, most1, PIECE, B), F32),
        pltpu.VMEM((3, most2, PIECE, B), F32),
        pltpu.VMEM((3, PIECE, B), F32),
        pltpu.VMEM((3, n_chip, PIECE, B), BF16),
        pltpu.VMEM((3, n_chip, PIECE, B), BF16),
        pltpu.VMEM((n_total, n_total), BF16),
        pltpu.SemaphoreType.DMA((NUM_SEMS,)),
        pltpu.SemaphoreType.DMA((NUM_SEMS,)),
    ]
    hbm = pl.BlockSpec(memory_space=pltpu.HBM)
    return pl.pallas_call(
        functools.partial(steps_kernel, cfg),
        out_shape=jax.ShapeDtypeStruct(theta.shape, F32),
        in_specs=[hbm, vmem, vmem, hbm],
        out_specs=hbm,
        scratch_shapes=scratch,
        compiler_params=pltpu.CompilerParams(collective_id=0, has_side_effects=True, vmem_limit_bytes=60 * 1024 * 1024),
        name="svgd_steps",
    )(theta, lam[None], mu[None], fac.T)


def solution(mesh, sizes=(4, 4, 4)):
    part_size = mesh.shape["part"]
    feat_size = mesh.shape["feat"]

    def local_steps(local_theta, prec_loc, mean_loc, factor_loc):
        rows_loc, feat_loc = local_theta.shape
        n_total = rows_loc * part_size
        feat_total = feat_loc * feat_size
        kern_width = 2.0 * feat_total / math.log(n_total)
        step_size = 0.15 * n_total * feat_total / math.log(n_total)
        return run_steps(local_theta, prec_loc, mean_loc, factor_loc, sizes, kern_width, step_size)

    row_spec = P(("ens", "part"), "feat")
    vec_spec = P(("ens", "feat"))
    fac_spec = P(("ens", "feat"), None)
    return jax.shard_map(local_steps, mesh=mesh, in_specs=(row_spec, vec_spec, vec_spec, fac_spec), out_specs=row_spec, check_vma=False)
```
